512 devices in a mesh: dp: 8 (over z), win: 8 (over y), mp: 8 (over x, core).
Axes of the slice: x: 4, y: 8, z: 8, core: 2. Of those that a mesh axis runs over, the one named last changes fastest.
Arguments:
- tokens: bfloat16 [75264, 768], P(('dp', 'win', 'mp')), may hold values from -6 to 6
- target: bfloat16 [75264, 768], P(('dp', 'win', 'mp')), may hold values from -16 to 16
- regions: int32 [1536, 49], P(('dp', 'win')), may hold values from 0 to 3
- rel_index: int32 [49, 49], replicated, may hold values from 0 to 168
- layer_norm_gain: float32 [768], replicated, may hold values from 0.5 to 1.5
- bias_table: float32 [169, 24], P(None, 'mp'), may hold values from -5 to 330
- w_qkv: bfloat16 [3, 768, 768], P(None, 'mp'), may hold values from -0.21875 to 0.21875
- w_proj: bfloat16 [768, 768], P('mp'), may hold values from -0.21875 to 0.21875
Outputs:
- input_gradient: float32 [75264, 768], P(('dp', 'win', 'mp'))
- grad_qkv: float32 [3, 768, 768], P(None, 'mp', ('dp', 'win'))
- grad_proj: float32 [768, 768], P('mp', ('dp', 'win'))
- grad_table: float32 [169, 24], P(None, 'mp')
- gain_gradient: float32 [768], replicated
- loss: float32 [], replicated
The draws below stay inside these ranges and needn't reach their ends.
All inputs are finite; a program needn't handle non-finite values.
Results may differ from the reference program's by a relative error of at most 0.01.
Values may be sent and summed in bfloat16 or wider, within the bound.
A program may use at most 64 MiB of HBM per device.

```python
import jax
import jax.numpy as jnp
from jax import lax

C = 768
HEADS = 24
HD = 32
WIN_TOK = 49
TABLE = 169
WINDOWS = 1536
TOKENS = 75264
N_MP = 8


def draw_bias_table(key, part):
    base_key = jax.random.fold_in(jax.random.fold_in(key, 7), 0)
    base = jnp.clip(jax.random.normal(base_key, (TABLE, HEADS), jnp.float32), -5.0, 5.0)
    return base


def draw_target(key, part):
    noise_key = jax.random.fold_in(key, 11)
    fraction = jnp.arange(TOKENS, dtype=jnp.float32)[:, None] / (TOKENS - 1.0)
    noise = jnp.clip(jax.random.normal(noise_key, (TOKENS, C), jnp.float32), -4.0, 4.0)
    result = noise * (1.0 + 3.0 * fraction)
    return result.astype(jnp.bfloat16)


def touch_ends(values, rng, smallest, largest):
    place = [jax.random.randint(jax.random.fold_in(rng, axis), (), 0, length) for axis, length in enumerate(values.shape)]
    main_axis = values.shape.index(max(values.shape))
    next_to = place[:main_axis] + [(place[main_axis] + 1) % values.shape[main_axis]] + place[main_axis + 1:]
    return values.at[tuple(place)].set(smallest).at[tuple(next_to)].set(largest)


def level_of(own_key, extent, pieces, low, high):
    gain = 1.0
    for position, shards_of in pieces:
        draws = jax.random.uniform(jax.random.fold_in(jax.random.fold_in(own_key, 6), position), (shards_of,), jnp.float32, low / len(pieces), high / len(pieces))
        gain = gain * jnp.repeat(jnp.exp(draws), extent[position] // shards_of).reshape((-1,) + (1,) * (len(extent) - 1 - position))
    return gain


def centred(stream_key, shape, width, most, pieces=(), kind=jnp.bfloat16):
    entries = width * jax.random.normal(stream_key, shape, jnp.float32)
    if pieces:
        entries = entries * level_of(stream_key, shape, pieces, -0.22, 0.18)
    return jnp.clip(entries, -most, most).astype(kind)


def setup_inputs(seed: int = 0) -> dict:
    key_of = jax.random.split(jax.random.key(seed), 9)
    tokens = centred(key_of[0], (TOKENS, C), 1.0, 6.0, ((0, 512),))
    target = draw_target(jax.random.fold_in(key_of[8], 71), 0)
    regions = touch_ends(jax.random.randint(key_of[2], (WINDOWS, WIN_TOK), 0, 4), jax.random.fold_in(key_of[2], 1), 0, 3).astype(jnp.int32)
    rel_index = touch_ends(jax.random.randint(key_of[3], (WIN_TOK, WIN_TOK), 0, TABLE), jax.random.fold_in(key_of[3], 1), 0, TABLE - 1).astype(jnp.int32)
    layer_norm_gain = jnp.clip(1.0 + 0.1 * jax.random.normal(key_of[4], (C,), jnp.float32), 0.5, 1.5)
    bias_table = draw_bias_table(jax.random.fold_in(key_of[8], 71), 0)
    w_qkv = centred(key_of[6], (3, C, C), C ** -0.5, 0.21875, ((1, 8),))
    w_proj = centred(key_of[7], (C, C), C ** -0.5, 0.21875, ((0, 8),))
    return dict(tokens=tokens, target=target, regions=regions, rel_index=rel_index, layer_norm_gain=layer_norm_gain, bias_table=bias_table, w_qkv=w_qkv, w_proj=w_proj)


def group_sum(left, right, form):

    def step(total, pair):
        term = jnp.einsum(form, pair[0].astype(jnp.float32), pair[1].astype(jnp.float32))
        rounded = lax.optimization_barrier(term.astype(jnp.bfloat16))
        return (total + rounded.astype(jnp.float32), None)
    first = jnp.einsum(form, left[0].astype(jnp.float32), right[0].astype(jnp.float32))
    total, unused = lax.scan(step, jnp.zeros(first.shape, jnp.float32), (left, right))
    return total

def reference(tokens, target, regions, rel_index, layer_norm_gain, bias_table, w_qkv, w_proj):
    f32 = jnp.float32
    brain_float_sixteen = jnp.bfloat16
    group_cols = C // N_MP
    x = tokens.astype(f32)
    mean_value = lax.optimization_barrier(jnp.mean(x, axis=1, keepdims=True))
    centered_input = x - mean_value
    var = lax.optimization_barrier(jnp.mean(centered_input * centered_input, axis=1, keepdims=True))
    inverse_deviation = lax.rsqrt(var + 1e-05)
    normalized_input = centered_input * inverse_deviation
    normed_input = (normalized_input * layer_norm_gain[None, :]).astype(brain_float_sixteen)
    qkv = jnp.einsum('rc,thc->trh', normed_input.astype(f32), w_qkv.astype(f32))
    scale = HD ** (-0.5)
    shape4 = (WINDOWS, WIN_TOK, HEADS, HD)
    query = (qkv[0] * scale).astype(brain_float_sixteen).reshape(shape4)
    keys = qkv[1].astype(brain_float_sixteen).reshape(shape4)
    values = qkv[2].astype(brain_float_sixteen).reshape(shape4)
    onehot = (rel_index.reshape(-1)[:, None] == jnp.arange(TABLE, dtype=jnp.int32)[None, :]).astype(f32)
    relbias = jnp.dot(onehot, bias_table, precision=lax.Precision.HIGHEST).T.reshape(HEADS, WIN_TOK, WIN_TOK)
    maskv = jnp.where(regions[:, :, None] == regions[:, None, :], 0.0, -100.0).astype(f32)
    scores = jnp.einsum('wqhd,wkhd->whqk', query.astype(f32), keys.astype(f32))
    scores = scores + relbias[None] + maskv[:, None]
    top = lax.optimization_barrier(jnp.max(scores, axis=-1, keepdims=True))
    expo = jnp.exp(scores - top)
    probs = expo / lax.optimization_barrier(jnp.sum(expo, axis=-1, keepdims=True))
    pb = probs.astype(brain_float_sixteen)
    attn = jnp.einsum('whqk,wkhd->wqhd', pb.astype(f32), values.astype(f32)).astype(brain_float_sixteen).reshape(TOKENS, C)
    attn_groups = attn.reshape(TOKENS, N_MP, group_cols).transpose(1, 0, 2)
    proj_groups = w_proj.reshape(N_MP, group_cols, C)
    ysum = group_sum(attn_groups, proj_groups, 'rh,hc->rc')
    error_values = x + ysum - target.astype(f32)
    loss = 0.5 * jnp.sum(error_values * error_values) / TOKENS
    gb = error_values.astype(brain_float_sixteen)
    dproj = jnp.dot(attn.T, gb, preferred_element_type=f32)
    dattn = jnp.dot(gb, w_proj.T, preferred_element_type=f32).astype(brain_float_sixteen).reshape(shape4)
    dprob = jnp.einsum('wqhd,wkhd->whqk', dattn.astype(f32), values.astype(f32))
    dvalue = jnp.einsum('whqk,wqhd->wkhd', pb.astype(f32), dattn.astype(f32))
    dscore = probs * (dprob - lax.optimization_barrier(jnp.sum(probs * dprob, axis=-1, keepdims=True)))
    dtable = jnp.dot(lax.optimization_barrier(jnp.sum(dscore, axis=0)).reshape(HEADS, -1), onehot, precision=lax.Precision.HIGHEST).T
    dbf = dscore.astype(brain_float_sixteen).astype(f32)
    dquery = jnp.einsum('whqk,wkhd->wqhd', dbf, keys.astype(f32)) * scale
    dkey = jnp.einsum('whqk,wqhd->wkhd', dbf, query.astype(f32))
    dqkv = jnp.stack([dquery, dkey, dvalue]).astype(brain_float_sixteen).reshape(3, TOKENS, C)
    dwqkv = jnp.einsum('trh,rc->thc', dqkv.astype(f32), normed_input.astype(f32))
    dqkv_groups = dqkv.reshape(3, TOKENS, N_MP, group_cols).transpose(2, 0, 1, 3)
    wqkv_groups = w_qkv.reshape(3, N_MP, group_cols, C).transpose(1, 0, 2, 3)
    normed_output_gradient = group_sum(dqkv_groups, wqkv_groups, 'trh,thc->rc')
    normalized_gradient = normed_output_gradient * layer_norm_gain[None, :]
    gradient_mean_first = lax.optimization_barrier(jnp.mean(normalized_gradient, axis=1, keepdims=True))
    gradient_mean_second = lax.optimization_barrier(jnp.mean(normalized_gradient * normalized_input, axis=1, keepdims=True))
    input_gradient = error_values + inverse_deviation * (normalized_gradient - gradient_mean_first - normalized_input * gradient_mean_second)
    shrink_factor = TOKENS ** (-0.5)
    gain_gradient = lax.optimization_barrier(jnp.sum(normed_output_gradient * normalized_input, axis=0)) * shrink_factor
    return (input_gradient, dwqkv * shrink_factor, dproj * shrink_factor, dtable * shrink_factor, gain_gradient, loss)
```

```python
import jax
import jax.numpy as jnp
from jax import lax
from jax.experimental import pallas as pl
from jax.experimental.pallas import tpu as pltpu
from jax.sharding import Mesh
from jax.sharding import PartitionSpec as P

C = 768
HD = 32
WIN_TOK = 49
TABLE = 169
ENT = 176
F32 = jnp.float32
BF16 = jnp.bfloat16
MESH = pl.DeviceIdType.MESH
VM = pl.BlockSpec(memory_space=pltpu.VMEM)


def dot(a, b, ca, cb):
    return lax.dot_general(a, b, (((ca,), (cb,)), ((), ())), preferred_element_type=F32)


def onehot_rows(relp, p):
    rows = jnp.concatenate([relp[16 * a + p : 16 * a + p + 1, 0:64] for a in range(4)], axis=1)
    entry = lax.broadcasted_iota(jnp.int32, (ENT, 256), 0)
    return jnp.where(entry == rows, 1.0, 0.0).astype(BF16)


def compute_kernel(
    tok_ref, tgt_ref, reg_ref, rel_ref, gain_ref, w_ref, tab_ref,
    gi_ref, gy_ref, gx_ref, gz_ref, sm_ref,
    pad_s, x_s, t_s, xh_s, xn_s, xt_s, xtp_s, gt_s, ysum_s, err_s, gb_s, dxn_s,
    relp_s, bt_s, bias_s, p_s, q_s, k_s, v_s, at_s, dsum_s,
):
    mp = lax.axis_index("x") * 2 + lax.axis_index("core")
    scale = HD**-0.5
    x_s[...] = jnp.zeros_like(x_s)
    t_s[...] = jnp.zeros_like(t_s)
    pad_s[0:147, :] = tok_ref[...].astype(F32)
    for w in range(3):
        x_s[64 * w : 64 * w + 49, :] = pad_s[49 * w : 49 * w + 49, :]
    pad_s[0:147, :] = tgt_ref[...].astype(F32)
    for w in range(3):
        t_s[64 * w : 64 * w + 49, :] = pad_s[49 * w : 49 * w + 49, :]
    x = x_s[...]
    mean = jnp.sum(x, axis=1, keepdims=True) * (1.0 / C)
    cen = x - mean
    var = jnp.sum(cen * cen, axis=1, keepdims=True) * (1.0 / C)
    inv = lax.rsqrt(var + 1e-05)
    xhat = cen * inv
    xh_s[...] = xhat
    xnf = xhat * gain_ref[...]
    xn_s[...] = xnf.astype(BF16)
    xt = jnp.transpose(xn_s[...].astype(F32))
    xt_s[:, 0:192] = xt.astype(BF16)
    pad2 = xtp_s
    pad2[...] = xt
    for y in range(8):
        blk = jnp.concatenate([pad2[96 * z + 12 * y : 96 * z + 12 * y + 12, :] for z in range(8)], axis=0)
        gt_s[96 * y : 96 * y + 96, :] = blk.astype(BF16)

    relp_s[...] = jnp.full(relp_s.shape, -1, jnp.int32)
    relp_s[0:49, 0:49] = rel_ref[...]
    relp = relp_s[...]
    tab = jnp.concatenate([tab_ref[g, 0:3, 0:ENT] for g in range(8)], axis=0)
    hi = tab.astype(BF16)
    rest = tab - hi.astype(F32)
    mid = rest.astype(BF16)
    low = (rest - mid.astype(F32)).astype(BF16)
    zero8 = jnp.zeros((8, ENT), F32)
    parts = jnp.concatenate(
        [t for one in (hi, mid, low) for t in (one.astype(F32), zero8)], axis=0
    ).astype(BF16)
    for p in range(16):
        got = dot(parts, onehot_rows(relp, p), 1, 0)
        got = got[0:24] + got[32:56] + got[64:88]
        bt_s.at[0][pl.ds(p, 24, stride=16), :] = got[:, 0:128]
        bt_s.at[1][pl.ds(p, 24, stride=16), :] = got[:, 128:256]
    keypad = jnp.where(lax.broadcasted_iota(jnp.int32, (64, 384), 0) < WIN_TOK, 0.0, -1e30)
    for i in range(4):
        turned = [jnp.transpose(bt_s[j, 96 * i : 96 * i + 96, :]) for j in range(2)]
        turned = [t[64 * a : 64 * a + 64] for t in turned for a in range(2)]
        bias_s[i] = jnp.concatenate(turned, axis=1) + keypad

    regs = jnp.concatenate(
        [reg_ref[pl.ds(3 * mp + w, 1), :].astype(F32) for w in range(3)] + [jnp.zeros((5, 49), F32)], axis=0
    )
    regs = jnp.concatenate([regs, jnp.zeros((8, 15), F32)], axis=1)
    lane = lax.broadcasted_iota(jnp.int32, (64, 384), 1)
    query_of = (lane // 96) * 16 + lane % 16
    pick = jnp.where(lax.broadcasted_iota(jnp.int32, (64, 384), 0) == query_of, 1.0, 0.0)
    reg_q = dot(regs, pick, 1, 0)
    eye = jnp.where(
        lax.broadcasted_iota(jnp.int32, (64, 64), 0) == lax.broadcasted_iota(jnp.int32, (64, 64), 1), 1.0, 0.0
    )
    reg_k = dot(eye, regs, 1, 1)

    def shift_mask(w):
        return jnp.where(reg_k[:, w : w + 1] == reg_q[w : w + 1, :], 0.0, -100.0)

    row = lax.broadcasted_iota(jnp.int32, (96, 192), 0)
    col = lax.broadcasted_iota(jnp.int32, (96, 192), 1)
    own = jnp.where(row // 16 == col // 32, 1.0, 0.0)
    own_bf = own.astype(BF16)

    def spread(block):
        return jnp.concatenate(
            [jnp.concatenate([block[16 * a : 16 * a + 16]] * 6, axis=0) * own_bf for a in range(4)], axis=0
        )

    def collapse(big):
        out = []
        for a in range(4):
            part = big[96 * a : 96 * a + 96] * own
            out.append(sum(part[16 * h : 16 * h + 16] for h in range(6)))
        return jnp.concatenate(out, axis=0)

    ysum_s[...] = jnp.zeros_like(ysum_s)

    def forward(i, carry):
        xn = xn_s[...]
        wq = w_ref[i, 0].reshape(192, C)
        wk = w_ref[i, 1].reshape(192, C)
        wv = w_ref[i, 2].reshape(192, C)
        q_s[i] = (dot(xn, wq, 1, 1) * scale).astype(BF16)
        k_s[i] = dot(xn, wk, 1, 1).astype(BF16)
        v_s[i] = dot(xn, wv, 1, 1).astype(BF16)
        for w in range(3):
            rows = slice(64 * w, 64 * w + 64)
            sc = dot(k_s[i, rows, :], spread(q_s[i, rows, :]), 1, 1)
            sc = sc + bias_s[i] + shift_mask(w)
            ex = jnp.exp(sc - jnp.max(sc, axis=0, keepdims=True))
            pr = ex / jnp.sum(ex, axis=0, keepdims=True)
            p_s[i, w] = pr
            at_s[i, rows, :] = collapse(dot(pr.astype(BF16), v_s[i, rows, :], 0, 0)).astype(BF16)
        ysum_s[...] += dot(at_s[i], w_ref[i, 3].reshape(192, C), 1, 0)
        return carry

    lax.fori_loop(0, 4, forward, 0)

    rowid = lax.broadcasted_iota(jnp.int32, (192, C), 0) % 64
    err = jnp.where(rowid < WIN_TOK, x_s[...] + ysum_s[...] - t_s[...], 0.0)
    err_s[...] = err
    gb_s[...] = err.astype(BF16)
    xt_s[:, 192:384] = jnp.transpose(gb_s[...].astype(F32)).astype(BF16)
    dxn_s[...] = jnp.zeros_like(dxn_s)

    def backward(i, carry):
        datt = dot(gb_s[...], w_ref[i, 3].reshape(192, C), 1, 1).astype(BF16)
        dqs, dks, dvs = [], [], []
        total = jnp.zeros((64, 384), F32)
        for w in range(3):
            rows = slice(64 * w, 64 * w + 64)
            da = spread(datt[rows])
            dp = dot(v_s[i, rows, :], da, 1, 1)
            pr = p_s[i, w]
            ds = pr * (dp - jnp.sum(pr * dp, axis=0, keepdims=True))
            total = total + ds
            db = ds.astype(BF16)
            dvs.append(dot(pr.astype(BF16), da, 1, 0))
            dks.append(dot(db, spread(q_s[i, rows, :]), 1, 0))
            dqs.append(collapse(dot(db, k_s[i, rows, :], 0, 0)) * scale)
        turned = [jnp.transpose(total[:, 96 * a : 96 * a + 96]) for a in range(4)]
        here = pl.ds(pl.multiple_of(96 * i, 96), 96)
        dsum_s[0, here, :] = jnp.concatenate(turned[0:2], axis=1)
        dsum_s[1, here, :] = jnp.concatenate(turned[2:4], axis=1)
        dq = jnp.concatenate(dqs, axis=0)
        dk = jnp.concatenate(dks, axis=0)
        dv = jnp.concatenate(dvs, axis=0)
        dqb, dkb, dvb = dq.astype(BF16), dk.astype(BF16), dv.astype(BF16)
        dxn_s[...] += (
            dot(dqb, w_ref[i, 0].reshape(192, C), 1, 0)
            + dot(dkb, w_ref[i, 1].reshape(192, C), 1, 0)
            + dot(dvb, w_ref[i, 2].reshape(192, C), 1, 0)
        )
        lead = jnp.concatenate([dqb[:, 0:128], dvb[:, 0:128]], axis=1)
        low_half = jnp.concatenate([dq[:, 128:192], dk], axis=1).astype(BF16)
        zeros = jnp.zeros((192, 64), F32)
        high_half = jnp.concatenate(
            [
                jnp.concatenate([dv[:, 128:192], jnp.zeros((192, 192), F32)], axis=1),
                jnp.concatenate([zeros, at_s[i].astype(F32)], axis=1),
            ],
            axis=0,
        ).astype(BF16)
        for b in range(8):
            rows = slice(96 * b, 96 * b + 96)
            one = dot(gt_s[rows, :], lead, 1, 0).astype(BF16)
            gy_ref[0, b, i] = one[:, 0:128]
            gy_ref[1, b, i] = one[:, 128:256]
            two = dot(xt_s[rows, 0:192], low_half, 1, 0).astype(BF16)
            gx_ref[0, i, b] = two[:, 0:128]
            gz_ref[0, b, i] = two[:, 128:256]
            three = dot(xt_s[rows, :], high_half, 1, 0).astype(BF16)
            gx_ref[1, i, b] = three[:, 0:128]
            gz_ref[1, b, i] = three[:, 128:256]
        return carry

    lax.fori_loop(0, 4, backward, 0)

    dxn = dxn_s[...]
    xhat = xh_s[...]
    dxh = dxn * gain_ref[...]
    m1 = jnp.sum(dxh, axis=1, keepdims=True) * (1.0 / C)
    m2 = jnp.sum(dxh * xhat, axis=1, keepdims=True) * (1.0 / C)
    out = err_s[...] + inv * (dxh - m1 - xhat * m2)
    for w in range(3):
        gi_ref[49 * w : 49 * w + 49, :] = out[64 * w : 64 * w + 49, :]
    gain = jnp.sum(dxn * xhat, axis=0, keepdims=True)
    sq = err_s[...]
    loss = jnp.sum(sq * sq, axis=0, keepdims=True)
    loss = sum(loss[:, 128 * j : 128 * j + 128] for j in range(6))
    loss = jnp.sum(loss, axis=1, keepdims=True) + jnp.zeros((1, 128), F32)
    tail = jnp.concatenate(
        [gain[:, 128 * j : 128 * j + 128] for j in range(6)] + [loss, jnp.zeros((1, 128), F32)], axis=0
    )

    dtab = jnp.zeros((64, ENT), F32)
    for p in range(16):
        ds = jnp.concatenate([dsum_s.at[j][pl.ds(p, 24, stride=16), :] for j in range(2)], axis=1)
        top = ds.astype(BF16)
        rem = (ds - top.astype(F32)).astype(BF16)
        z8 = jnp.zeros((8, 256), F32)
        both = jnp.concatenate([top.astype(F32), z8, rem.astype(F32), z8], axis=0).astype(BF16)
        dtab = dtab + dot(both, onehot_rows(relp, p), 1, 1)
    dtab = dtab[0:24] + dtab[32:56]
    for g in range(8):
        sm_ref[g] = jnp.zeros((8, 384), F32)
        sm_ref[g, 0:3, 0:ENT] = dtab[3 * g : 3 * g + 3]
        sm_ref[g, :, 256:384] = tail


def compute(tokens, target, regions, rel_index, gain, weights, tables):
    f = lambda *s: pltpu.VMEM(s, F32)
    b = lambda *s: pltpu.VMEM(s, BF16)
    return pl.pallas_call(
        compute_kernel,
        name="window_compute",
        out_shape=(
            jax.ShapeDtypeStruct((147, C), F32),
            jax.ShapeDtypeStruct((2, 8, 4, 96, 128), BF16),
            jax.ShapeDtypeStruct((2, 4, 8, 96, 128), BF16),
            jax.ShapeDtypeStruct((2, 8, 4, 96, 128), BF16),
            jax.ShapeDtypeStruct((8, 8, 384), F32),
        ),
        in_specs=[VM] * 7,
        out_specs=(VM,) * 5,
        scratch_shapes=[
            f(152, C), f(192, C), f(192, C), f(192, C), b(192, C), b(C, 384), f(C, 192), b(C, 192),
            f(192, C), f(192, C), b(192, C), f(192, C),
            pltpu.VMEM((64, 128), jnp.int32), f(2, 384, 128), f(4, 64, 384), f(4, 3, 64, 384),
            b(4, 192, 192), b(4, 192, 192), b(4, 192, 192), b(4, 192, 192), f(2, 384, 128),
        ],
        compiler_params=pltpu.CompilerParams(vmem_limit_bytes=60 * 2**20),
    )(tokens, target, regions, rel_index, gain, weights, tables)


def place():
    return lax.axis_index("dp"), lax.axis_index("win"), lax.axis_index("x"), lax.axis_index("core")


def meet(peers):
    barrier = pltpu.get_barrier_semaphore()
    for peer in peers:
        pl.semaphore_signal(barrier, inc=1, device_id=peer, device_id_type=MESH)
    pl.semaphore_wait(barrier, len(peers))


def mp_peers(z, y, x, c):
    far = [(z, y, lax.rem(x + d, 4), core) for d in (1, 2, 3) for core in (c, 1 - c)]
    return [(z, y, x, 1 - c)] + far


def shift(v, d, n):
    return lax.rem(v + (d % n), n)


def gather_kernel(
    wqkv_ref, wproj_ref, tab_ref, w_ref, t_ref,
    send_x, recv_x, send_y, recv_y, send_z, recv_z, send_c, recv_c, send_t, recv_t, own_sem,
):
    z, y, x, c = place()
    color = lax.rem(y + 2 * z, 4)
    partner = (z, y, x, 1 - c)
    mine = 2 * x + c
    talk = mp_peers(z, y, x, c)
    ys = [(z, shift(y, d, 8), x, c) for d in (1, -1)]
    zs = [(shift(z, d, 8), y, x, c) for d in (1, -1)]
    meet(talk + ys + zs)

    started = []

    def push(src, dst, ssem, rsem, to):
        copy = pltpu.make_async_remote_copy(
            src_ref=src, dst_ref=dst, send_sem=ssem, recv_sem=rsem, device_id=to, device_id_type=MESH
        )
        copy.start()
        started.append(copy)

    def landed(dst, rsem):
        pltpu.make_async_remote_copy(
            src_ref=dst, dst_ref=dst, send_sem=rsem, recv_sem=rsem, device_id=partner, device_id_type=MESH
        ).wait_recv()

    for j, d in enumerate((1, -1)):
        to = (z, y, shift(x, d, 4), c)
        for one in range(4):
            src = wqkv_ref.at[one] if one < 3 else wproj_ref

            @pl.when(color == one)
            def _(src=src, one=one, to=to, j=j):
                pltpu.make_async_remote_copy(
                    src_ref=src, dst_ref=w_ref.at[x, one, c], send_sem=send_x.at[j],
                    recv_sem=recv_x.at[j], device_id=to, device_id_type=MESH,
                ).start()

    for j, to in enumerate(talk):
        push(tab_ref, t_ref.at[mine], send_t.at[j], recv_t.at[j], to)
    for one in range(4):
        src = wqkv_ref.at[one] if one < 3 else wproj_ref
        push(src, w_ref.at[x, one, c], send_c.at[one], recv_c.at[one], partner)
    locals_ = []
    for one in range(4):
        src = wqkv_ref.at[one] if one < 3 else wproj_ref
        local = pltpu.make_async_copy(src, w_ref.at[x, one, c], own_sem.at[one])
        local.start()
        locals_.append(local)
    local = pltpu.make_async_copy(tab_ref, t_ref.at[mine], own_sem.at[4])
    local.start()
    locals_.append(local)

    def half(j):
        return pl.ds(48 * j, 48)

    def hand_on(slot, xs):
        piece = w_ref.at[xs, color, c]
        for j in range(2):
            push(piece, piece, send_y.at[slot, j], recv_y.at[slot, j], ys[j])
        for j in range(2):
            part = w_ref.at[xs, color, c, half(j)]
            push(part, part, send_z.at[slot, j], recv_z.at[slot, j], zs[j])
        push(piece, piece, send_c.at[4 + 5 * slot], recv_c.at[4 + 5 * slot], partner)

    sources = [shift(x, -1, 4), shift(x, 1, 4)]
    for slot in range(2):
        piece = w_ref.at[sources[slot], color, c]
        landed(piece, recv_x.at[slot])
        part = w_ref.at[sources[slot], color, c, half(slot)]
        push(part, part, send_x.at[2 + slot], recv_x.at[2 + slot], (z, y, shift(x, 1 - 2 * slot, 4), c))
        hand_on(slot, sources[slot])
    opposite = shift(x, 2, 4)
    for slot in range(2):
        landed(w_ref.at[opposite, color, c, half(slot)], recv_x.at[2 + slot])
    hand_on(2, opposite)

    sources.append(opposite)
    after = lax.rem(color + 1, 4)
    before = lax.rem(color + 3, 4)
    across = lax.rem(color + 2, 4)
    for slot in range(3):
        xs = sources[slot]
        for j, tint in enumerate((before, after)):
            piece = w_ref.at[xs, tint, c]
            landed(piece, recv_y.at[slot, j])
            at = 5 + 5 * slot + j
            push(piece, piece, send_c.at[at], recv_c.at[at], partner)
        for j in range(2):
            part = w_ref.at[xs, across, c, half(j)]
            landed(part, recv_z.at[slot, j])
            at = 7 + 5 * slot + j
            push(part, part, send_c.at[at], recv_c.at[at], partner)

    other = 1 - c
    for one in range(4):
        landed(w_ref.at[x, one, other], recv_c.at[one])
    for slot in range(3):
        xs = sources[slot]
        landed(w_ref.at[xs, color, other], recv_c.at[4 + 5 * slot])
        landed(w_ref.at[xs, before, other], recv_c.at[5 + 5 * slot])
        landed(w_ref.at[xs, after, other], recv_c.at[6 + 5 * slot])
        for j in range(2):
            landed(w_ref.at[xs, across, other, half(j)], recv_c.at[7 + 5 * slot + j])
    landed(t_ref.at[2 * x + other], recv_t.at[0])
    for d in (1, 2, 3):
        from_x = shift(x, -d, 4)
        landed(t_ref.at[2 * from_x + c], recv_t.at[2 * d - 1])
        landed(t_ref.at[2 * from_x + other], recv_t.at[2 * d])
    for copy in started:
        copy.wait_send()
    for j in range(2):
        pltpu.make_async_remote_copy(
            src_ref=wproj_ref, dst_ref=wproj_ref, send_sem=send_x.at[j], recv_sem=recv_x.at[j],
            device_id=partner, device_id_type=MESH,
        ).wait_send()
    for local in locals_:
        local.wait()


def gather(w_qkv, w_proj, table):
    dma = pltpu.SemaphoreType.DMA
    return pl.pallas_call(
        gather_kernel,
        name="gather_weights",
        out_shape=(
            jax.ShapeDtypeStruct((4, 4, 2, 96, C), BF16),
            jax.ShapeDtypeStruct((8, 8, 256), F32),
        ),
        in_specs=[VM] * 3,
        out_specs=(VM, VM),
        scratch_shapes=[
            dma((4,)), dma((4,)), dma((3, 2)), dma((3, 2)), dma((3, 2)), dma((3, 2)),
            dma((19,)), dma((19,)), dma((7,)), dma((7,)), dma((5,)),
        ],
        compiler_params=pltpu.CompilerParams(
            collective_id=0, has_side_effects=True, vmem_limit_bytes=40 * 2**20
        ),
    )(w_qkv, w_proj, table)


def reduce_kernel(
    gy_ref, gx_ref, gz_ref, sm_ref, out_ref, small_ref,
    ry, rx, rz, cy, cx, cz, s2y, s2x, s2z, flat, a3, b3, r3a, r3b, part_s, sm0, sm1, sm2, ss1, ss2,
    send_d, recv_d, send_r, recv_r, send_2, recv_2, send_3, recv_3, send_s, recv_s, send_f, recv_f,
):
    z, y, x, c = place()
    partner = (z, y, x, 1 - c)
    talk = mp_peers(z, y, x, c)
    line_y = [(z, shift(y, d, 8), x, c) for d in range(1, 8)]
    line_z = [(shift(z, d, 8), y, x, c) for d in range(1, 8)]
    line_x = [(z, y, shift(x, d, 4), c) for d in range(1, 4)]
    meet(talk + line_y + line_z)
    started = []

    def push(src, dst, ssem, rsem, to):
        copy = pltpu.make_async_remote_copy(
            src_ref=src, dst_ref=dst, send_sem=ssem, recv_sem=rsem, device_id=to, device_id_type=MESH
        )
        copy.start()
        started.append(copy)

    def landed(dst, rsem):
        pltpu.make_async_remote_copy(
            src_ref=dst, dst_ref=dst, send_sem=rsem, recv_sem=rsem, device_id=partner, device_id_type=MESH
        ).wait_recv()

    parts = (
        (0, gy_ref, ry, cy, y, 8, 4, lambda d: (z, shift(y, d, 8), x, c)),
        (1, gz_ref, rz, cz, z, 8, 4, lambda d: (shift(z, d, 8), y, x, c)),
        (2, gx_ref, rx, cx, x, 4, 8, lambda d: (z, y, shift(x, d, 4), c)),
    )

    def offsets(n):
        half = n // 2
        return [half] + [sign * d for d in range(half - 1, 0, -1) for sign in (1, -1)] + [0]

    for j, peer in enumerate(talk):
        to = 2 * peer[2] + peer[3]
        push(sm_ref.at[to], sm0.at[j], send_s.at[j], recv_s.at[j], peer)

    for k in range(8):
        for num, g, r, ring, me, n, m, reach in parts:
            if k < n:
                block = shift(me, offsets(n)[k], n)
                push(g.at[1 - c, block], r.at[block], send_d.at[num, k], recv_d.at[num, k], partner)

    def take(part, k):
        num, g, r, ring, me, n, m, reach = part
        block = shift(me, offsets(n)[k], n)
        landed(r.at[block], recv_d.at[num, k])
        for s in range(m):
            r[block, s] = r[block, s] + g[c, block, s]
        return block

    def send_chunk(part, block, sign, step, chunk):
        num, g, r, ring, me, n, m, reach = part
        h = m // 2
        way = 0 if sign == 1 else 1
        push(
            r.at[block, pl.ds(chunk * h, h)], ring.at[way, step - 1, chunk],
            send_r.at[num, way, step - 1, chunk], recv_r.at[num, way, step - 1, chunk], reach(sign),
        )

    def add_chunk(part, block, sign, step, chunk):
        num, g, r, ring, me, n, m, reach = part
        h = m // 2
        way = 0 if sign == 1 else 1
        landed(ring.at[way, step - 1, chunk], recv_r.at[num, way, step - 1, chunk])
        for s in range(h):
            r[block, chunk * h + s] = r[block, chunk * h + s] + ring[way, step - 1, chunk, s]

    for part in parts:
        block = take(part, 0)
        send_chunk(part, block, 1, 1, 0)
        send_chunk(part, block, -1, 1, 1)
    blocks = {}
    for k in range(1, 8):
        for part in parts:
            if k < part[5]:
                blocks[part[0], offsets(part[5])[k]] = take(part, k)

    def level(part, step):
        half = part[5] // 2
        for chunk in range(2):
            for sign in (1, -1):
                block = blocks[part[0], sign * (half + 1 - step)]
                if step > 2 or (chunk == 0) == (sign == 1):
                    add_chunk(part, block, sign, step - 1, chunk)
                send_chunk(part, block, sign, step, chunk)

    def finish(part):
        half = part[5] // 2
        for chunk in range(2):
            for sign in (1, -1):
                add_chunk(part, blocks[part[0], 0], sign, half, chunk)

    for part in parts:
        level(part, 2)
    for j in range(7):
        landed(sm0.at[j], recv_s.at[j])
    ss1[...] = sm_ref[2 * x + c] + sum(sm0[j] for j in range(7))
    for j, to in enumerate(line_y):
        push(ss1, sm1.at[j], send_s.at[7 + j], recv_s.at[7 + j], to)
    finish(parts[2])
    for j, d in enumerate(range(1, 8)):
        push(rx.at[x, shift(z, d, 8)], s2x.at[j], send_2.at[j], recv_2.at[j], line_z[j])
    for part in parts[:2]:
        level(part, 3)
    for part in parts[:2]:
        level(part, 4)
    for j in range(7):
        landed(sm1.at[j], recv_s.at[7 + j])
    ss2[...] = ss1[...] + sum(sm1[j] for j in range(7))
    for j, to in enumerate(line_z):
        push(ss2, sm2.at[j], send_s.at[14 + j], recv_s.at[14 + j], to)
    finish(parts[0])
    for j, d in enumerate(range(1, 4)):
        push(ry.at[y, shift(x, d, 4)], s2y.at[j], send_2.at[7 + j], recv_2.at[7 + j], line_x[j])
    finish(parts[1])
    for j, d in enumerate(range(1, 4)):
        push(rz.at[z, shift(x, d, 4)], s2z.at[j], send_2.at[10 + j], recv_2.at[10 + j], line_x[j])

    a3[...] = jnp.zeros_like(a3)
    b3[...] = jnp.zeros_like(b3)
    total = rx[x, z].astype(F32)
    for j in range(7):
        landed(s2x.at[j], recv_2.at[j])
        total = total + s2x[j].astype(F32)
    flat[0] = total
    for i in range(8):
        b3[i, 0, 0:12, :] = flat[0, 12 * i : 12 * i + 12, :]
    total = ry[y, x].astype(F32)
    for j in range(3):
        landed(s2y.at[j], recv_2.at[7 + j])
        total = total + s2y[j].astype(F32)
    flat[1] = total
    for i in range(8):
        a3[i, 0:12, :] = flat[1, 12 * i : 12 * i + 12, :]
    for j, d in enumerate(range(1, 8)):
        push(a3.at[shift(z, d, 8)], r3a.at[j], send_3.at[j], recv_3.at[j], line_z[j])
    total = rz[z, x].astype(F32)
    for j in range(3):
        landed(s2z.at[j], recv_2.at[10 + j])
        total = total + s2z[j].astype(F32)
    flat[2] = total
    for i in range(8):
        b3[i, 1, 0:12, :] = flat[2, 12 * i : 12 * i + 12, :]
    for j, d in enumerate(range(1, 8)):
        push(b3.at[shift(y, d, 8)], r3b.at[j], send_3.at[7 + j], recv_3.at[7 + j], line_y[j])

    total = ss2[...]
    for j in range(7):
        landed(sm2.at[j], recv_s.at[14 + j])
        total = total + sm2[j]
    small_ref[...] = total
    total = a3[z]
    for j in range(7):
        landed(r3a.at[j], recv_3.at[j])
        total = total + r3a[j]
    part_s[:, 0:128] = total
    total = b3[y]
    for j in range(7):
        landed(r3b.at[j], recv_3.at[7 + j])
        total = total + r3b[j]
    part_s[:, 128:256] = total[0]
    part_s[:, 256:384] = total[1]
    out_ref[c] = part_s[...]
    push(part_s, out_ref.at[c], send_f.at[0], recv_f.at[0], partner)
    landed(out_ref.at[1 - c], recv_f.at[0])
    for copy in started:
        copy.wait_send()


def reduce_all(gy, gx, gz, small):
    dma = pltpu.SemaphoreType.DMA
    b = lambda *s: pltpu.VMEM(s, BF16)
    f = lambda *s: pltpu.VMEM(s, F32)
    return pl.pallas_call(
        reduce_kernel,
        name="reduce_gradients",
        out_shape=(
            jax.ShapeDtypeStruct((2, 16, 384), F32),
            jax.ShapeDtypeStruct((8, 384), F32),
        ),
        in_specs=[VM] * 4,
        out_specs=(VM, VM),
        scratch_shapes=[
            b(8, 4, 96, 128), b(4, 8, 96, 128), b(8, 4, 96, 128),
            b(2, 4, 2, 2, 96, 128), b(2, 2, 2, 4, 96, 128), b(2, 4, 2, 2, 96, 128),
            b(3, 96, 128), b(7, 96, 128), b(3, 96, 128), f(3, 96, 128),
            f(8, 16, 128), f(8, 2, 16, 128), f(7, 16, 128), f(7, 2, 16, 128), f(16, 384),
            f(7, 8, 384), f(7, 8, 384), f(7, 8, 384), f(8, 384), f(8, 384),
            dma((3, 8)), dma((3, 8)), dma((3, 2, 4, 2)), dma((3, 2, 4, 2)), dma((13,)), dma((13,)),
            dma((14,)), dma((14,)), dma((21,)), dma((21,)), dma((1,)), dma((1,)),
        ],
        compiler_params=pltpu.CompilerParams(
            collective_id=1, has_side_effects=True, vmem_limit_bytes=40 * 2**20
        ),
    )(gy, gx, gz, small)


def per_device(tokens, target, regions, rel_index, layer_norm_gain, bias_table, w_qkv, w_proj):
    table = jnp.pad(bias_table.T, ((0, 5), (0, 256 - TABLE)))
    weights, tables = gather(w_qkv, w_proj, table)
    gi, gy, gx, gz, small = compute(
        tokens, target, regions, rel_index, layer_norm_gain.reshape(1, C), weights, tables
    )
    out, small = reduce_all(gy, gx, gz, small)
    count = everyone(tokens)
    shrink = count**-0.5
    rows = jnp.concatenate([out[0, 0:12], out[1, 0:12]], axis=1).reshape(12, 4, 2, 96)
    rows = lax.dynamic_index_in_dim(rows, lax.axis_index("core"), 2, keepdims=False)
    rows = jnp.transpose(rows, (1, 2, 0)) * shrink
    return (
        gi,
        rows[0:3],
        rows[3],
        small[0:3, 0:TABLE].T * shrink,
        small[0:6, 256:384].reshape(C) * shrink,
        small[6, 256] * (0.5 / count),
    )


def everyone(tokens):
    return tokens.shape[0] * lax.axis_size(DP_WIN_MP)


MP = ("x", "core")
DP_WIN_MP = ("dp", "win", "x", "core")


def solution(mesh):
    split = Mesh(
        mesh.devices.reshape(mesh.shape["dp"], mesh.shape["win"], 4, 2), ("dp", "win", "x", "core")
    )
    return jax.shard_map(
        per_device,
        mesh=split,
        in_specs=(
            P(DP_WIN_MP, None), P(DP_WIN_MP, None), P(("dp", "win"), None), P(), P(),
            P(None, MP), P(None, MP, None), P(MP, None),
        ),
        out_specs=(
            P(DP_WIN_MP, None), P(None, MP, ("dp", "win")), P(MP, ("dp", "win")), P(None, MP), P(), P(),
        ),
        check_vma=False,
    )
```

```python
import functools

import jax
import jax.numpy as jnp
from jax import lax
from jax.experimental import pallas as pl
from jax.experimental.pallas import tpu as pltpu
from jax.sharding import Mesh
from jax.sharding import PartitionSpec as P

C = 768
HD = 32
WIN_TOK = 49
TABLE = 169
ENT = 176
F32 = jnp.float32
BF16 = jnp.bfloat16
MESH = pl.DeviceIdType.MESH
VM = pl.BlockSpec(memory_space=pltpu.VMEM)


def dot(a, b, ca, cb):
    return lax.dot_general(a, b, (((ca,), (cb,)), ((), ())), preferred_element_type=F32)


def onehot_rows(relp, p):
    rows = jnp.concatenate([relp[16 * a + p : 16 * a + p + 1, 0:64] for a in range(4)], axis=1)
    entry = lax.broadcasted_iota(jnp.int32, (ENT, 256), 0)
    return jnp.where(entry == rows, 1.0, 0.0).astype(BF16)


def compute_kernel(
    tok_ref, tgt_ref, reg_ref, rel_ref, gain_ref, w_ref, tab_ref,
    gi_ref, gy_ref, gx_ref, gz_ref, sm_ref,
    pad_s, x_s, t_s, xh_s, xn_s, xt_s, xtp_s, gt_s, ysum_s, err_s, gb_s, dxn_s,
    relp_s, bt_s, bias_s, p_s, q_s, k_s, v_s, at_s, dsum_s,
):
    mp = lax.axis_index("x") * 2 + lax.axis_index("core")
    scale = HD**-0.5
    x_s[...] = jnp.zeros_like(x_s)
    t_s[...] = jnp.zeros_like(t_s)
    pad_s[0:147, :] = tok_ref[...].astype(F32)
    for w in range(3):
        x_s[64 * w : 64 * w + 49, :] = pad_s[49 * w : 49 * w + 49, :]
    pad_s[0:147, :] = tgt_ref[...].astype(F32)
    for w in range(3):
        t_s[64 * w : 64 * w + 49, :] = pad_s[49 * w : 49 * w + 49, :]
    x = x_s[...]
    mean = jnp.sum(x, axis=1, keepdims=True) * (1.0 / C)
    cen = x - mean
    var = jnp.sum(cen * cen, axis=1, keepdims=True) * (1.0 / C)
    inv = lax.rsqrt(var + 1e-05)
    xhat = cen * inv
    xh_s[...] = xhat
    xnf = xhat * gain_ref[...].reshape(1, C)
    xn_s[...] = xnf.astype(BF16)
    xt = jnp.transpose(xn_s[...].astype(F32))
    xt_s[:, 0:192] = xt.astype(BF16)
    pad2 = xtp_s
    pad2[...] = xt
    for y in range(8):
        blk = jnp.concatenate([pad2[96 * z + 12 * y : 96 * z + 12 * y + 12, :] for z in range(8)], axis=0)
        gt_s[96 * y : 96 * y + 96, :] = blk.astype(BF16)

    relp_s[...] = jnp.full(relp_s.shape, -1, jnp.int32)
    relp_s[0:49, 0:49] = rel_ref[...]
    relp = relp_s[...]
    tab = jnp.concatenate([tab_ref[g, 0:3, 0:ENT] for g in range(8)], axis=0)
    hi = tab.astype(BF16)
    rest = tab - hi.astype(F32)
    mid = rest.astype(BF16)
    low = (rest - mid.astype(F32)).astype(BF16)
    zero8 = jnp.zeros((8, ENT), F32)
    parts = jnp.concatenate(
        [t for one in (hi, mid, low) for t in (one.astype(F32), zero8)], axis=0
    ).astype(BF16)
    for p in range(16):
        got = dot(parts, onehot_rows(relp, p), 1, 0)
        got = got[0:24] + got[32:56] + got[64:88]
        bt_s.at[0][pl.ds(p, 24, stride=16), :] = got[:, 0:128]
        bt_s.at[1][pl.ds(p, 24, stride=16), :] = got[:, 128:256]
    keypad = jnp.where(lax.broadcasted_iota(jnp.int32, (64, 384), 0) < WIN_TOK, 0.0, -1e30)
    for i in range(4):
        turned = [jnp.transpose(bt_s[j, 96 * i : 96 * i + 96, :]) for j in range(2)]
        turned = [t[64 * a : 64 * a + 64] for t in turned for a in range(2)]
        bias_s[i] = jnp.concatenate(turned, axis=1) + keypad

    regs = jnp.concatenate(
        [reg_ref[pl.ds(3 * mp + w, 1), :].astype(F32) for w in range(3)] + [jnp.zeros((5, 49), F32)], axis=0
    )
    regs = jnp.concatenate([regs, jnp.zeros((8, 15), F32)], axis=1)
    lane = lax.broadcasted_iota(jnp.int32, (64, 384), 1)
    query_of = (lane // 96) * 16 + lane % 16
    pick = jnp.where(lax.broadcasted_iota(jnp.int32, (64, 384), 0) == query_of, 1.0, 0.0)
    reg_q = dot(regs, pick, 1, 0)
    eye = jnp.where(
        lax.broadcasted_iota(jnp.int32, (64, 64), 0) == lax.broadcasted_iota(jnp.int32, (64, 64), 1), 1.0, 0.0
    )
    reg_k = dot(eye, regs, 1, 1)

    def shift_mask(w):
        return jnp.where(reg_k[:, w : w + 1] == reg_q[w : w + 1, :], 0.0, -100.0)

    row = lax.broadcasted_iota(jnp.int32, (96, 192), 0)
    col = lax.broadcasted_iota(jnp.int32, (96, 192), 1)
    own = jnp.where(row // 16 == col // 32, 1.0, 0.0)
    own_bf = own.astype(BF16)

    def spread(block):
        return jnp.concatenate(
            [jnp.concatenate([block[16 * a : 16 * a + 16]] * 6, axis=0) * own_bf for a in range(4)], axis=0
        )

    def collapse(big):
        out = []
        for a in range(4):
            part = big[96 * a : 96 * a + 96] * own
            out.append(sum(part[16 * h : 16 * h + 16] for h in range(6)))
        return jnp.concatenate(out, axis=0)

    ysum_s[...] = jnp.zeros_like(ysum_s)

    def forward(i, carry):
        xn = xn_s[...]
        wq = w_ref[i, 0].reshape(192, C)
        wk = w_ref[i, 1].reshape(192, C)
        wv = w_ref[i, 2].reshape(192, C)
        q_s[i] = (dot(xn, wq, 1, 1) * scale).astype(BF16)
        k_s[i] = dot(xn, wk, 1, 1).astype(BF16)
        v_s[i] = dot(xn, wv, 1, 1).astype(BF16)
        for w in range(3):
            rows = slice(64 * w, 64 * w + 64)
            sc = dot(k_s[i, rows, :], spread(q_s[i, rows, :]), 1, 1)
            sc = sc + bias_s[i] + shift_mask(w)
            ex = jnp.exp(sc - jnp.max(sc, axis=0, keepdims=True))
            pr = ex / jnp.sum(ex, axis=0, keepdims=True)
            p_s[i, w] = pr
            at_s[i, rows, :] = collapse(dot(pr.astype(BF16), v_s[i, rows, :], 0, 0)).astype(BF16)
        ysum_s[...] += dot(at_s[i], w_ref[i, 3].reshape(192, C), 1, 0)
        return carry

    lax.fori_loop(0, 4, forward, 0)

    rowid = lax.broadcasted_iota(jnp.int32, (192, C), 0) % 64
    err = jnp.where(rowid < WIN_TOK, x_s[...] + ysum_s[...] - t_s[...], 0.0)
    err_s[...] = err
    gb_s[...] = err.astype(BF16)
    xt_s[:, 192:384] = jnp.transpose(gb_s[...].astype(F32)).astype(BF16)
    dxn_s[...] = jnp.zeros_like(dxn_s)

    def backward(i, carry):
        datt = dot(gb_s[...], w_ref[i, 3].reshape(192, C), 1, 1).astype(BF16)
        dqs, dks, dvs = [], [], []
        total = jnp.zeros((64, 384), F32)
        for w in range(3):
            rows = slice(64 * w, 64 * w + 64)
            da = spread(datt[rows])
            dp = dot(v_s[i, rows, :], da, 1, 1)
            pr = p_s[i, w]
            ds = pr * (dp - jnp.sum(pr * dp, axis=0, keepdims=True))
            total = total + ds
            db = ds.astype(BF16)
            dvs.append(dot(pr.astype(BF16), da, 1, 0))
            dks.append(dot(db, spread(q_s[i, rows, :]), 1, 0))
            dqs.append(collapse(dot(db, k_s[i, rows, :], 0, 0)) * scale)
        turned = [jnp.transpose(total[:, 96 * a : 96 * a + 96]) for a in range(4)]
        here = pl.ds(pl.multiple_of(96 * i, 96), 96)
        dsum_s[0, here, :] = jnp.concatenate(turned[0:2], axis=1)
        dsum_s[1, here, :] = jnp.concatenate(turned[2:4], axis=1)
        dq = jnp.concatenate(dqs, axis=0)
        dk = jnp.concatenate(dks, axis=0)
        dv = jnp.concatenate(dvs, axis=0)
        dqb, dkb, dvb = dq.astype(BF16), dk.astype(BF16), dv.astype(BF16)
        dxn_s[...] += (
            dot(dqb, w_ref[i, 0].reshape(192, C), 1, 0)
            + dot(dkb, w_ref[i, 1].reshape(192, C), 1, 0)
            + dot(dvb, w_ref[i, 2].reshape(192, C), 1, 0)
        )
        lead = jnp.concatenate([dqb[:, 0:128], dvb[:, 0:128]], axis=1)
        low_half = jnp.concatenate([dq[:, 128:192], dk], axis=1).astype(BF16)
        zeros = jnp.zeros((192, 64), F32)
        high_half = jnp.concatenate(
            [
                jnp.concatenate([dv[:, 128:192], jnp.zeros((192, 192), F32)], axis=1),
                jnp.concatenate([zeros, at_s[i].astype(F32)], axis=1),
            ],
            axis=0,
        ).astype(BF16)
        for b in range(8):
            rows = slice(96 * b, 96 * b + 96)
            one = dot(gt_s[rows, :], lead, 1, 0).astype(BF16)
            gy_ref[0, b, i] = one[:, 0:128]
            gy_ref[1, b, i] = one[:, 128:256]
            two = dot(xt_s[rows, 0:192], low_half, 1, 0).astype(BF16)
            gx_ref[0, i, b] = two[:, 0:128]
            gz_ref[0, b, i] = two[:, 128:256]
            three = dot(xt_s[rows, :], high_half, 1, 0).astype(BF16)
            gx_ref[1, i, b] = three[:, 0:128]
            gz_ref[1, b, i] = three[:, 128:256]
        return carry

    lax.fori_loop(0, 4, backward, 0)

    dxn = dxn_s[...]
    xhat = xh_s[...]
    dxh = dxn * gain_ref[...].reshape(1, C)
    m1 = jnp.sum(dxh, axis=1, keepdims=True) * (1.0 / C)
    m2 = jnp.sum(dxh * xhat, axis=1, keepdims=True) * (1.0 / C)
    out = err_s[...] + inv * (dxh - m1 - xhat * m2)
    for w in range(3):
        gi_ref[49 * w : 49 * w + 49, :] = out[64 * w : 64 * w + 49, :]
    gain = jnp.sum(dxn * xhat, axis=0, keepdims=True)
    sq = err_s[...]
    loss = jnp.sum(sq * sq, axis=0, keepdims=True)
    loss = sum(loss[:, 128 * j : 128 * j + 128] for j in range(6))
    loss = jnp.sum(loss, axis=1, keepdims=True) + jnp.zeros((1, 128), F32)
    tail = jnp.concatenate(
        [gain[:, 128 * j : 128 * j + 128] for j in range(6)] + [loss, jnp.zeros((1, 128), F32)], axis=0
    )

    dtab = jnp.zeros((64, ENT), F32)
    for p in range(16):
        ds = jnp.concatenate([dsum_s.at[j][pl.ds(p, 24, stride=16), :] for j in range(2)], axis=1)
        top = ds.astype(BF16)
        rem = (ds - top.astype(F32)).astype(BF16)
        z8 = jnp.zeros((8, 256), F32)
        both = jnp.concatenate([top.astype(F32), z8, rem.astype(F32), z8], axis=0).astype(BF16)
        dtab = dtab + dot(both, onehot_rows(relp, p), 1, 1)
    dtab = dtab[0:24] + dtab[32:56]
    for g in range(8):
        sm_ref[g] = jnp.zeros((8, 384), F32)
        sm_ref[g, 0:3, 0:ENT] = dtab[3 * g : 3 * g + 3]
        sm_ref[g, :, 256:384] = tail


def place():
    return lax.axis_index("dp"), lax.axis_index("win"), lax.axis_index("x"), lax.axis_index("core")


def meet(peers):
    barrier = pltpu.get_barrier_semaphore()
    for peer in peers:
        pl.semaphore_signal(barrier, inc=1, device_id=peer, device_id_type=MESH)
    pl.semaphore_wait(barrier, len(peers))


def mp_peers(z, y, x, c):
    far = [(z, y, lax.rem(x + d, 4), core) for d in (1, 2, 3) for core in (c, 1 - c)]
    return [(z, y, x, 1 - c)] + far


def shift(v, d, n):
    return lax.rem(v + (d % n), n)


def gather_kernel(
    wqkv_ref, wproj_ref, tab_ref, w_ref, t_ref,
    send_x, recv_x, send_y, recv_y, send_z, recv_z, send_c, recv_c, send_t, recv_t, own_sem,
):
    z, y, x, c = place()
    color = lax.rem(y + 2 * z, 4)
    partner = (z, y, x, 1 - c)
    mine = 2 * x + c
    talk = mp_peers(z, y, x, c)
    ys = [(z, shift(y, d, 8), x, c) for d in (1, -1)]
    zs = [(shift(z, d, 8), y, x, c) for d in (1, -1)]

    started = []

    def push(src, dst, ssem, rsem, to):
        copy = pltpu.make_async_remote_copy(
            src_ref=src, dst_ref=dst, send_sem=ssem, recv_sem=rsem, device_id=to, device_id_type=MESH
        )
        copy.start()
        started.append(copy)

    def landed(dst, rsem):
        pltpu.make_async_remote_copy(
            src_ref=dst, dst_ref=dst, send_sem=rsem, recv_sem=rsem, device_id=partner, device_id_type=MESH
        ).wait_recv()

    for j, d in enumerate((1, -1)):
        to = (z, y, shift(x, d, 4), c)
        for one in range(4):
            src = wqkv_ref.at[one] if one < 3 else wproj_ref

            @pl.when(color == one)
            def _(src=src, one=one, to=to, j=j):
                pltpu.make_async_remote_copy(
                    src_ref=src, dst_ref=w_ref.at[x, one, c], send_sem=send_x.at[j],
                    recv_sem=recv_x.at[j], device_id=to, device_id_type=MESH,
                ).start()

    for j, to in enumerate(talk):
        push(tab_ref, t_ref.at[mine], send_t.at[j], recv_t.at[j], to)
    for one in range(4):
        src = wqkv_ref.at[one] if one < 3 else wproj_ref
        push(src, w_ref.at[x, one, c], send_c.at[one], recv_c.at[one], partner)
    locals_ = []
    for one in range(4):
        src = wqkv_ref.at[one] if one < 3 else wproj_ref
        local = pltpu.make_async_copy(src, w_ref.at[x, one, c], own_sem.at[one])
        local.start()
        locals_.append(local)
    local = pltpu.make_async_copy(tab_ref, t_ref.at[mine], own_sem.at[4])
    local.start()
    locals_.append(local)

    def half(j):
        return pl.ds(48 * j, 48)

    def hand_on(slot, xs):
        piece = w_ref.at[xs, color, c]
        for j in range(2):
            push(piece, piece, send_y.at[slot, j], recv_y.at[slot, j], ys[j])
        for j in range(2):
            part = w_ref.at[xs, color, c, half(j)]
            push(part, part, send_z.at[slot, j], recv_z.at[slot, j], zs[j])
        push(piece, piece, send_c.at[4 + 5 * slot], recv_c.at[4 + 5 * slot], partner)

    sources = [shift(x, -1, 4), shift(x, 1, 4)]
    for slot in range(2):
        piece = w_ref.at[sources[slot], color, c]
        landed(piece, recv_x.at[slot])
        part = w_ref.at[sources[slot], color, c, half(slot)]
        push(part, part, send_x.at[2 + slot], recv_x.at[2 + slot], (z, y, shift(x, 1 - 2 * slot, 4), c))
        hand_on(slot, sources[slot])
    opposite = shift(x, 2, 4)
    for slot in range(2):
        landed(w_ref.at[opposite, color, c, half(slot)], recv_x.at[2 + slot])
    hand_on(2, opposite)

    sources.append(opposite)
    after = lax.rem(color + 1, 4)
    before = lax.rem(color + 3, 4)
    across = lax.rem(color + 2, 4)
    for slot in range(3):
        xs = sources[slot]
        for j, tint in enumerate((before, after)):
            piece = w_ref.at[xs, tint, c]
            landed(piece, recv_y.at[slot, j])
            at = 5 + 5 * slot + j
            push(piece, piece, send_c.at[at], recv_c.at[at], partner)
        for j in range(2):
            part = w_ref.at[xs, across, c, half(j)]
            landed(part, recv_z.at[slot, j])
            at = 7 + 5 * slot + j
            push(part, part, send_c.at[at], recv_c.at[at], partner)

    other = 1 - c
    for one in range(4):
        landed(w_ref.at[x, one, other], recv_c.at[one])
    for slot in range(3):
        xs = sources[slot]
        landed(w_ref.at[xs, color, other], recv_c.at[4 + 5 * slot])
        landed(w_ref.at[xs, before, other], recv_c.at[5 + 5 * slot])
        landed(w_ref.at[xs, after, other], recv_c.at[6 + 5 * slot])
        for j in range(2):
            landed(w_ref.at[xs, across, other, half(j)], recv_c.at[7 + 5 * slot + j])
    landed(t_ref.at[2 * x + other], recv_t.at[0])
    for d in (1, 2, 3):
        from_x = shift(x, -d, 4)
        landed(t_ref.at[2 * from_x + c], recv_t.at[2 * d - 1])
        landed(t_ref.at[2 * from_x + other], recv_t.at[2 * d])
    for copy in started:
        copy.wait_send()
    for j in range(2):
        pltpu.make_async_remote_copy(
            src_ref=wproj_ref, dst_ref=wproj_ref, send_sem=send_x.at[j], recv_sem=recv_x.at[j],
            device_id=partner, device_id_type=MESH,
        ).wait_send()
    for local in locals_:
        local.wait()


def reduce_kernel(
    gy_ref, gx_ref, gz_ref, sm_ref, gq_ref, gp_ref, gtab_ref, ggain_ref, loss_ref, count, out_s,
    ry, rx, rz, cy, cx, cz, s2y, s2x, s2z, flat, a3, b3, r3a, r3b, part_s, sm0, sm1, sm2, ss1, ss2,
    send_d, recv_d, send_r, recv_r, send_2, recv_2, send_3, recv_3, send_s, recv_s, send_f, recv_f,
):
    z, y, x, c = place()
    partner = (z, y, x, 1 - c)
    talk = mp_peers(z, y, x, c)
    line_y = [(z, shift(y, d, 8), x, c) for d in range(1, 8)]
    line_z = [(shift(z, d, 8), y, x, c) for d in range(1, 8)]
    line_x = [(z, y, shift(x, d, 4), c) for d in range(1, 4)]
    started = []

    def push(src, dst, ssem, rsem, to):
        copy = pltpu.make_async_remote_copy(
            src_ref=src, dst_ref=dst, send_sem=ssem, recv_sem=rsem, device_id=to, device_id_type=MESH
        )
        copy.start()
        started.append(copy)

    def landed(dst, rsem):
        pltpu.make_async_remote_copy(
            src_ref=dst, dst_ref=dst, send_sem=rsem, recv_sem=rsem, device_id=partner, device_id_type=MESH
        ).wait_recv()

    parts = (
        (0, gy_ref, ry, cy, y, 8, 4, lambda d: (z, shift(y, d, 8), x, c)),
        (1, gz_ref, rz, cz, z, 8, 4, lambda d: (shift(z, d, 8), y, x, c)),
        (2, gx_ref, rx, cx, x, 4, 8, lambda d: (z, y, shift(x, d, 4), c)),
    )

    def offsets(n):
        half = n // 2
        return [half] + [sign * d for d in range(half - 1, 0, -1) for sign in (1, -1)] + [0]

    for j, peer in enumerate(talk):
        to = 2 * peer[2] + peer[3]
        push(sm_ref.at[to], sm0.at[j], send_s.at[j], recv_s.at[j], peer)

    for k in range(8):
        for num, g, r, ring, me, n, m, reach in parts:
            if k < n:
                block = shift(me, offsets(n)[k], n)
                push(g.at[1 - c, block], r.at[block], send_d.at[num, k], recv_d.at[num, k], partner)

    def take(part, k):
        num, g, r, ring, me, n, m, reach = part
        block = shift(me, offsets(n)[k], n)
        landed(r.at[block], recv_d.at[num, k])
        for s in range(m):
            r[block, s] = r[block, s] + g[c, block, s]
        return block

    def send_chunk(part, block, sign, step, chunk):
        num, g, r, ring, me, n, m, reach = part
        h = m // 2
        way = 0 if sign == 1 else 1
        push(
            r.at[block, pl.ds(chunk * h, h)], ring.at[way, step - 1, chunk],
            send_r.at[num, way, step - 1, chunk], recv_r.at[num, way, step - 1, chunk], reach(sign),
        )

    def add_chunk(part, block, sign, step, chunk):
        num, g, r, ring, me, n, m, reach = part
        h = m // 2
        way = 0 if sign == 1 else 1
        landed(ring.at[way, step - 1, chunk], recv_r.at[num, way, step - 1, chunk])
        for s in range(h):
            r[block, chunk * h + s] = r[block, chunk * h + s] + ring[way, step - 1, chunk, s]

    for part in parts:
        block = take(part, 0)
        send_chunk(part, block, 1, 1, 0)
        send_chunk(part, block, -1, 1, 1)
    blocks = {}
    for k in range(1, 8):
        for part in parts:
            if k < part[5]:
                blocks[part[0], offsets(part[5])[k]] = take(part, k)

    def level(part, step):
        half = part[5] // 2
        for chunk in range(2):
            for sign in (1, -1):
                block = blocks[part[0], sign * (half + 1 - step)]
                if step > 2 or (chunk == 0) == (sign == 1):
                    add_chunk(part, block, sign, step - 1, chunk)
                send_chunk(part, block, sign, step, chunk)

    def finish(part):
        half = part[5] // 2
        for chunk in range(2):
            for sign in (1, -1):
                add_chunk(part, blocks[part[0], 0], sign, half, chunk)

    for part in parts:
        level(part, 2)
    for j in range(7):
        landed(sm0.at[j], recv_s.at[j])
    ss1[...] = sm_ref[2 * x + c] + sum(sm0[j] for j in range(7))
    for j, to in enumerate(line_y):
        push(ss1, sm1.at[j], send_s.at[7 + j], recv_s.at[7 + j], to)
    finish(parts[2])
    for j, d in enumerate(range(1, 8)):
        push(rx.at[x, shift(z, d, 8)], s2x.at[j], send_2.at[j], recv_2.at[j], line_z[j])
    for part in parts[:2]:
        level(part, 3)
    for part in parts[:2]:
        level(part, 4)
    for j in range(7):
        landed(sm1.at[j], recv_s.at[7 + j])
    ss2[...] = ss1[...] + sum(sm1[j] for j in range(7))
    for j, to in enumerate(line_z):
        push(ss2, sm2.at[j], send_s.at[14 + j], recv_s.at[14 + j], to)
    finish(parts[0])
    for j, d in enumerate(range(1, 4)):
        push(ry.at[y, shift(x, d, 4)], s2y.at[j], send_2.at[7 + j], recv_2.at[7 + j], line_x[j])
    finish(parts[1])
    for j, d in enumerate(range(1, 4)):
        push(rz.at[z, shift(x, d, 4)], s2z.at[j], send_2.at[10 + j], recv_2.at[10 + j], line_x[j])

    a3[...] = jnp.zeros_like(a3)
    b3[...] = jnp.zeros_like(b3)
    total = rx[x, z].astype(F32)
    for j in range(7):
        landed(s2x.at[j], recv_2.at[j])
        total = total + s2x[j].astype(F32)
    flat[0] = total
    for i in range(8):
        b3[i, 0, 0:12, :] = flat[0, 12 * i : 12 * i + 12, :]
    total = ry[y, x].astype(F32)
    for j in range(3):
        landed(s2y.at[j], recv_2.at[7 + j])
        total = total + s2y[j].astype(F32)
    flat[1] = total
    for i in range(8):
        a3[i, 0:12, :] = flat[1, 12 * i : 12 * i + 12, :]
    for j, d in enumerate(range(1, 8)):
        push(a3.at[shift(z, d, 8)], r3a.at[j], send_3.at[j], recv_3.at[j], line_z[j])
    total = rz[z, x].astype(F32)
    for j in range(3):
        landed(s2z.at[j], recv_2.at[10 + j])
        total = total + s2z[j].astype(F32)
    flat[2] = total
    for i in range(8):
        b3[i, 1, 0:12, :] = flat[2, 12 * i : 12 * i + 12, :]
    for j, d in enumerate(range(1, 8)):
        push(b3.at[shift(y, d, 8)], r3b.at[j], send_3.at[7 + j], recv_3.at[7 + j], line_y[j])

    total = ss2[...]
    for j in range(7):
        landed(sm2.at[j], recv_s.at[14 + j])
        total = total + sm2[j]
    shrink = count**-0.5
    gtab_ref[...] = total[0:3, 0:TABLE] * shrink
    for j in range(6):
        ggain_ref[pl.ds(128 * j, 128)] = total[j : j + 1, 256:384].reshape(128) * shrink
    loss_ref[...] = total[6:7, 256:384] * (0.5 / count)
    total = a3[z]
    for j in range(7):
        landed(r3a.at[j], recv_3.at[j])
        total = total + r3a[j]
    part_s[:, 0:128] = total
    total = b3[y]
    for j in range(7):
        landed(r3b.at[j], recv_3.at[7 + j])
        total = total + r3b[j]
    part_s[:, 128:256] = total[0]
    part_s[:, 256:384] = total[1]
    out_s[c] = part_s[...]
    push(part_s, out_s.at[c], send_f.at[0], recv_f.at[0], partner)
    landed(out_s.at[1 - c], recv_f.at[0])
    for t in range(4):
        at = 192 * (t % 2)
        both = out_s[t // 2, 0:12, :] * shrink
        mine = jnp.where(c == 0, both[:, at : at + 96], both[:, at + 96 : at + 192])
        if t < 3:
            gq_ref[t] = mine
        else:
            gp_ref[...] = mine
    for copy in started:
        copy.wait_send()


def whole_kernel(count, *refs):
    ins, outs, rest = refs[:8], refs[8:14], refs[14:]
    tok, tgt, reg, rel, gain, table, wqkv, wproj = ins
    gi, gq, gp, gtab, ggain, loss = outs
    tab_s, w_s, t_s = rest[:3]
    gather_s, compute_s, reduce_s = rest[3:14], rest[14:39], rest[39:]
    z, y, x, c = place()
    tab_s[...] = jnp.zeros_like(tab_s)
    tab_s[0:3, 0:TABLE] = table[...]
    meet(
        mp_peers(z, y, x, c)
        + [(z, shift(y, d, 8), x, c) for d in range(1, 8)]
        + [(shift(z, d, 8), y, x, c) for d in range(1, 8)]
    )
    gather_kernel(wqkv, wproj, tab_s, w_s, t_s, *gather_s)
    gy, gx, gz, sm = compute_s[:4]
    compute_kernel(tok, tgt, reg, rel, gain, w_s, t_s, gi, gy, gx, gz, sm, *compute_s[4:])
    reduce_kernel(gy, gx, gz, sm, gq, gp, gtab, ggain, loss, count, *reduce_s)


def whole(count, *args):
    dma = pltpu.SemaphoreType.DMA
    f = lambda *s: pltpu.VMEM(s, F32)
    b = lambda *s: pltpu.VMEM(s, BF16)
    shape = jax.ShapeDtypeStruct
    return pl.pallas_call(
        functools.partial(whole_kernel, count),
        name="window_layer",
        out_shape=(
            shape((147, C), F32), shape((3, 12, 96), F32), shape((12, 96), F32),
            shape((3, TABLE), F32), shape((C,), F32), shape((1, 128), F32),
        ),
        in_specs=[VM] * 8,
        out_specs=(VM,) * 6,
        scratch_shapes=[
            f(8, 256), b(4, 4, 2, 96, C), f(8, 8, 256),
            dma((4,)), dma((4,)), dma((3, 2)), dma((3, 2)), dma((3, 2)), dma((3, 2)),
            dma((19,)), dma((19,)), dma((7,)), dma((7,)), dma((5,)),
            b(2, 8, 4, 96, 128), b(2, 4, 8, 96, 128), b(2, 8, 4, 96, 128), f(8, 8, 384),
            f(152, C), f(192, C), f(192, C), f(192, C), b(192, C), b(C, 384), f(C, 192), b(C, 192),
            f(192, C), f(192, C), b(192, C), f(192, C),
            pltpu.VMEM((64, 128), jnp.int32), f(2, 384, 128), f(4, 64, 384), f(4, 3, 64, 384),
            b(4, 192, 192), b(4, 192, 192), b(4, 192, 192), b(4, 192, 192), f(2, 384, 128),
            f(2, 16, 384),
            b(8, 4, 96, 128), b(4, 8, 96, 128), b(8, 4, 96, 128),
            b(2, 4, 2, 2, 96, 128), b(2, 2, 2, 4, 96, 128), b(2, 4, 2, 2, 96, 128),
            b(3, 96, 128), b(7, 96, 128), b(3, 96, 128), f(3, 96, 128),
            f(8, 16, 128), f(8, 2, 16, 128), f(7, 16, 128), f(7, 2, 16, 128), f(16, 384),
            f(7, 8, 384), f(7, 8, 384), f(7, 8, 384), f(8, 384), f(8, 384),
            dma((3, 8)), dma((3, 8)), dma((3, 2, 4, 2)), dma((3, 2, 4, 2)), dma((13,)), dma((13,)),
            dma((14,)), dma((14,)), dma((21,)), dma((21,)), dma((1,)), dma((1,)),
        ],
        compiler_params=pltpu.CompilerParams(
            collective_id=0, has_side_effects=True, vmem_limit_bytes=60 * 2**20
        ),
    )(*args)


MP = ("x", "core")
DP_WIN_MP = ("dp", "win", "x", "core")


def per_device(tokens, target, regions, rel_index, layer_norm_gain, bias_table, w_qkv, w_proj):
    count = tokens.shape[0] * lax.axis_size(DP_WIN_MP)
    gi, gq, gp, gtab, ggain, loss = whole(
        count, tokens, target, regions, rel_index, layer_norm_gain, bias_table.T, w_qkv, w_proj
    )
    return gi, jnp.transpose(gq, (0, 2, 1)), gp.T, gtab.T, ggain, loss[0, 0]


def solution(mesh):
    split = Mesh(
        mesh.devices.reshape(mesh.shape["dp"], mesh.shape["win"], 4, 2), ("dp", "win", "x", "core")
    )
    return jax.shard_map(
        per_device,
        mesh=split,
        in_specs=(
            P(DP_WIN_MP, None), P(DP_WIN_MP, None), P(("dp", "win"), None), P(), P(),
            P(None, MP), P(None, MP, None), P(MP, None),
        ),
        out_specs=(
            P(DP_WIN_MP, None), P(None, MP, ("dp", "win")), P(MP, ("dp", "win")), P(None, MP), P(), P(),
        ),
        check_vma=False,
    )
```

```python
import functools

import jax
import jax.numpy as jnp
from jax import lax
from jax.experimental import pallas as pl
from jax.experimental.pallas import tpu as pltpu
from jax.sharding import Mesh
from jax.sharding import PartitionSpec as P

C = 768
HD = 32
WIN_TOK = 49
TABLE = 169
ENT = 176
F32 = jnp.float32
BF16 = jnp.bfloat16
MESH = pl.DeviceIdType.MESH
VM = pl.BlockSpec(memory_space=pltpu.VMEM)
MP = ("x", "core")
DP_WIN_MP = ("dp", "win", "x", "core")
BIG = (0, C // 2)


def dot(a, b, ca, cb):
    return lax.dot_general(a, b, (((ca,), (cb,)), ((), ())), preferred_element_type=F32)


def onehot_rows(relp, p):
    rows = jnp.concatenate([relp[16 * a + p : 16 * a + p + 1, 0:64] for a in range(4)], axis=1)
    entry = lax.broadcasted_iota(jnp.int32, (ENT, 256), 0)
    return jnp.where(entry == rows, 1.0, 0.0).astype(BF16)


def shift(v, d, n):
    return lax.rem(v + (d % n), n)


def whole_kernel(count, *refs):
    (
        tok_hbm, tgt_hbm, reg_hbm, rel_hbm, gain_hbm, table_hbm, wqkv_hbm, wproj_hbm,
        gi_ref, gq_ref, gp_ref, gtab_ref, ggain_ref, loss_ref,
        tok_ref, tgt_ref, reg_ref, rel_ref, gain_ref, table_ref, tab_s, w_ref, t_ref,
        send_x, recv_x, send_o, recv_o, send_n, recv_n, send_c, recv_c, send_t, recv_t, own_sem,
        pad_s, x_s, t_s, xh_s, xn_s, xt_s, xtf_s, xtp_s, ysum_s, err_s, gb_s, dxn_s,
        relp_s, bt_s, bias_s, p_s, q_s, k_s, v_s, at_s, dsum_s, sm_ref,
        gy_s, gz_s, gx_s, ry, rz, rx, cy, cz, dy, dz, cxf,
        s2y, s2z, s2x, flat, a3, b3, r3a, r3b, part_s, sm0, sm1, sm2, ss1, ss2,
        send_d, recv_d, send_r, recv_r, send_v, recv_v, send_rx, recv_rx,
        send_2, recv_2, send_3, recv_3, send_s, recv_s,
    ) = refs
    z, y, x, c = (lax.axis_index(name) for name in DP_WIN_MP)
    mp = 2 * x + c
    scale = HD**-0.5
    shrink = count**-0.5
    partner = (z, y, x, 1 - c)
    talk = [partner] + [(z, y, shift(x, d, 4), core) for d in (1, 2, 3) for core in (c, 1 - c)]
    line_y = [(z, shift(y, d, 8), x, c) for d in range(1, 8)]
    line_z = [(shift(z, d, 8), y, x, c) for d in range(1, 8)]
    line_x = [(z, y, shift(x, d, 4), c) for d in range(1, 4)]
    started = []

    def push(src, dst, ssem, rsem, to):
        copy = pltpu.make_async_remote_copy(
            src_ref=src, dst_ref=dst, send_sem=ssem, recv_sem=rsem, device_id=to, device_id_type=MESH
        )
        copy.start()
        started.append(copy)

    def landed(dst, rsem):
        pltpu.make_async_remote_copy(
            src_ref=dst, dst_ref=dst, send_sem=rsem, recv_sem=rsem, device_id=partner, device_id_type=MESH
        ).wait_recv()

    barrier = pltpu.get_barrier_semaphore()
    peers = talk + line_y + line_z
    peers += [to[:3] + (1 - c,) for to in line_y + line_z]
    for peer in peers:
        pl.semaphore_signal(barrier, inc=1, device_id=peer, device_id_type=MESH)

    load = [
        pltpu.make_async_copy(src, dst, own_sem.at[k])
        for k, (src, dst) in enumerate(
            (
                (tok_hbm, tok_ref), (wqkv_hbm.at[0], w_ref.at[x, 0, c]), (wqkv_hbm.at[1], w_ref.at[x, 1, c]),
                (wqkv_hbm.at[2], w_ref.at[x, 2, c]), (wproj_hbm, w_ref.at[x, 3, c]), (table_hbm, table_ref),
                (gain_hbm, gain_ref), (tgt_hbm, tgt_ref), (rel_hbm, rel_ref), (reg_hbm, reg_ref),
            )
        )
    ]
    for one in load:
        one.start()
    tab_s[...] = jnp.zeros_like(tab_s)
    load[5].wait()
    tab_s[0:3, 0:TABLE] = table_ref[...]
    t_ref[mp] = tab_s[...]
    load[0].wait()
    load[6].wait()
    load[7].wait()
    x_s[...] = jnp.zeros_like(x_s)
    t_s[...] = jnp.zeros_like(t_s)
    pad_s[0:147, :] = tok_ref[...].astype(F32)
    for w in range(3):
        x_s[64 * w : 64 * w + 49, :] = pad_s[49 * w : 49 * w + 49, :]
    pad_s[0:147, :] = tgt_ref[...].astype(F32)
    for w in range(3):
        t_s[64 * w : 64 * w + 49, :] = pad_s[49 * w : 49 * w + 49, :]
    xx = x_s[...]
    mean = jnp.sum(xx, axis=1, keepdims=True) * (1.0 / C)
    cen = xx - mean
    var = jnp.sum(cen * cen, axis=1, keepdims=True) * (1.0 / C)
    inv = lax.rsqrt(var + 1e-05)
    xh_s[...] = cen * inv
    xn_s[...] = (xh_s[...] * gain_ref[...].reshape(1, C)).astype(BF16)

    pl.semaphore_wait(barrier, len(peers))

    colors = (lax.rem(y + 2 * z, 4), lax.rem(z + 2 * y, 4))
    near_y = [(z, shift(y, d, 8), x, c) for d in (1, -1)]
    near_z = [(shift(z, d, 8), y, x, c) for d in (1, -1)]
    strong = (near_y, near_z)
    weak = (near_z, near_y)

    def rows_of(m):
        return pl.ds(48 * m, 48)

    def piece(xs, tint, core, m):
        return w_ref.at[xs, tint, core, rows_of(m)]

    def lanes(xs, tint, core, m, j):
        return w_ref.at[xs, tint, core, rows_of(m), pl.ds(BIG[j], C // 2)]

    for k in range(1, 5):
        load[k].wait()
    for m in range(2):
        for j, d in enumerate((1, -1)):
            there = piece(x, colors[m], c, m)
            push(there, there, send_x.at[m, j], recv_x.at[m, j], (z, y, shift(x, d, 4), c))
        if m == 0:
            for j, to in enumerate(talk):
                push(tab_s, t_ref.at[mp], send_t.at[j], recv_t.at[j], to)
    for one in range(4):
        there = w_ref.at[x, one, c]
        push(there, there, send_c.at[one], recv_c.at[one], partner)
    load[8].wait()
    load[9].wait()

    xt = jnp.transpose(xn_s[...].astype(F32))
    xt_s[:, 0:192] = xt.astype(BF16)
    xtf_s[...] = xt
    for b in range(8):
        block = jnp.concatenate([xtf_s[96 * k + 12 * b : 96 * k + 12 * b + 12, :] for k in range(8)], axis=0)
        xtp_s[96 * b : 96 * b + 96, :] = block.astype(BF16)
    relp_s[...] = jnp.full(relp_s.shape, -1, jnp.int32)
    relp_s[0:49, 0:49] = rel_ref[...]
    relp = relp_s[...]
    regs = jnp.concatenate(
        [reg_ref[pl.ds(3 * mp + w, 1), :].astype(F32) for w in range(3)] + [jnp.zeros((5, 49), F32)], axis=0
    )
    regs = jnp.concatenate([regs, jnp.zeros((8, 15), F32)], axis=1)
    lane = lax.broadcasted_iota(jnp.int32, (64, 384), 1)
    query_of = (lane // 96) * 16 + lane % 16
    pick = jnp.where(lax.broadcasted_iota(jnp.int32, (64, 384), 0) == query_of, 1.0, 0.0)
    reg_q = dot(regs, pick, 1, 0)
    eye = jnp.where(
        lax.broadcasted_iota(jnp.int32, (64, 64), 0) == lax.broadcasted_iota(jnp.int32, (64, 64), 1), 1.0, 0.0
    )
    reg_k = dot(eye, regs, 1, 1)
    row = lax.broadcasted_iota(jnp.int32, (96, 192), 0)
    col = lax.broadcasted_iota(jnp.int32, (96, 192), 1)
    own = jnp.where(row // 16 == col // 32, 1.0, 0.0)
    own_bf = own.astype(BF16)

    left, right, opposite = shift(x, -1, 4), shift(x, 1, 4), shift(x, 2, 4)
    sources = (left, right, opposite)

    def hand_on(slot, m):
        xs = sources[slot]
        tint = colors[m]
        for j in range(2):
            push(piece(xs, tint, c, m), piece(xs, tint, c, m),
                 send_n.at[slot, m, j], recv_n.at[slot, m, j], strong[m][j])
        for j in range(2):
            push(lanes(xs, tint, c, m, j), lanes(xs, tint, c, m, j),
                 send_n.at[slot, m, 2 + j], recv_n.at[slot, m, 2 + j], weak[m][j])
        push(piece(xs, tint, c, m), piece(xs, tint, c, m),
             send_c.at[4 + 10 * slot + 5 * m], recv_c.at[4 + 10 * slot + 5 * m], partner)

    for m in range(2):
        for slot in range(2):
            landed(piece(sources[slot], colors[m], c, m), recv_x.at[m, slot])
            if slot == m:
                there = piece(sources[slot], colors[m], c, m)
                push(there, there, send_o.at[m], recv_o.at[m], (z, y, shift(x, 1 - 2 * slot, 4), c))
            hand_on(slot, m)

    landed(t_ref.at[2 * x + 1 - c], recv_t.at[0])
    for d in (1, 2, 3):
        landed(t_ref.at[2 * shift(x, -d, 4) + c], recv_t.at[2 * d - 1])
        landed(t_ref.at[2 * shift(x, -d, 4) + 1 - c], recv_t.at[2 * d])
    tab = jnp.concatenate([t_ref[g, 0:3, 0:ENT] for g in range(8)], axis=0)
    hi = tab.astype(BF16)
    rest = tab - hi.astype(F32)
    mid = rest.astype(BF16)
    low = (rest - mid.astype(F32)).astype(BF16)
    zero8 = jnp.zeros((8, ENT), F32)
    parts = jnp.concatenate(
        [t for one in (hi, mid, low) for t in (one.astype(F32), zero8)], axis=0
    ).astype(BF16)
    for p in range(16):
        got = dot(parts, onehot_rows(relp, p), 1, 0)
        got = got[0:24] + got[32:56] + got[64:88]
        bt_s.at[0][pl.ds(p, 24, stride=16), :] = got[:, 0:128]
        bt_s.at[1][pl.ds(p, 24, stride=16), :] = got[:, 128:256]
    keypad = jnp.where(lax.broadcasted_iota(jnp.int32, (64, 384), 0) < WIN_TOK, 0.0, -1e30)
    for i in range(4):
        turned = [jnp.transpose(bt_s[j, 96 * i : 96 * i + 96, :]) for j in range(2)]
        turned = [t[64 * a : 64 * a + 64] for t in turned for a in range(2)]
        bias_s[i] = jnp.concatenate(turned, axis=1) + keypad

    def shift_mask(w):
        return jnp.where(reg_k[:, w : w + 1] == reg_q[w : w + 1, :], 0.0, -100.0)

    def spread(block):
        return jnp.concatenate(
            [jnp.concatenate([block[16 * a : 16 * a + 16]] * 6, axis=0) * own_bf for a in range(4)], axis=0
        )

    def collapse(big):
        out = []
        for a in range(4):
            part = big[96 * a : 96 * a + 96] * own
            out.append(sum(part[16 * h : 16 * h + 16] for h in range(6)))
        return jnp.concatenate(out, axis=0)

    def weight(xs, t):
        return w_ref[xs, t].reshape(192, C)

    def forward(i, xs, first):
        xn = xn_s[...]
        q_s[i] = (dot(xn, weight(xs, 0), 1, 1) * scale).astype(BF16)
        k_s[i] = dot(xn, weight(xs, 1), 1, 1).astype(BF16)
        v_s[i] = dot(xn, weight(xs, 2), 1, 1).astype(BF16)
        for w in range(3):
            rows = slice(64 * w, 64 * w + 64)
            sc = dot(k_s[i, rows, :], spread(q_s[i, rows, :]), 1, 1)
            sc = sc + bias_s[xs] + shift_mask(w)
            ex = jnp.exp(sc - jnp.max(sc, axis=0, keepdims=True))
            pr = ex / jnp.sum(ex, axis=0, keepdims=True)
            p_s[i, w] = pr
            at_s[i, rows, :] = collapse(dot(pr.astype(BF16), v_s[i, rows, :], 0, 0)).astype(BF16)
        part = dot(at_s[i], weight(xs, 3), 1, 0)
        ysum_s[...] = part if first else ysum_s[...] + part

    order = (opposite, right, left, x)

    def near_tints(m):
        return [lax.rem(colors[m] + d, 4) for d in (3, 1)], lax.rem(colors[m] + 2, 4)

    def hand_over(slot):
        xs = sources[slot]
        for m in range(2):
            tints, across = near_tints(m)
            for j in range(2):
                there = piece(xs, tints[j], c, m)
                landed(there, recv_n.at[slot, m, j])
                at = 5 + 10 * slot + 5 * m + j
                push(there, there, send_c.at[at], recv_c.at[at], partner)
            for j in range(2):
                there = lanes(xs, across, c, m, j)
                landed(there, recv_n.at[slot, m, 2 + j])
                at = 7 + 10 * slot + 5 * m + j
                push(there, there, send_c.at[at], recv_c.at[at], partner)

    def whole_slot(slot):
        xs = sources[slot]
        for m in range(2):
            tints, across = near_tints(m)
            at = 4 + 10 * slot + 5 * m
            landed(piece(xs, colors[m], 1 - c, m), recv_c.at[at])
            for j in range(2):
                landed(piece(xs, tints[j], 1 - c, m), recv_c.at[at + 1 + j])
                landed(lanes(xs, across, 1 - c, m, j), recv_c.at[at + 3 + j])

    for m in range(2):
        landed(piece(opposite, colors[m], c, m), recv_o.at[m])
        hand_on(2, m)
    for one in range(4):
        landed(w_ref.at[x, one, 1 - c], recv_c.at[one])
    forward(3, x, True)
    hand_over(0)
    hand_over(1)
    whole_slot(0)
    forward(2, left, False)
    hand_over(2)
    whole_slot(1)
    forward(1, right, False)
    whole_slot(2)
    forward(0, opposite, False)

    rowid = lax.broadcasted_iota(jnp.int32, (192, C), 0) % 64
    err = jnp.where(rowid < WIN_TOK, x_s[...] + ysum_s[...] - t_s[...], 0.0)
    err_s[...] = err
    gb_s[...] = err.astype(BF16)
    xt_s[:, 192:384] = jnp.transpose(err).astype(BF16)

    def backward(i, first):
        xs = order[i]
        datt = dot(gb_s[...], weight(xs, 3), 1, 1).astype(BF16)
        dqs, dks, dvs = [], [], []
        total = jnp.zeros((64, 384), F32)
        for w in range(3):
            rows = slice(64 * w, 64 * w + 64)
            da = spread(datt[rows])
            dp = dot(v_s[i, rows, :], da, 1, 1)
            pr = p_s[i, w]
            ds = pr * (dp - jnp.sum(pr * dp, axis=0, keepdims=True))
            total = total + ds
            db = ds.astype(BF16)
            dvs.append(dot(pr.astype(BF16), da, 1, 0))
            dks.append(dot(db, spread(q_s[i, rows, :]), 1, 0))
            dqs.append(collapse(dot(db, k_s[i, rows, :], 0, 0)) * scale)
        turned = [jnp.transpose(total[:, 96 * a : 96 * a + 96]) for a in range(4)]
        here = pl.ds(pl.multiple_of(96 * xs, 96), 96)
        dsum_s[0, here, :] = jnp.concatenate(turned[0:2], axis=1)
        dsum_s[1, here, :] = jnp.concatenate(turned[2:4], axis=1)
        dq = jnp.concatenate(dqs, axis=0)
        dk = jnp.concatenate(dks, axis=0)
        dv = jnp.concatenate(dvs, axis=0)
        dqb, dkb, dvb = dq.astype(BF16), dk.astype(BF16), dv.astype(BF16)
        lead = jnp.concatenate([dqb[:, 0:128], dvb[:, 0:128]], axis=1)
        low_half = jnp.concatenate([dq[:, 128:192], dk], axis=1).astype(BF16)
        zeros = jnp.zeros((192, 64), F32)
        high_half = jnp.concatenate(
            [
                jnp.concatenate([dv[:, 128:192], jnp.zeros((192, 192), F32)], axis=1),
                jnp.concatenate([zeros, at_s[i].astype(F32)], axis=1),
            ],
            axis=0,
        ).astype(BF16)
        for b in range(8):
            rows = slice(96 * b, 96 * b + 96)
            one = dot(xtp_s[rows, :], lead, 1, 0).astype(BF16)
            gy_s[0, i, b] = one[:, 0:128]
            gy_s[1, i, b] = one[:, 128:256]
            two = dot(xt_s[rows, 0:192], low_half, 1, 0).astype(BF16)
            gx_s[0, i, b] = two[:, 0:128]
            gz_s[0, i, b] = two[:, 128:256]
            three = dot(xt_s[rows, :], high_half, 1, 0).astype(BF16)
            gx_s[1, i, b] = three[:, 0:128]
            gz_s[1, i, b] = three[:, 128:256]
        for num, (g, r) in enumerate(((gy_s, ry), (gz_s, rz), (gx_s, rx))):
            push(g.at[1 - c, i], r.at[i], send_d.at[num, i], recv_d.at[num, i], partner)
        part = (
            dot(dqb, weight(xs, 0), 1, 0) + dot(dkb, weight(xs, 1), 1, 0) + dot(dvb, weight(xs, 2), 1, 0)
        )
        dxn_s[...] = part if first else dxn_s[...] + part

    direct = (dy, dz)
    rings = (
        (0, gy_s, ry, cy, y, lambda d: (z, shift(y, d, 8), x, c)),
        (1, gz_s, rz, cz, z, lambda d: (shift(z, d, 8), y, x, c)),
    )

    def take(i):
        for num, g, r, ring, me, reach in rings:
            landed(r.at[i], recv_d.at[num, i])
            for b in range(8):
                r[i, b] = r[i, b] + g[c, i, b]
            if i < 2:
                far = shift(me, 4, 8)
                for way, sign in enumerate((1, -1)):
                    push(r.at[i, far, rows_of(way)], ring.at[way, 0, i, rows_of(way)],
                         send_r.at[num, way, 0, i], recv_r.at[num, way, 0, i], reach(sign))
            else:
                for d in (4, 3, 5, 2, 6, 1, 7):
                    push(r.at[i, shift(me, d, 8)], direct[num].at[i - 2, d - 1],
                         send_v.at[num, i - 2, d - 1], recv_v.at[num, i - 2, d - 1], reach(d))
        landed(rx.at[i], recv_d.at[2, i])
        for b in range(8):
            rx[i, b] = rx[i, b] + gx_s[c, i, b]
        if i < 3:
            push(rx.at[i], cxf.at[i], send_rx.at[i], recv_rx.at[i], (z, y, order[i], c))

    def step(i, s):
        for num, g, r, ring, me, reach in rings:
            for way, sign in enumerate((1, -1)):
                block = shift(me, sign * (5 - s), 8)
                if s == 2:
                    landed(ring.at[way, 0, i, rows_of(way)], recv_r.at[num, way, 0, i])
                    cut = slice(48 * way, 48 * way + 48)
                    r[i, block, cut, :] = r[i, block, cut, :] + ring[way, 0, i, cut, :]
                else:
                    landed(ring.at[way, s - 2, i], recv_r.at[num, way, s - 2, i])
                    r[i, block] = r[i, block] + ring[way, s - 2, i]
                push(r.at[i, block], ring.at[way, s - 1, i],
                     send_r.at[num, way, s - 1, i], recv_r.at[num, way, s - 1, i], reach(sign))

    def finish(num, i):
        num, g, r, ring, me, reach = rings[num]
        if i < 2:
            for way in range(2):
                landed(ring.at[way, 3, i], recv_r.at[num, way, 3, i])
            total = r[i, me].astype(F32) + ring[0, 3, i].astype(F32) + ring[1, 3, i].astype(F32)
        else:
            total = r[i, me].astype(F32)
            for d in (1, 7, 2, 6, 3, 5, 4):
                landed(direct[num].at[i - 2, d - 1], recv_v.at[num, i - 2, d - 1])
                total = total + direct[num][i - 2, d - 1].astype(F32)
        r[i, me] = total.astype(BF16)
        buf = (s2y, s2z)[num]
        if i < 3:
            to = (z, y, order[i], c)
            push(r.at[i, me], buf.at[i], send_2.at[num, i], recv_2.at[num, i], to)

    backward(0, True)
    backward(1, False)
    take(0)
    backward(2, False)
    take(1)
    step(0, 2)
    backward(3, False)
    take(2)
    step(1, 2)
    step(0, 3)

    dxn = dxn_s[...]
    xhat = xh_s[...]
    dxh = dxn * gain_ref[...].reshape(1, C)
    m1 = jnp.sum(dxh, axis=1, keepdims=True) * (1.0 / C)
    m2 = jnp.sum(dxh * xhat, axis=1, keepdims=True) * (1.0 / C)
    out = err_s[...] + inv * (dxh - m1 - xhat * m2)
    for w in range(3):
        gi_ref[49 * w : 49 * w + 49, :] = out[64 * w : 64 * w + 49, :]
    gain = jnp.sum(dxn * xhat, axis=0, keepdims=True)
    sq = err_s[...]
    loss = jnp.sum(sq * sq, axis=0, keepdims=True)
    loss = sum(loss[:, 128 * j : 128 * j + 128] for j in range(6))
    loss = jnp.sum(loss, axis=1, keepdims=True) + jnp.zeros((1, 128), F32)
    tail = jnp.concatenate(
        [gain[:, 128 * j : 128 * j + 128] for j in range(6)] + [loss, jnp.zeros((1, 128), F32)], axis=0
    )

    take(3)
    step(1, 3)
    step(0, 4)

    dtab = jnp.zeros((64, ENT), F32)
    for p in range(16):
        ds = jnp.concatenate([dsum_s.at[j][pl.ds(p, 24, stride=16), :] for j in range(2)], axis=1)
        top = ds.astype(BF16)
        rem = (ds - top.astype(F32)).astype(BF16)
        z8 = jnp.zeros((8, 256), F32)
        both = jnp.concatenate([top.astype(F32), z8, rem.astype(F32), z8], axis=0).astype(BF16)
        dtab = dtab + dot(both, onehot_rows(relp, p), 1, 1)
    dtab = dtab[0:24] + dtab[32:56]
    for g in range(8):
        sm_ref[g] = jnp.zeros((8, 384), F32)
        sm_ref[g, 0:3, 0:ENT] = dtab[3 * g : 3 * g + 3]
        sm_ref[g, :, 256:384] = tail
    for j, peer in enumerate(talk):
        push(sm_ref.at[2 * peer[2] + peer[3]], sm0.at[j], send_s.at[j], recv_s.at[j], peer)

    for b in range(8):
        total = rx[3, b].astype(F32)
        for i in range(3):
            if b == 0:
                landed(cxf.at[i], recv_rx.at[i])
            total = total + cxf[i, b].astype(F32)
        rx[3, b] = total.astype(BF16)
    for d in (4, 3, 5, 2, 6, 1, 7):
        push(rx.at[3, shift(z, d, 8)], s2x.at[d - 1], send_2.at[2, d - 1], recv_2.at[2, d - 1], line_z[d - 1])
    step(1, 4)
    finish(0, 0)
    finish(1, 0)
    for j in range(7):
        landed(sm0.at[j], recv_s.at[j])
    ss1[...] = sm_ref[mp] + sum(sm0[j] for j in range(7))
    for j, to in enumerate(line_y):
        push(ss1, sm1.at[j], send_s.at[7 + j], recv_s.at[7 + j], to)
    finish(0, 1)
    finish(1, 1)
    finish(0, 2)
    finish(1, 2)
    finish(0, 3)
    finish(1, 3)
    for j in range(7):
        landed(sm1.at[j], recv_s.at[7 + j])
    ss2[...] = ss1[...] + sum(sm1[j] for j in range(7))
    for j, to in enumerate(line_z):
        push(ss2, sm2.at[j], send_s.at[14 + j], recv_s.at[14 + j], to)

    a3[...] = jnp.zeros_like(a3)
    b3[...] = jnp.zeros_like(b3)

    def collect(num, r, me, buf):
        total = r[3, me].astype(F32)
        for i in range(3):
            landed(buf.at[i], recv_2.at[num, i])
            total = total + buf[i].astype(F32)
        flat[num] = total

    def spread_out(src, me, dst, num, reach):
        for d in (4, 3, 5, 2, 6, 1, 7, 0):
            for k, core in enumerate((c, 1 - c)):
                if d or k:
                    push(src.at[shift(me, d, 8)], dst.at[k, d], send_3.at[num, k, d], recv_3.at[num, k, d],
                         reach(d, core))

    def gathered(src, me, dst, num, k):
        total = src[me] if k == 0 else 0.0
        for d in (0, 1, 7, 2, 6, 3, 5, 4):
            if d or k:
                landed(dst.at[k, d], recv_3.at[num, k, d])
                total = total + dst[k, d]
        return total

    collect(0, ry, y, s2y)
    for i in range(8):
        a3[i, 0:12, :] = flat[0, 12 * i : 12 * i + 12, :]
    spread_out(a3, z, r3a, 0, lambda d, core: (shift(z, d, 8), y, x, core))
    collect(1, rz, z, s2z)
    for i in range(8):
        b3[i, 1, 0:12, :] = flat[1, 12 * i : 12 * i + 12, :]
    total = rx[3, z].astype(F32)
    for j in range(7):
        landed(s2x.at[j], recv_2.at[2, j])
        total = total + s2x[j].astype(F32)
    flat[2] = total
    for i in range(8):
        b3[i, 0, 0:12, :] = flat[2, 12 * i : 12 * i + 12, :]
    spread_out(b3, y, r3b, 1, lambda d, core: (z, shift(y, d, 8), x, core))

    total = ss2[...]
    for j in range(7):
        landed(sm2.at[j], recv_s.at[14 + j])
        total = total + sm2[j]
    gtab_ref[...] = total[0:3, 0:TABLE] * shrink
    for j in range(6):
        ggain_ref[pl.ds(128 * j, 128)] = total[j : j + 1, 256:384].reshape(128) * shrink
    loss_ref[...] = total[6:7, 256:384] * (0.5 / count)
    for k, core in enumerate((c, 1 - c)):
        part_s[core, :, 0:128] = gathered(a3, z, r3a, 0, k)
    for k, core in enumerate((c, 1 - c)):
        total = gathered(b3, y, r3b, 1, k)
        part_s[core, :, 128:256] = total[0]
        part_s[core, :, 256:384] = total[1]
    for t in range(4):
        at = 192 * (t % 2)
        both = part_s[t // 2, 0:12, :] * shrink
        mine = jnp.where(c == 0, both[:, at : at + 96], both[:, at + 96 : at + 192])
        if t < 3:
            gq_ref[t] = mine
        else:
            gp_ref[...] = mine
    for copy in started:
        copy.wait_send()


def whole(count, *args):
    dma = pltpu.SemaphoreType.DMA
    f = lambda *s: pltpu.VMEM(s, F32)
    b = lambda *s: pltpu.VMEM(s, BF16)
    shape = jax.ShapeDtypeStruct
    return pl.pallas_call(
        functools.partial(whole_kernel, count),
        name="window_layer",
        out_shape=(
            shape((147, C), F32), shape((3, 12, 96), F32), shape((12, 96), F32),
            shape((3, TABLE), F32), shape((C,), F32), shape((1, 128), F32),
        ),
        in_specs=[pl.BlockSpec(memory_space=pltpu.HBM)] * 8,
        out_specs=(VM,) * 6,
        scratch_shapes=[
            b(147, C), b(147, C), pltpu.VMEM((24, 49), jnp.int32), pltpu.VMEM((49, 49), jnp.int32), f(C), f(3, TABLE),
            f(8, 256), b(4, 4, 2, 96, C), f(8, 8, 256),
            dma((2, 2)), dma((2, 2)), dma((2,)), dma((2,)), dma((3, 2, 4)), dma((3, 2, 4)),
            dma((34,)), dma((34,)), dma((7,)), dma((7,)), dma((10,)),
            f(152, C), f(192, C), f(192, C), f(192, C), b(192, C), b(C, 384), f(C, 192), b(C, 192),
            f(192, C), f(192, C), b(192, C), f(192, C),
            pltpu.VMEM((64, 128), jnp.int32), f(2, 384, 128), f(4, 64, 384), f(4, 3, 64, 384),
            b(4, 192, 192), b(4, 192, 192), b(4, 192, 192), b(4, 192, 192), f(2, 384, 128), f(8, 8, 384),
            b(2, 4, 8, 96, 128), b(2, 4, 8, 96, 128), b(2, 4, 8, 96, 128),
            b(4, 8, 96, 128), b(4, 8, 96, 128), b(4, 8, 96, 128),
            b(2, 4, 2, 96, 128), b(2, 4, 2, 96, 128), b(2, 7, 96, 128), b(2, 7, 96, 128), b(3, 8, 96, 128),
            b(3, 96, 128), b(3, 96, 128), b(7, 96, 128), f(3, 96, 128),
            f(8, 16, 128), f(8, 2, 16, 128), f(2, 8, 16, 128), f(2, 8, 2, 16, 128), f(2, 16, 384),
            f(7, 8, 384), f(7, 8, 384), f(7, 8, 384), f(8, 384), f(8, 384),
            dma((3, 4)), dma((3, 4)), dma((2, 2, 4, 2)), dma((2, 2, 4, 2)), dma((2, 2, 7)), dma((2, 2, 7)), dma((3,)), dma((3,)),
            dma((3, 7)), dma((3, 7)), dma((2, 2, 8)), dma((2, 2, 8)), dma((21,)), dma((21,)),
        ],
        compiler_params=pltpu.CompilerParams(
            collective_id=0, has_side_effects=True, vmem_limit_bytes=40 * 2**20
        ),
    )(*args)


def hand_out_kernel(*refs):
    copies = [pltpu.make_async_copy(refs[k], refs[6 + k], refs[12].at[k]) for k in range(6)]
    for copy in copies:
        copy.start()
    for copy in copies:
        copy.wait()


def hand_out(*arrays):
    return pl.pallas_call(
        hand_out_kernel,
        name="hand_out",
        out_shape=tuple(jax.ShapeDtypeStruct(a.shape, a.dtype) for a in arrays),
        in_specs=[VM] * 6,
        out_specs=(pl.BlockSpec(memory_space=pl.ANY),) * 6,
        scratch_shapes=[pltpu.SemaphoreType.DMA((6,))],
        compiler_params=pltpu.CompilerParams(vmem_limit_bytes=8 * 2**20),
    )(*arrays)


def per_device(tokens, target, regions, rel_index, layer_norm_gain, bias_table, w_qkv, w_proj):
    count = tokens.shape[0] * lax.axis_size(DP_WIN_MP)
    args = (tokens, target, regions, rel_index, layer_norm_gain, bias_table.T, w_qkv, w_proj)
    done = whole(count, *[pltpu.with_memory_space_constraint(one, pltpu.HBM) for one in args])
    gi, gq, gp, gtab, ggain, loss = hand_out(*done)
    return gi, jnp.transpose(gq, (0, 2, 1)), gp.T, gtab.T, ggain, loss[0, 0]


def solution(mesh):
    split = Mesh(mesh.devices.reshape(mesh.shape["dp"], mesh.shape["win"], 4, 2), DP_WIN_MP)
    return jax.shard_map(
        per_device,
        mesh=split,
        in_specs=(
            P(DP_WIN_MP, None), P(DP_WIN_MP, None), P(("dp", "win"), None), P(), P(),
            P(None, MP), P(None, MP, None), P(MP, None),
        ),
        out_specs=(
            P(DP_WIN_MP, None), P(None, MP, ("dp", "win")), P(MP, ("dp", "win")), P(None, MP), P(), P(),
        ),
        check_vma=False,
    )
```

```python
import functools

import jax
import jax.numpy as jnp
from jax import lax
from jax.experimental import pallas as pl
from jax.experimental.pallas import tpu as pltpu
from jax.sharding import Mesh
from jax.sharding import PartitionSpec as P

C = 768
HD = 32
WIN_TOK = 49
TABLE = 169
ENT = 176
F32 = jnp.float32
BF16 = jnp.bfloat16
MESH = pl.DeviceIdType.MESH
VM = pl.BlockSpec(memory_space=pltpu.VMEM)
MP = ("x", "core")
DP_WIN_MP = ("dp", "win", "x", "core")
BIG = (0, C // 2)


def dot(a, b, ca, cb):
    return lax.dot_general(a, b, (((ca,), (cb,)), ((), ())), preferred_element_type=F32)


def onehot_rows(relp, p):
    rows = jnp.concatenate([relp[16 * a + p : 16 * a + p + 1, 0:64] for a in range(4)], axis=1)
    entry = lax.broadcasted_iota(jnp.int32, (ENT, 256), 0)
    return jnp.where(entry == rows, 1.0, 0.0).astype(BF16)


def shift(v, d, n):
    return lax.rem(v + (d % n), n)


def whole_kernel(count, *refs):
    (
        tok_hbm, tgt_hbm, reg_hbm, rel_hbm, gain_hbm, table_hbm, wqkv_hbm, wproj_hbm,
        gi_ref, gq_ref, gp_ref, gtab_ref, ggain_ref, loss_ref,
        tok_ref, tgt_ref, reg_ref, rel_ref, gain_ref, table_ref, tab_s, w_ref, t_ref,
        send_w, recv_x, recv_o, recv_n, send_c, recv_c, send_t, recv_t, own_sem,
        pad_s, x_s, t_s, xh_s, xn_s, xt_s, xtf_s, xtp_s, ysum_s, err_s, gb_s, dxn_s,
        relp_s, bt_s, bias_s, p_s, q_s, k_s, v_s, at_s, dsum_s, sm_ref,
        grads, sums, ring, direct, cxf, s2, s2x, flat, a3, b3, r3a, r3b, part_s, sm0, sm1, sm2, ss1, ss2,
        send_d, recv_d, send_v, recv_r, recv_v, send_rx, recv_rx,
        send_2, recv_2, send_3, recv_3, send_s, recv_s,
    ) = refs
    z, y, x, c = (lax.axis_index(name) for name in DP_WIN_MP)
    mp = 2 * x + c
    scale = HD**-0.5
    shrink = count**-0.5
    partner = (z, y, x, 1 - c)
    talk = [partner] + [(z, y, shift(x, d, 4), core) for d in (1, 2, 3) for core in (c, 1 - c)]
    line_y = [(z, shift(y, d, 8), x, c) for d in range(1, 8)]
    line_z = [(shift(z, d, 8), y, x, c) for d in range(1, 8)]
    line_x = [(z, y, shift(x, d, 4), c) for d in range(1, 4)]
    def push(src, dst, ssem, rsem, to):
        pltpu.make_async_remote_copy(
            src_ref=src, dst_ref=dst, send_sem=ssem, recv_sem=rsem, device_id=to, device_id_type=MESH
        ).start()

    def landed(dst, rsem):
        pltpu.make_async_remote_copy(
            src_ref=dst, dst_ref=dst, send_sem=rsem, recv_sem=rsem, device_id=partner, device_id_type=MESH
        ).wait_recv()

    def left_here(amount, ssem):
        pltpu.make_async_remote_copy(
            src_ref=amount, dst_ref=amount, send_sem=ssem, recv_sem=ssem, device_id=partner, device_id_type=MESH
        ).wait_send()

    barrier = pltpu.get_barrier_semaphore()
    peers = talk + line_y + line_z
    peers += [to[:3] + (1 - c,) for to in line_y + line_z]
    for peer in peers:
        pl.semaphore_signal(barrier, inc=1, device_id=peer, device_id_type=MESH)

    load = [
        pltpu.make_async_copy(src, dst, own_sem.at[k])
        for k, (src, dst) in enumerate(
            (
                (tok_hbm, tok_ref), (wqkv_hbm.at[0], w_ref.at[x, 0, c]), (wqkv_hbm.at[1], w_ref.at[x, 1, c]),
                (wqkv_hbm.at[2], w_ref.at[x, 2, c]), (wproj_hbm, w_ref.at[x, 3, c]), (table_hbm, table_ref),
                (gain_hbm, gain_ref), (tgt_hbm, tgt_ref), (rel_hbm, rel_ref), (reg_hbm, reg_ref),
            )
        )
    ]
    for one in load:
        one.start()
    tab_s[...] = jnp.zeros_like(tab_s)
    load[5].wait()
    tab_s[0:3, 0:TABLE] = table_ref[...]
    t_ref[mp] = tab_s[...]
    load[0].wait()
    load[6].wait()
    load[7].wait()
    x_s[...] = jnp.zeros_like(x_s)
    t_s[...] = jnp.zeros_like(t_s)
    pad_s[0:147, :] = tok_ref[...].astype(F32)
    for w in range(3):
        x_s[64 * w : 64 * w + 49, :] = pad_s[49 * w : 49 * w + 49, :]
    pad_s[0:147, :] = tgt_ref[...].astype(F32)
    for w in range(3):
        t_s[64 * w : 64 * w + 49, :] = pad_s[49 * w : 49 * w + 49, :]
    xx = x_s[...]
    mean = jnp.sum(xx, axis=1, keepdims=True) * (1.0 / C)
    cen = xx - mean
    var = jnp.sum(cen * cen, axis=1, keepdims=True) * (1.0 / C)
    inv = lax.rsqrt(var + 1e-05)
    xh_s[...] = cen * inv
    xn_s[...] = (xh_s[...] * gain_ref[...].reshape(1, C)).astype(BF16)

    pl.semaphore_wait(barrier, len(peers))

    colors = (lax.rem(y + 2 * z, 4), lax.rem(z + 2 * y, 4))
    near_y = [(z, shift(y, d, 8), x, c) for d in (1, -1)]
    near_z = [(shift(z, d, 8), y, x, c) for d in (1, -1)]
    strong = (near_y, near_z)
    weak = (near_z, near_y)

    def rows_of(m):
        return pl.ds(48 * m, 48)

    def piece(xs, tint, core, m):
        return w_ref.at[xs, tint, core, rows_of(m)]

    def lanes(xs, tint, core, m, j):
        return w_ref.at[xs, tint, core, rows_of(m), pl.ds(BIG[j], C // 2)]

    for k in range(1, 5):
        load[k].wait()
    for m in range(2):
        for j, d in enumerate((1, -1)):
            there = piece(x, colors[m], c, m)
            push(there, there, send_w.at[0], recv_x.at[m], (z, y, shift(x, d, 4), c))
        if m == 0:
            for to in talk:
                push(tab_s, t_ref.at[mp], send_t.at[0], recv_t.at[0], to)
    for one in range(4):
        there = w_ref.at[x, one, c]
        push(there, there, send_c.at[0], recv_c.at[3], partner)
    load[8].wait()
    load[9].wait()

    xt = jnp.transpose(xn_s[...].astype(F32))
    xt_s[:, 0:192] = xt.astype(BF16)
    xtf_s[...] = xt
    for b in range(8):
        block = jnp.concatenate([xtf_s[96 * k + 12 * b : 96 * k + 12 * b + 12, :] for k in range(8)], axis=0)
        xtp_s[96 * b : 96 * b + 96, :] = block.astype(BF16)
    relp_s[...] = jnp.full(relp_s.shape, -1, jnp.int32)
    relp_s[0:49, 0:49] = rel_ref[...]
    relp = relp_s[...]
    regs = jnp.concatenate(
        [reg_ref[pl.ds(3 * mp + w, 1), :].astype(F32) for w in range(3)] + [jnp.zeros((5, 49), F32)], axis=0
    )
    regs = jnp.concatenate([regs, jnp.zeros((8, 15), F32)], axis=1)
    lane = lax.broadcasted_iota(jnp.int32, (64, 384), 1)
    query_of = (lane // 96) * 16 + lane % 16
    pick = jnp.where(lax.broadcasted_iota(jnp.int32, (64, 384), 0) == query_of, 1.0, 0.0)
    reg_q = dot(regs, pick, 1, 0)
    eye = jnp.where(
        lax.broadcasted_iota(jnp.int32, (64, 64), 0) == lax.broadcasted_iota(jnp.int32, (64, 64), 1), 1.0, 0.0
    )
    reg_k = dot(eye, regs, 1, 1)
    row = lax.broadcasted_iota(jnp.int32, (96, 192), 0)
    col = lax.broadcasted_iota(jnp.int32, (96, 192), 1)
    own = jnp.where(row // 16 == col // 32, 1.0, 0.0)
    own_bf = own.astype(BF16)

    left, right, opposite = shift(x, -1, 4), shift(x, 1, 4), shift(x, 2, 4)
    sources = (left, right, opposite)

    def hand_on(slot, m):
        xs = sources[slot]
        tint = colors[m]
        for j in range(2):
            push(piece(xs, tint, c, m), piece(xs, tint, c, m), send_w.at[0], recv_n.at[slot], strong[m][j])
        for j in range(2):
            push(lanes(xs, tint, c, m, j), lanes(xs, tint, c, m, j), send_w.at[0], recv_n.at[slot], weak[m][j])
        push(piece(xs, tint, c, m), piece(xs, tint, c, m), send_c.at[0], recv_c.at[slot], partner)

    def from_sides(m):
        landed(w_ref.at[left, 0, c], recv_x.at[m])
        there = piece(sources[m], colors[m], c, m)
        push(there, there, send_w.at[0], recv_o.at[m], (z, y, shift(x, 1 - 2 * m, 4), c))
        for slot in range(2):
            hand_on(slot, m)

    from_sides(0)

    landed(t_ref.at[pl.ds(0, 7)], recv_t.at[0])
    tab = jnp.concatenate([t_ref[g, 0:3, 0:ENT] for g in range(8)], axis=0)
    hi = tab.astype(BF16)
    rest = tab - hi.astype(F32)
    mid = rest.astype(BF16)
    low = (rest - mid.astype(F32)).astype(BF16)
    zero8 = jnp.zeros((8, ENT), F32)
    parts = jnp.concatenate(
        [t for one in (hi, mid, low) for t in (one.astype(F32), zero8)], axis=0
    ).astype(BF16)
    for p in range(16):
        got = dot(parts, onehot_rows(relp, p), 1, 0)
        got = got[0:24] + got[32:56] + got[64:88]
        bt_s.at[0][pl.ds(p, 24, stride=16), :] = got[:, 0:128]
        bt_s.at[1][pl.ds(p, 24, stride=16), :] = got[:, 128:256]
    keypad = jnp.where(lax.broadcasted_iota(jnp.int32, (64, 384), 0) < WIN_TOK, 0.0, -1e30)
    for i in range(4):
        turned = [jnp.transpose(bt_s[j, 96 * i : 96 * i + 96, :]) for j in range(2)]
        turned = [t[64 * a : 64 * a + 64] for t in turned for a in range(2)]
        bias_s[i] = jnp.concatenate(turned, axis=1) + keypad

    def shift_mask(w):
        return jnp.where(reg_k[:, w : w + 1] == reg_q[w : w + 1, :], 0.0, -100.0)

    def spread(block):
        return jnp.concatenate(
            [jnp.concatenate([block[16 * a : 16 * a + 16]] * 6, axis=0) * own_bf for a in range(4)], axis=0
        )

    def collapse(big):
        out = []
        for a in range(4):
            part = big[96 * a : 96 * a + 96] * own
            out.append(sum(part[16 * h : 16 * h + 16] for h in range(6)))
        return jnp.concatenate(out, axis=0)

    def weight(xs, t):
        return w_ref[xs, t].reshape(192, C)

    def forward(i, xs, first):
        xn = xn_s[...]
        q_s[i] = (dot(xn, weight(xs, 0), 1, 1) * scale).astype(BF16)
        k_s[i] = dot(xn, weight(xs, 1), 1, 1).astype(BF16)
        v_s[i] = dot(xn, weight(xs, 2), 1, 1).astype(BF16)
        for w in range(3):
            rows = slice(64 * w, 64 * w + 64)
            sc = dot(k_s[i, rows, :], spread(q_s[i, rows, :]), 1, 1)
            sc = sc + bias_s[xs] + shift_mask(w)
            ex = jnp.exp(sc - jnp.max(sc, axis=0, keepdims=True))
            pr = ex / jnp.sum(ex, axis=0, keepdims=True)
            p_s[i, w] = pr
            at_s[i, rows, :] = collapse(dot(pr.astype(BF16), v_s[i, rows, :], 0, 0)).astype(BF16)
        part = dot(at_s[i], weight(xs, 3), 1, 0)
        ysum_s[...] = part if first else ysum_s[...] + part

    order = (opposite, right, left, x)

    def near_tints(m):
        return [lax.rem(colors[m] + d, 4) for d in (3, 1)], lax.rem(colors[m] + 2, 4)

    def hand_over(slot):
        xs = sources[slot]
        landed(w_ref.at[xs, pl.ds(0, 3), c], recv_n.at[slot])
        for m in range(2):
            tints, across = near_tints(m)
            for j in range(2):
                there = piece(xs, tints[j], c, m)
                push(there, there, send_c.at[0], recv_c.at[slot], partner)
            for j in range(2):
                there = lanes(xs, across, c, m, j)
                push(there, there, send_c.at[0], recv_c.at[slot], partner)

    def whole_slot(slot):
        landed(w_ref.at[sources[slot], :, 1 - c], recv_c.at[slot])

    landed(w_ref.at[x, :, 1 - c], recv_c.at[3])
    forward(3, x, True)
    from_sides(1)
    for m in range(2):
        landed(piece(opposite, colors[m], c, m), recv_o.at[m])
        hand_on(2, m)
    hand_over(0)
    hand_over(1)
    whole_slot(0)
    forward(2, left, False)
    hand_over(2)
    whole_slot(1)
    forward(1, right, False)
    whole_slot(2)
    forward(0, opposite, False)

    rowid = lax.broadcasted_iota(jnp.int32, (192, C), 0) % 64
    err = jnp.where(rowid < WIN_TOK, x_s[...] + ysum_s[...] - t_s[...], 0.0)
    err_s[...] = err
    gb_s[...] = err.astype(BF16)
    xt_s[:, 192:384] = jnp.transpose(err).astype(BF16)

    def backward(i, first):
        xs = order[i]
        datt = dot(gb_s[...], weight(xs, 3), 1, 1).astype(BF16)
        dqs, dks, dvs = [], [], []
        total = jnp.zeros((64, 384), F32)
        for w in range(3):
            rows = slice(64 * w, 64 * w + 64)
            da = spread(datt[rows])
            dp = dot(v_s[i, rows, :], da, 1, 1)
            pr = p_s[i, w]
            ds = pr * (dp - jnp.sum(pr * dp, axis=0, keepdims=True))
            total = total + ds
            db = ds.astype(BF16)
            dvs.append(dot(pr.astype(BF16), da, 1, 0))
            dks.append(dot(db, spread(q_s[i, rows, :]), 1, 0))
            dqs.append(collapse(dot(db, k_s[i, rows, :], 0, 0)) * scale)
        turned = [jnp.transpose(total[:, 96 * a : 96 * a + 96]) for a in range(4)]
        here = pl.ds(pl.multiple_of(96 * xs, 96), 96)
        dsum_s[0, here, :] = jnp.concatenate(turned[0:2], axis=1)
        dsum_s[1, here, :] = jnp.concatenate(turned[2:4], axis=1)
        dq = jnp.concatenate(dqs, axis=0)
        dk = jnp.concatenate(dks, axis=0)
        dv = jnp.concatenate(dvs, axis=0)
        dqb, dkb, dvb = dq.astype(BF16), dk.astype(BF16), dv.astype(BF16)
        lead = jnp.concatenate([dqb[:, 0:128], dvb[:, 0:128]], axis=1)
        low_half = jnp.concatenate([dq[:, 128:192], dk], axis=1).astype(BF16)
        zeros = jnp.zeros((192, 64), F32)
        high_half = jnp.concatenate(
            [
                jnp.concatenate([dv[:, 128:192], jnp.zeros((192, 192), F32)], axis=1),
                jnp.concatenate([zeros, at_s[i].astype(F32)], axis=1),
            ],
            axis=0,
        ).astype(BF16)
        for b in range(8):
            rows = slice(96 * b, 96 * b + 96)
            one = dot(xtp_s[rows, :], lead, 1, 0).astype(BF16)
            grads[0, 0, i, b] = one[:, 0:128]
            grads[0, 1, i, b] = one[:, 128:256]
            two = dot(xt_s[rows, 0:192], low_half, 1, 0).astype(BF16)
            grads[2, 0, i, b] = two[:, 0:128]
            grads[1, 0, i, b] = two[:, 128:256]
            three = dot(xt_s[rows, :], high_half, 1, 0).astype(BF16)
            grads[2, 1, i, b] = three[:, 0:128]
            grads[1, 1, i, b] = three[:, 128:256]
        for num in range(3):
            push(grads.at[num, 1 - c, i], sums.at[num, i], send_d.at[0], recv_d.at[i], partner)
        part = (
            dot(dqb, weight(xs, 0), 1, 0) + dot(dkb, weight(xs, 1), 1, 0) + dot(dvb, weight(xs, 2), 1, 0)
        )
        dxn_s[...] = part if first else dxn_s[...] + part

    lines = (
        (0, y, lambda d: (z, shift(y, d, 8), x, c)),
        (1, z, lambda d: (shift(z, d, 8), y, x, c)),
    )
    far_first = (4, 3, 5, 2, 6, 1, 7)

    def take(i):
        landed(sums.at[:, i], recv_d.at[i])
        for num in range(3):
            for b in range(8):
                sums[num, i, b] = sums[num, i, b] + grads[num, c, i, b]
        if i < 3:
            push(sums.at[2, i], cxf.at[i], send_rx.at[0], recv_rx.at[0], (z, y, order[i], c))
        if i == 0:
            for num, me, reach in lines:
                far = shift(me, 4, 8)
                for way, sign in enumerate((1, -1)):
                    push(sums.at[num, 0, far, rows_of(way)], ring.at[num, way, 0, rows_of(way)],
                         send_v.at[0], recv_r.at[0], reach(sign))
        else:
            for d in far_first:
                for num, me, reach in lines:
                    push(sums.at[num, i, shift(me, d, 8)], direct.at[num, i - 1, d - 1],
                         send_v.at[0], recv_v.at[i - 1], reach(d))

    def step(s):
        landed(ring.at[0, :, 0] if s == 2 else ring.at[:, :, s - 2], recv_r.at[s - 2])
        for num, me, reach in lines:
            for way, sign in enumerate((1, -1)):
                block = shift(me, sign * (5 - s), 8)
                rows = slice(48 * way, 48 * way + 48) if s == 2 else slice(0, 96)
                sums[num, 0, block, rows, :] = sums[num, 0, block, rows, :] + ring[num, way, s - 2, rows, :]
                push(sums.at[num, 0, block], ring.at[num, way, s - 1], send_v.at[0], recv_r.at[s - 1], reach(sign))

    def finish(i):
        if i == 0:
            landed(ring.at[:, :, 3], recv_r.at[3])
        else:
            landed(direct.at[:, i - 1], recv_v.at[i - 1])
        for num, me, reach in lines:
            total = sums[num, i, me].astype(F32)
            if i == 0:
                total = total + ring[num, 0, 3].astype(F32) + ring[num, 1, 3].astype(F32)
            else:
                for d in range(1, 8):
                    total = total + direct[num, i - 1, d - 1].astype(F32)
            sums[num, i, me] = total.astype(BF16)
            if i < 3:
                push(sums.at[num, i, me], s2.at[num, i], send_2.at[0], recv_2.at[0], (z, y, order[i], c))

    backward(0, True)
    backward(1, False)
    take(0)
    backward(2, False)
    step(2)
    take(1)
    backward(3, False)
    step(3)
    take(2)

    dxn = dxn_s[...]
    xhat = xh_s[...]
    dxh = dxn * gain_ref[...].reshape(1, C)
    m1 = jnp.sum(dxh, axis=1, keepdims=True) * (1.0 / C)
    m2 = jnp.sum(dxh * xhat, axis=1, keepdims=True) * (1.0 / C)
    out = err_s[...] + inv * (dxh - m1 - xhat * m2)
    for w in range(3):
        gi_ref[49 * w : 49 * w + 49, :] = out[64 * w : 64 * w + 49, :]
    gain = jnp.sum(dxn * xhat, axis=0, keepdims=True)
    sq = err_s[...]
    loss = jnp.sum(sq * sq, axis=0, keepdims=True)
    loss = sum(loss[:, 128 * j : 128 * j + 128] for j in range(6))
    loss = jnp.sum(loss, axis=1, keepdims=True) + jnp.zeros((1, 128), F32)
    tail = jnp.concatenate(
        [gain[:, 128 * j : 128 * j + 128] for j in range(6)] + [loss, jnp.zeros((1, 128), F32)], axis=0
    )

    dtab = jnp.zeros((64, ENT), F32)
    for p in range(16):
        ds = jnp.concatenate([dsum_s.at[j][pl.ds(p, 24, stride=16), :] for j in range(2)], axis=1)
        top = ds.astype(BF16)
        rem = (ds - top.astype(F32)).astype(BF16)
        z8 = jnp.zeros((8, 256), F32)
        both = jnp.concatenate([top.astype(F32), z8, rem.astype(F32), z8], axis=0).astype(BF16)
        dtab = dtab + dot(both, onehot_rows(relp, p), 1, 1)
    dtab = dtab[0:24] + dtab[32:56]
    for g in range(8):
        sm_ref[g] = jnp.zeros((8, 384), F32)
        sm_ref[g, 0:3, 0:ENT] = dtab[3 * g : 3 * g + 3]
        sm_ref[g, :, 256:384] = tail
    for j, peer in enumerate(talk):
        push(sm_ref.at[2 * peer[2] + peer[3]], sm0.at[j], send_s.at[0], recv_s.at[0], peer)

    step(4)
    take(3)
    landed(cxf, recv_rx.at[0])
    for b in range(8):
        total = sums[2, 3, b].astype(F32)
        for i in range(3):
            total = total + cxf[i, b].astype(F32)
        sums[2, 3, b] = total.astype(BF16)
    for d in far_first:
        push(sums.at[2, 3, shift(z, d, 8)], s2x.at[d - 1], send_2.at[1], recv_2.at[1], line_z[d - 1])
    landed(sm0, recv_s.at[0])
    ss1[...] = sm_ref[mp] + sum(sm0[j] for j in range(7))
    for j, to in enumerate(line_y):
        push(ss1, sm1.at[j], send_s.at[1], recv_s.at[1], to)
    for i in range(4):
        finish(i)
    landed(sm1, recv_s.at[1])
    ss2[...] = ss1[...] + sum(sm1[j] for j in range(7))
    for j, to in enumerate(line_z):
        push(ss2, sm2.at[j], send_s.at[2], recv_s.at[2], to)

    a3[...] = jnp.zeros_like(a3)
    b3[...] = jnp.zeros_like(b3)

    def collect(num, me):
        total = sums[num, 3, me].astype(F32)
        for i in range(3):
            total = total + s2[num, i].astype(F32)
        flat[num] = total

    def spread_out(src, me, dst, num, reach):
        for d in (4, 3, 5, 2, 6, 1, 7, 0):
            for k, core in enumerate((c, 1 - c)):
                if d or k:
                    push(src.at[shift(me, d, 8)], dst.at[8 * k + d - 1], send_3.at[num], recv_3.at[num], reach(d, core))

    def gathered(src, me, dst, k):
        total = src[me] if k == 0 else dst[7]
        for d in range(1, 8):
            total = total + dst[8 * k + d - 1]
        return total

    landed(s2, recv_2.at[0])
    collect(0, y)
    for i in range(8):
        a3[i, 0:12, :] = flat[0, 12 * i : 12 * i + 12, :]
    spread_out(a3, z, r3a, 0, lambda d, core: (shift(z, d, 8), y, x, core))
    collect(1, z)
    for i in range(8):
        b3[i, 1, 0:12, :] = flat[1, 12 * i : 12 * i + 12, :]
    landed(s2x, recv_2.at[1])
    total = sums[2, 3, z].astype(F32)
    for j in range(7):
        total = total + s2x[j].astype(F32)
    flat[2] = total
    for i in range(8):
        b3[i, 0, 0:12, :] = flat[2, 12 * i : 12 * i + 12, :]
    spread_out(b3, y, r3b, 1, lambda d, core: (z, shift(y, d, 8), x, core))

    landed(sm2, recv_s.at[2])
    total = ss2[...] + sum(sm2[j] for j in range(7))
    gtab_ref[...] = total[0:3, 0:TABLE] * shrink
    for j in range(6):
        ggain_ref[pl.ds(128 * j, 128)] = total[j : j + 1, 256:384].reshape(128) * shrink
    loss_ref[...] = total[6:7, 256:384] * (0.5 / count)
    landed(r3a, recv_3.at[0])
    for k, core in enumerate((c, 1 - c)):
        part_s[core, :, 0:128] = gathered(a3, z, r3a, k)
    landed(r3b, recv_3.at[1])
    for k, core in enumerate((c, 1 - c)):
        total = gathered(b3, y, r3b, k)
        part_s[core, :, 128:256] = total[0]
        part_s[core, :, 256:384] = total[1]
    for t in range(4):
        at = 192 * (t % 2)
        both = part_s[t // 2, 0:12, :] * shrink
        mine = jnp.where(c == 0, both[:, at : at + 96], both[:, at + 96 : at + 192])
        if t < 3:
            gq_ref[t] = mine
        else:
            gp_ref[...] = mine
    left_here(w_ref.at[:, pl.ds(0, 3), 0], send_w.at[0])
    left_here(w_ref.at[:, :, 0], send_c.at[0])
    left_here(t_ref.at[pl.ds(0, 7)], send_t.at[0])
    left_here(grads.at[:, 0], send_d.at[0])
    left_here(grads.at[0, :, :, pl.ds(0, 7)], send_v.at[0])
    left_here(cxf, send_rx.at[0])
    left_here(s2, send_2.at[0])
    left_here(s2x, send_2.at[1])
    left_here(r3a, send_3.at[0])
    left_here(r3b, send_3.at[1])
    for k, amount in enumerate((sm0, sm1, sm2)):
        left_here(amount, send_s.at[k])


def whole(count, *args):
    dma = pltpu.SemaphoreType.DMA
    f = lambda *s: pltpu.VMEM(s, F32)
    b = lambda *s: pltpu.VMEM(s, BF16)
    shape = jax.ShapeDtypeStruct
    return pl.pallas_call(
        functools.partial(whole_kernel, count),
        name="window_layer",
        out_shape=(
            shape((147, C), F32), shape((3, 12, 96), F32), shape((12, 96), F32),
            shape((3, TABLE), F32), shape((C,), F32), shape((1, 128), F32),
        ),
        in_specs=[pl.BlockSpec(memory_space=pltpu.HBM)] * 8,
        out_specs=(VM,) * 6,
        scratch_shapes=[
            b(147, C), b(147, C), pltpu.VMEM((24, 49), jnp.int32), pltpu.VMEM((49, 49), jnp.int32), f(C), f(3, TABLE),
            f(8, 256), b(4, 4, 2, 96, C), f(8, 8, 256),
            dma((1,)), dma((2,)), dma((2,)), dma((3,)), dma((1,)), dma((4,)), dma((1,)), dma((1,)), dma((10,)),
            f(152, C), f(192, C), f(192, C), f(192, C), b(192, C), b(C, 384), f(C, 192), b(C, 192),
            f(192, C), f(192, C), b(192, C), f(192, C),
            pltpu.VMEM((64, 128), jnp.int32), f(2, 384, 128), f(4, 64, 384), f(4, 3, 64, 384),
            b(4, 192, 192), b(4, 192, 192), b(4, 192, 192), b(4, 192, 192), f(2, 384, 128), f(8, 8, 384),
            b(3, 2, 4, 8, 96, 128), b(3, 4, 8, 96, 128), b(2, 2, 4, 96, 128), b(2, 3, 7, 96, 128),
            b(3, 8, 96, 128), b(2, 3, 96, 128), b(7, 96, 128), f(3, 96, 128),
            f(8, 16, 128), f(8, 2, 16, 128), f(15, 16, 128), f(15, 2, 16, 128), f(2, 16, 384),
            f(7, 8, 384), f(7, 8, 384), f(7, 8, 384), f(8, 384), f(8, 384),
            dma((1,)), dma((4,)), dma((1,)), dma((4,)), dma((3,)), dma((1,)), dma((1,)),
            dma((2,)), dma((2,)), dma((2,)), dma((2,)), dma((3,)), dma((3,)),
        ],
        compiler_params=pltpu.CompilerParams(
            collective_id=0, has_side_effects=True, vmem_limit_bytes=40 * 2**20
        ),
    )(*args)


def hand_out_kernel(*refs):
    copies = [pltpu.make_async_copy(refs[k], refs[6 + k], refs[12].at[k]) for k in range(6)]
    for copy in copies:
        copy.start()
    for copy in copies:
        copy.wait()


def hand_out(*arrays):
    return pl.pallas_call(
        hand_out_kernel,
        name="hand_out",
        out_shape=tuple(jax.ShapeDtypeStruct(a.shape, a.dtype) for a in arrays),
        in_specs=[VM] * 6,
        out_specs=(pl.BlockSpec(memory_space=pl.ANY),) * 6,
        scratch_shapes=[pltpu.SemaphoreType.DMA((6,))],
        compiler_params=pltpu.CompilerParams(vmem_limit_bytes=8 * 2**20),
    )(*arrays)


def per_device(tokens, target, regions, rel_index, layer_norm_gain, bias_table, w_qkv, w_proj):
    count = tokens.shape[0] * lax.axis_size(DP_WIN_MP)
    args = (tokens, target, regions, rel_index, layer_norm_gain, bias_table.T, w_qkv, w_proj)
    done = whole(count, *[pltpu.with_memory_space_constraint(one, pltpu.HBM) for one in args])
    gi, gq, gp, gtab, ggain, loss = hand_out(*done)
    return gi, jnp.transpose(gq, (0, 2, 1)), gp.T, gtab.T, ggain, loss[0, 0]


def solution(mesh):
    split = Mesh(mesh.devices.reshape(mesh.shape["dp"], mesh.shape["win"], 4, 2), DP_WIN_MP)
    return jax.shard_map(
        per_device,
        mesh=split,
        in_specs=(
            P(DP_WIN_MP, None), P(DP_WIN_MP, None), P(("dp", "win"), None), P(), P(),
            P(None, MP), P(None, MP, None), P(MP, None),
        ),
        out_specs=(
            P(DP_WIN_MP, None), P(None, MP, ("dp", "win")), P(MP, ("dp", "win")), P(None, MP), P(), P(),
        ),
        check_vma=False,
    )
```

```python
import functools

import jax
import jax.numpy as jnp
from jax import lax
from jax.experimental import pallas as pl
from jax.experimental.pallas import tpu as pltpu
from jax.sharding import Mesh
from jax.sharding import PartitionSpec as P

C = 768
HD = 32
WIN_TOK = 49
TABLE = 169
ENT = 176
F32 = jnp.float32
BF16 = jnp.bfloat16
MESH = pl.DeviceIdType.MESH
VM = pl.BlockSpec(memory_space=pltpu.VMEM)
MP = ("x", "core")
DP_WIN_MP = ("dp", "win", "x", "core")
BIG = (0, C // 2)


def dot(a, b, ca, cb):
    return lax.dot_general(a, b, (((ca,), (cb,)), ((), ())), preferred_element_type=F32)


def onehot_rows(relp, p):
    rows = jnp.concatenate([relp[16 * a + p : 16 * a + p + 1, 0:64] for a in range(4)], axis=1)
    entry = lax.broadcasted_iota(jnp.int32, (ENT, 256), 0)
    return jnp.where(entry == rows, 1.0, 0.0).astype(BF16)


def shift(v, d, n):
    return lax.rem(v + (d % n), n)


def whole_kernel(count, *refs):
    (
        tok_hbm, tgt_hbm, reg_hbm, rel_hbm, gain_hbm, table_hbm, wqkv_hbm, wproj_hbm,
        gi_ref, gq_ref, gp_ref, gtab_ref, ggain_ref, loss_ref,
        tok_ref, tgt_ref, reg_ref, rel_ref, gain_ref, table_ref, tab_s, w_ref, t_ref,
        send_w, recv_x, recv_o, recv_n, send_c, recv_c, send_t, recv_t, own_sem,
        pad_s, x_s, t_s, xh_s, xn_s, xt_s, xtf_s, xtp_s, ysum_s, err_s, gb_s, dxn_s,
        relp_s, bt_s, bias_s, p_s, q_s, k_s, v_s, at_s, dsum_s, sm_ref,
        grads, sums, direct, cxf, s2, s2x, flat, a3, b3, x3, r3a, r3b, r3x, part_s, sm0, sm1, sm2, ss1, ss2,
        send_d, recv_d, send_v, recv_v, send_rx, recv_rx,
        send_2, recv_2, send_3, recv_3, send_s, recv_s,
    ) = refs
    z, y, x, c = (lax.axis_index(name) for name in DP_WIN_MP)
    mp = 2 * x + c
    scale = HD**-0.5
    shrink = count**-0.5
    partner = (z, y, x, 1 - c)
    talk = [partner] + [(z, y, shift(x, d, 4), core) for d in (1, 2, 3) for core in (c, 1 - c)]
    line_y = [(z, shift(y, d, 8), x, c) for d in range(1, 8)]
    line_z = [(shift(z, d, 8), y, x, c) for d in range(1, 8)]
    line_x = [(z, y, shift(x, d, 4), c) for d in range(1, 4)]
    def push(src, dst, ssem, rsem, to):
        pltpu.make_async_remote_copy(
            src_ref=src, dst_ref=dst, send_sem=ssem, recv_sem=rsem, device_id=to, device_id_type=MESH
        ).start()

    def landed(dst, rsem):
        pltpu.make_async_remote_copy(
            src_ref=dst, dst_ref=dst, send_sem=rsem, recv_sem=rsem, device_id=partner, device_id_type=MESH
        ).wait_recv()

    def left_here(amount, ssem):
        pltpu.make_async_remote_copy(
            src_ref=amount, dst_ref=amount, send_sem=ssem, recv_sem=ssem, device_id=partner, device_id_type=MESH
        ).wait_send()

    barrier = pltpu.get_barrier_semaphore()
    peers = talk + line_y + line_z
    peers += [to[:3] + (1 - c,) for to in line_y + line_z]
    for peer in peers:
        pl.semaphore_signal(barrier, inc=1, device_id=peer, device_id_type=MESH)

    load = [
        pltpu.make_async_copy(src, dst, own_sem.at[k])
        for k, (src, dst) in enumerate(
            (
                (tok_hbm, tok_ref), (wqkv_hbm.at[0], w_ref.at[x, 0, c]), (wqkv_hbm.at[1], w_ref.at[x, 1, c]),
                (wqkv_hbm.at[2], w_ref.at[x, 2, c]), (wproj_hbm, w_ref.at[x, 3, c]), (table_hbm, table_ref),
                (gain_hbm, gain_ref), (tgt_hbm, tgt_ref), (rel_hbm, rel_ref), (reg_hbm, reg_ref),
            )
        )
    ]
    for one in load:
        one.start()
    tab_s[...] = jnp.zeros_like(tab_s)
    load[5].wait()
    for h in range(3):
        tab_s[:, 256 * h : 256 * h + TABLE] = table_ref[h : h + 1, :]
    t_ref[mp] = tab_s[...]
    load[0].wait()
    load[6].wait()
    load[7].wait()
    x_s[...] = jnp.zeros_like(x_s)
    t_s[...] = jnp.zeros_like(t_s)
    pad_s[0:147, :] = tok_ref[...].astype(F32)
    for w in range(3):
        x_s[64 * w : 64 * w + 49, :] = pad_s[49 * w : 49 * w + 49, :]
    pad_s[0:147, :] = tgt_ref[...].astype(F32)
    for w in range(3):
        t_s[64 * w : 64 * w + 49, :] = pad_s[49 * w : 49 * w + 49, :]
    xx = x_s[...]
    mean = jnp.sum(xx, axis=1, keepdims=True) * (1.0 / C)
    cen = xx - mean
    var = jnp.sum(cen * cen, axis=1, keepdims=True) * (1.0 / C)
    inv = lax.rsqrt(var + 1e-05)
    xh_s[...] = cen * inv
    xn_s[...] = (xh_s[...] * gain_ref[...].reshape(1, C)).astype(BF16)

    pl.semaphore_wait(barrier, len(peers))

    colors = (lax.rem(y + 2 * z, 4), lax.rem(z + 2 * y, 4))
    near_y = [(z, shift(y, d, 8), x, c) for d in (1, -1)]
    near_z = [(shift(z, d, 8), y, x, c) for d in (1, -1)]
    strong = (near_y, near_z)
    weak = (near_z, near_y)

    def rows_of(m):
        return pl.ds(48 * m, 48)

    def piece(xs, tint, core, m):
        return w_ref.at[xs, tint, core, rows_of(m)]

    def lanes(xs, tint, core, m, j):
        return w_ref.at[xs, tint, core, rows_of(m), pl.ds(BIG[j], C // 2)]

    for to in talk:
        push(tab_s, t_ref.at[mp], send_t.at[0], recv_t.at[0], to)
    for k in range(1, 5):
        load[k].wait()
    for m in range(2):
        for j, d in enumerate((1, -1)):
            there = piece(x, colors[m], c, m)
            push(there, there, send_w.at[0], recv_x.at[m], (z, y, shift(x, d, 4), c))
    for one in range(4):
        there = w_ref.at[x, one, c]
        push(there, there, send_c.at[0], recv_c.at[3], partner)
    load[8].wait()
    load[9].wait()

    xt = jnp.transpose(xn_s[...].astype(F32))
    xt_s[:, 0:192] = xt.astype(BF16)
    xtf_s[...] = xt
    for b in range(8):
        block = jnp.concatenate([xtf_s[96 * k + 12 * b : 96 * k + 12 * b + 12, :] for k in range(8)], axis=0)
        xtp_s[96 * b : 96 * b + 96, 0:192] = block.astype(BF16)
    relp_s[...] = jnp.full(relp_s.shape, -1, jnp.int32)
    relp_s[0:49, 0:49] = rel_ref[...]
    relp = relp_s[...]
    regs = jnp.concatenate(
        [reg_ref[pl.ds(3 * mp + w, 1), :].astype(F32) for w in range(3)] + [jnp.zeros((5, 49), F32)], axis=0
    )
    regs = jnp.concatenate([regs, jnp.zeros((8, 15), F32)], axis=1)
    lane = lax.broadcasted_iota(jnp.int32, (64, 384), 1)
    query_of = (lane // 96) * 16 + lane % 16
    pick = jnp.where(lax.broadcasted_iota(jnp.int32, (64, 384), 0) == query_of, 1.0, 0.0)
    reg_q = dot(regs, pick, 1, 0)
    eye = jnp.where(
        lax.broadcasted_iota(jnp.int32, (64, 64), 0) == lax.broadcasted_iota(jnp.int32, (64, 64), 1), 1.0, 0.0
    )
    reg_k = dot(eye, regs, 1, 1)
    row = lax.broadcasted_iota(jnp.int32, (96, 192), 0)
    col = lax.broadcasted_iota(jnp.int32, (96, 192), 1)
    own = jnp.where(row // 16 == col // 32, 1.0, 0.0)
    own_bf = own.astype(BF16)

    left, right, opposite = shift(x, -1, 4), shift(x, 1, 4), shift(x, 2, 4)
    sources = (left, right, opposite)

    def hand_on(slot, m):
        xs = sources[slot]
        tint = colors[m]
        for j in range(2):
            push(piece(xs, tint, c, m), piece(xs, tint, c, m), send_w.at[0], recv_n.at[slot], strong[m][j])
        for j in range(2):
            push(lanes(xs, tint, c, m, j), lanes(xs, tint, c, m, j), send_w.at[0], recv_n.at[slot], weak[m][j])
        push(piece(xs, tint, c, m), piece(xs, tint, c, m), send_c.at[0], recv_c.at[slot], partner)

    def from_sides(m):
        landed(w_ref.at[left, 0, c], recv_x.at[m])
        there = piece(sources[m], colors[m], c, m)
        push(there, there, send_w.at[0], recv_o.at[m], (z, y, shift(x, 1 - 2 * m, 4), c))
        hand_on(0, m)

    landed(t_ref.at[pl.ds(0, 7)], recv_t.at[0])
    tab = jnp.concatenate(
        [t_ref[g, 0:1, 256 * h : 256 * h + ENT] for g in range(8) for h in range(3)], axis=0
    )
    hi = tab.astype(BF16)
    rest = tab - hi.astype(F32)
    mid = rest.astype(BF16)
    low = (rest - mid.astype(F32)).astype(BF16)
    zero8 = jnp.zeros((8, ENT), F32)
    parts = jnp.concatenate(
        [t for one in (hi, mid, low) for t in (one.astype(F32), zero8)], axis=0
    ).astype(BF16)
    for p in range(16):
        got = dot(parts, onehot_rows(relp, p), 1, 0)
        got = got[0:24] + got[32:56] + got[64:88]
        bt_s.at[0][pl.ds(p, 24, stride=16), :] = got[:, 0:128]
        bt_s.at[1][pl.ds(p, 24, stride=16), :] = got[:, 128:256]
    keypad = jnp.where(lax.broadcasted_iota(jnp.int32, (64, 384), 0) < WIN_TOK, 0.0, -1e30)
    for i in range(4):
        turned = [jnp.transpose(bt_s[j, 96 * i : 96 * i + 96, :]) for j in range(2)]
        turned = [t[64 * a : 64 * a + 64] for t in turned for a in range(2)]
        bias_s[i] = jnp.concatenate(turned, axis=1) + keypad

    def shift_mask(w):
        return jnp.where(reg_k[:, w : w + 1] == reg_q[w : w + 1, :], 0.0, -100.0)

    def spread(block):
        return jnp.concatenate(
            [jnp.concatenate([block[16 * a : 16 * a + 16]] * 6, axis=0) * own_bf for a in range(4)], axis=0
        )

    def collapse(big):
        out = []
        for a in range(4):
            part = big[96 * a : 96 * a + 96] * own
            out.append(sum(part[16 * h : 16 * h + 16] for h in range(6)))
        return jnp.concatenate(out, axis=0)

    def weight(xs, t):
        return w_ref[xs, t].reshape(192, C)

    def forward(i, xs, first):
        xn = xn_s[...]
        q_s[i] = (dot(xn, weight(xs, 0), 1, 1) * scale).astype(BF16)
        k_s[i] = dot(xn, weight(xs, 1), 1, 1).astype(BF16)
        v_s[i] = dot(xn, weight(xs, 2), 1, 1).astype(BF16)
        for w in range(3):
            rows = slice(64 * w, 64 * w + 64)
            sc = dot(k_s[i, rows, :], spread(q_s[i, rows, :]), 1, 1)
            sc = sc + bias_s[xs] + shift_mask(w)
            ex = jnp.exp(sc - jnp.max(sc, axis=0, keepdims=True))
            pr = ex / jnp.sum(ex, axis=0, keepdims=True)
            p_s[i, w] = pr
            at_s[i, rows, :] = collapse(dot(pr.astype(BF16), v_s[i, rows, :], 0, 0)).astype(BF16)
        part = dot(at_s[i], weight(xs, 3), 1, 0)
        ysum_s[...] = part if first else ysum_s[...] + part

    order = (opposite, right, left, x)

    def near_tints(m):
        return [lax.rem(colors[m] + d, 4) for d in (3, 1)], lax.rem(colors[m] + 2, 4)

    def hand_over(slot):
        xs = sources[slot]
        landed(w_ref.at[xs, pl.ds(0, 3), c], recv_n.at[slot])
        for m in range(2):
            tints, across = near_tints(m)
            for j in range(2):
                there = piece(xs, tints[j], c, m)
                push(there, there, send_c.at[0], recv_c.at[slot], partner)
            for j in range(2):
                there = lanes(xs, across, c, m, j)
                push(there, there, send_c.at[0], recv_c.at[slot], partner)

    def whole_slot(slot):
        landed(w_ref.at[sources[slot], :, 1 - c], recv_c.at[slot])

    from_sides(0)
    from_sides(1)
    hand_on(1, 0)
    hand_on(1, 1)
    landed(w_ref.at[x, :, 1 - c], recv_c.at[3])
    forward(3, x, True)
    for m in range(2):
        landed(piece(opposite, colors[m], c, m), recv_o.at[m])
        hand_on(2, m)
    hand_over(0)
    hand_over(1)
    whole_slot(0)
    forward(2, left, False)
    hand_over(2)
    whole_slot(1)
    forward(1, right, False)
    whole_slot(2)
    forward(0, opposite, False)

    rowid = lax.broadcasted_iota(jnp.int32, (192, C), 0) % 64
    err = jnp.where(rowid < WIN_TOK, x_s[...] + ysum_s[...] - t_s[...], 0.0)
    err_s[...] = err
    gb_s[...] = err.astype(BF16)
    turned = jnp.transpose(err)
    xt_s[:, 192:384] = turned.astype(BF16)
    xtf_s[...] = turned
    for b in range(8):
        block = jnp.concatenate([xtf_s[96 * k + 12 * b : 96 * k + 12 * b + 12, :] for k in range(8)], axis=0)
        xtp_s[96 * b : 96 * b + 96, 192:384] = block.astype(BF16)

    def backward(i, first, middle):
        xs = order[i]
        datt = dot(gb_s[...], weight(xs, 3), 1, 1).astype(BF16)
        dqs, dks, dvs = [], [], []
        total = jnp.zeros((64, 384), F32)
        for w in range(3):
            rows = slice(64 * w, 64 * w + 64)
            da = spread(datt[rows])
            dp = dot(v_s[i, rows, :], da, 1, 1)
            pr = p_s[i, w]
            ds = pr * (dp - jnp.sum(pr * dp, axis=0, keepdims=True))
            total = total + ds
            db = ds.astype(BF16)
            dvs.append(dot(pr.astype(BF16), da, 1, 0))
            dks.append(dot(db, spread(q_s[i, rows, :]), 1, 0))
            dqs.append(collapse(dot(db, k_s[i, rows, :], 0, 0)) * scale)
        turned = [jnp.transpose(total[:, 96 * a : 96 * a + 96]) for a in range(4)]
        here = pl.ds(pl.multiple_of(96 * xs, 96), 96)
        dsum_s[0, here, :] = jnp.concatenate(turned[0:2], axis=1)
        dsum_s[1, here, :] = jnp.concatenate(turned[2:4], axis=1)
        dq = jnp.concatenate(dqs, axis=0)
        dk = jnp.concatenate(dks, axis=0)
        dv = jnp.concatenate(dvs, axis=0)
        dqb, dkb, dvb = dq.astype(BF16), dk.astype(BF16), dv.astype(BF16)
        middle()
        lead = jnp.concatenate([dqb[:, 0:128], dvb[:, 0:128]], axis=1)
        low_half = jnp.concatenate([dq[:, 128:192], dk], axis=1).astype(BF16)
        zeros = jnp.zeros((192, 64), F32)
        att = at_s[i].astype(F32)
        mixed = jnp.concatenate(
            [
                jnp.concatenate([dv[:, 128:192], zeros], axis=1),
                jnp.concatenate([zeros, att[:, 0:64]], axis=1),
            ],
            axis=0,
        ).astype(BF16)
        last = att[:, 64:192].astype(BF16)
        for b in range(8):
            rows = slice(96 * b, 96 * b + 96)
            one = dot(xtp_s[rows, 0:192], lead, 1, 0).astype(BF16)
            grads[0, 0, i, b] = one[:, 0:128]
            grads[0, 1, i, b] = one[:, 128:256]
            two = dot(xt_s[rows, 0:192], low_half, 1, 0).astype(BF16)
            grads[2, 0, i, b] = two[:, 0:128]
            grads[1, 0, i, b] = two[:, 128:256]
            grads[2, 1, i, b] = dot(xtp_s[rows, :], mixed, 1, 0).astype(BF16)
            grads[1, 1, i, b] = dot(xt_s[rows, 192:384], last, 1, 0).astype(BF16)
        for num in range(3):
            push(grads.at[num, 1 - c, i], sums.at[num, i], send_d.at[0], recv_d.at[i], partner)
        part = (
            dot(dqb, weight(xs, 0), 1, 0) + dot(dkb, weight(xs, 1), 1, 0) + dot(dvb, weight(xs, 2), 1, 0)
        )
        dxn_s[...] = part if first else dxn_s[...] + part

    lines = (
        (0, y, lambda d: (z, shift(y, d, 8), x, c)),
        (1, z, lambda d: (shift(z, d, 8), y, x, c)),
    )
    far_first = (4, 3, 5, 2, 6, 1, 7)

    def take(i):
        landed(sums.at[:, i], recv_d.at[i])
        for num in range(3):
            for b in range(8):
                sums[num, i, b] = sums[num, i, b] + grads[num, c, i, b]
        if i < 3:
            push(sums.at[2, i], cxf.at[i], send_rx.at[0], recv_rx.at[0], (z, y, order[i], c))
        for d in far_first:
            for num, me, reach in lines:
                push(sums.at[num, i, shift(me, d, 8)], direct.at[num, i, d - 1], send_v.at[0], recv_v.at[i], reach(d))

    def finish(i):
        landed(direct.at[:, i], recv_v.at[i])
        for num, me, reach in lines:
            total = sums[num, i, me].astype(F32)
            for d in range(1, 8):
                total = total + direct[num, i, d - 1].astype(F32)
            sums[num, i, me] = total.astype(BF16)
            if i < 3:
                push(sums.at[num, i, me], s2.at[num, i], send_2.at[0], recv_2.at[0], (z, y, order[i], c))

    backward(0, True, lambda: None)
    backward(1, False, lambda: take(0))
    backward(2, False, lambda: take(1))
    backward(3, False, lambda: take(2))

    dxn = dxn_s[...]
    xhat = xh_s[...]
    dxh = dxn * gain_ref[...].reshape(1, C)
    m1 = jnp.sum(dxh, axis=1, keepdims=True) * (1.0 / C)
    m2 = jnp.sum(dxh * xhat, axis=1, keepdims=True) * (1.0 / C)
    out = err_s[...] + inv * (dxh - m1 - xhat * m2)
    for w in range(3):
        gi_ref[49 * w : 49 * w + 49, :] = out[64 * w : 64 * w + 49, :]
    gain = jnp.sum(dxn * xhat, axis=0, keepdims=True)
    sq = err_s[...]
    loss = jnp.sum(sq * sq, axis=0, keepdims=True)
    loss = sum(loss[:, 128 * j : 128 * j + 128] for j in range(6))
    loss = jnp.sum(loss, axis=1, keepdims=True) + jnp.zeros((1, 128), F32)
    tail = jnp.concatenate(
        [gain[:, 128 * j : 128 * j + 128] for j in range(6)] + [loss, jnp.zeros((1, 128), F32)], axis=0
    )

    dtab = jnp.zeros((64, ENT), F32)
    for p in range(16):
        ds = jnp.concatenate([dsum_s.at[j][pl.ds(p, 24, stride=16), :] for j in range(2)], axis=1)
        top = ds.astype(BF16)
        rem = (ds - top.astype(F32)).astype(BF16)
        z8 = jnp.zeros((8, 256), F32)
        both = jnp.concatenate([top.astype(F32), z8, rem.astype(F32), z8], axis=0).astype(BF16)
        dtab = dtab + dot(both, onehot_rows(relp, p), 1, 1)
    dtab = dtab[0:24] + dtab[32:56]
    for g in range(8):
        sm_ref[g] = jnp.zeros((8, 384), F32)
        sm_ref[g, 0:3, 0:ENT] = dtab[3 * g : 3 * g + 3]
        sm_ref[g, :, 256:384] = tail
    for j, peer in enumerate(talk):
        push(sm_ref.at[2 * peer[2] + peer[3]], sm0.at[j], send_s.at[0], recv_s.at[0], peer)

    take(3)
    finish(0)
    first_x = z * (1 - c) + y * c
    then_x = y * (1 - c) + z * c
    landed(cxf, recv_rx.at[0])
    for b in range(8):
        total = sums[2, 3, b].astype(F32)
        for i in range(3):
            total = total + cxf[i, b].astype(F32)
        sums[2, 3, b] = total.astype(BF16)
    for d in far_first:
        to = (lax.rem(z + d * (1 - c), 8), lax.rem(y + d * c, 8), x, c)
        push(sums.at[2, 3, shift(first_x, d, 8)], s2x.at[d - 1], send_2.at[1], recv_2.at[1], to)
    finish(1)
    landed(sm0, recv_s.at[0])
    ss1[...] = sm_ref[mp] + sum(sm0[j] for j in range(7))
    for j, to in enumerate(line_y):
        push(ss1, sm1.at[j], send_s.at[1], recv_s.at[1], to)
    finish(2)
    finish(3)
    landed(sm1, recv_s.at[1])
    ss2[...] = ss1[...] + sum(sm1[j] for j in range(7))
    for j, to in enumerate(line_z):
        push(ss2, sm2.at[j], send_s.at[2], recv_s.at[2], to)

    a3[...] = jnp.zeros_like(a3)
    b3[...] = jnp.zeros_like(b3)
    x3[...] = jnp.zeros_like(x3)

    def collect(num, me):
        total = sums[num, 3, me].astype(F32)
        for i in range(3):
            total = total + s2[num, i].astype(F32)
        flat[num] = total

    def spread_out(src, me, dst, num, reach):
        for d in (4, 3, 5, 2, 6, 1, 7, 0):
            for k, core in enumerate((c, 1 - c)):
                if d or k:
                    push(src.at[shift(me, d, 8)], dst.at[8 * k + d - 1], send_3.at[num], recv_3.at[num], reach(d, core))

    def gathered(src, me, dst, k):
        total = src[me] if k == 0 else dst[7]
        for d in range(1, 8):
            total = total + dst[8 * k + d - 1]
        return total

    landed(s2, recv_2.at[0])
    collect(0, y)
    for i in range(8):
        a3[i, 0:12, :] = flat[0, 12 * i : 12 * i + 12, :]
    spread_out(a3, z, r3a, 0, lambda d, core: (shift(z, d, 8), y, x, core))
    collect(1, z)
    for i in range(8):
        b3[i, 0:12, :] = flat[1, 12 * i : 12 * i + 12, :]
    spread_out(b3, y, r3b, 1, lambda d, core: (z, shift(y, d, 8), x, core))
    landed(s2x, recv_2.at[1])
    total = sums[2, 3, first_x].astype(F32)
    for j in range(7):
        total = total + s2x[j].astype(F32)
    flat[2] = total
    for i in range(8):
        x3[i, 0:12, :] = flat[2, 12 * i : 12 * i + 12, :]
    spread_out(
        x3, then_x, r3x, 2, lambda d, core: (lax.rem(z + d * c, 8), lax.rem(y + d * (1 - c), 8), x, core)
    )

    landed(sm2, recv_s.at[2])
    total = ss2[...] + sum(sm2[j] for j in range(7))
    gtab_ref[...] = total[0:3, 0:TABLE] * shrink
    for j in range(6):
        ggain_ref[pl.ds(128 * j, 128)] = total[j : j + 1, 256:384].reshape(128) * shrink
    loss_ref[...] = total[6:7, 256:384] * (0.5 / count)
    landed(r3a, recv_3.at[0])
    for k, core in enumerate((c, 1 - c)):
        part_s[core, :, 0:128] = gathered(a3, z, r3a, k)
    landed(r3b, recv_3.at[1])
    for k, core in enumerate((c, 1 - c)):
        part_s[core, :, 256:384] = gathered(b3, y, r3b, k)
    landed(r3x, recv_3.at[2])
    for k, core in enumerate((c, 1 - c)):
        part_s[core, :, 128:256] = gathered(x3, then_x, r3x, k)
    for t in range(4):
        at = 192 * (t % 2)
        both = part_s[t // 2, 0:12, :] * shrink
        mine = jnp.where(c == 0, both[:, at : at + 96], both[:, at + 96 : at + 192])
        if t < 3:
            gq_ref[t] = mine
        else:
            gp_ref[...] = mine
    left_here(w_ref.at[:, pl.ds(0, 3), 0], send_w.at[0])
    left_here(w_ref.at[:, :, 0], send_c.at[0])
    left_here(t_ref.at[pl.ds(0, 7)], send_t.at[0])
    left_here(grads.at[:, 0], send_d.at[0])
    left_here(grads.at[0, :, :, pl.ds(0, 7)], send_v.at[0])
    left_here(cxf, send_rx.at[0])
    left_here(s2, send_2.at[0])
    left_here(s2x, send_2.at[1])
    left_here(r3a, send_3.at[0])
    left_here(r3b, send_3.at[1])
    left_here(r3x, send_3.at[2])
    for k, amount in enumerate((sm0, sm1, sm2)):
        left_here(amount, send_s.at[k])


def whole(count, *args):
    dma = pltpu.SemaphoreType.DMA
    f = lambda *s: pltpu.VMEM(s, F32)
    b = lambda *s: pltpu.VMEM(s, BF16)
    shape = jax.ShapeDtypeStruct
    return pl.pallas_call(
        functools.partial(whole_kernel, count),
        name="window_layer",
        out_shape=(
            shape((147, C), F32), shape((3, 12, 96), F32), shape((12, 96), F32),
            shape((3, TABLE), F32), shape((C,), F32), shape((1, 128), F32),
        ),
        in_specs=[pl.BlockSpec(memory_space=pltpu.HBM)] * 8,
        out_specs=(VM,) * 6,
        scratch_shapes=[
            b(147, C), b(147, C), pltpu.VMEM((24, 49), jnp.int32), pltpu.VMEM((49, 49), jnp.int32), f(C), f(3, TABLE),
            f(1, C), b(4, 4, 2, 96, C), f(8, 1, C),
            dma((1,)), dma((2,)), dma((2,)), dma((3,)), dma((1,)), dma((4,)), dma((1,)), dma((1,)), dma((10,)),
            f(152, C), f(192, C), f(192, C), f(192, C), b(192, C), b(C, 384), f(C, 192), b(C, 384),
            f(192, C), f(192, C), b(192, C), f(192, C),
            pltpu.VMEM((64, 128), jnp.int32), f(2, 384, 128), f(4, 64, 384), f(4, 3, 64, 384),
            b(4, 192, 192), b(4, 192, 192), b(4, 192, 192), b(4, 192, 192), f(2, 384, 128), f(8, 8, 384),
            b(3, 2, 4, 8, 96, 128), b(3, 4, 8, 96, 128), b(2, 4, 7, 96, 128),
            b(3, 8, 96, 128), b(2, 3, 96, 128), b(7, 96, 128), f(3, 96, 128),
            f(8, 16, 128), f(8, 16, 128), f(8, 16, 128), f(15, 16, 128), f(15, 16, 128), f(15, 16, 128),
            f(2, 16, 384),
            f(7, 8, 384), f(7, 8, 384), f(7, 8, 384), f(8, 384), f(8, 384),
            dma((1,)), dma((4,)), dma((1,)), dma((4,)), dma((1,)), dma((1,)),
            dma((2,)), dma((2,)), dma((3,)), dma((3,)), dma((3,)), dma((3,)),
        ],
        compiler_params=pltpu.CompilerParams(
            collective_id=0, has_side_effects=True, vmem_limit_bytes=40 * 2**20
        ),
    )(*args)


def hand_out_kernel(*refs):
    copies = [pltpu.make_async_copy(refs[k], refs[6 + k], refs[12].at[k]) for k in range(6)]
    for copy in copies:
        copy.start()
    for copy in copies:
        copy.wait()


def hand_out(*arrays):
    return pl.pallas_call(
        hand_out_kernel,
        name="hand_out",
        out_shape=tuple(jax.ShapeDtypeStruct(a.shape, a.dtype) for a in arrays),
        in_specs=[VM] * 6,
        out_specs=(pl.BlockSpec(memory_space=pl.ANY),) * 6,
        scratch_shapes=[pltpu.SemaphoreType.DMA((6,))],
        compiler_params=pltpu.CompilerParams(vmem_limit_bytes=8 * 2**20),
    )(*arrays)


def per_device(tokens, target, regions, rel_index, layer_norm_gain, bias_table, w_qkv, w_proj):
    count = tokens.shape[0] * lax.axis_size(DP_WIN_MP)
    args = (tokens, target, regions, rel_index, layer_norm_gain, bias_table.T, w_qkv, w_proj)
    done = whole(count, *[pltpu.with_memory_space_constraint(one, pltpu.HBM) for one in args])
    gi, gq, gp, gtab, ggain, loss = hand_out(*done)
    return gi, jnp.transpose(gq, (0, 2, 1)), gp.T, gtab.T, ggain, loss[0, 0]


def solution(mesh):
    split = Mesh(mesh.devices.reshape(mesh.shape["dp"], mesh.shape["win"], 4, 2), DP_WIN_MP)
    return jax.shard_map(
        per_device,
        mesh=split,
        in_specs=(
            P(DP_WIN_MP, None), P(DP_WIN_MP, None), P(("dp", "win"), None), P(), P(),
            P(None, MP), P(None, MP, None), P(MP, None),
        ),
        out_specs=(
            P(DP_WIN_MP, None), P(None, MP, ("dp", "win")), P(MP, ("dp", "win")), P(None, MP), P(), P(),
        ),
        check_vma=False,
    )
```

```python
import functools

import jax
import jax.numpy as jnp
from jax import lax
from jax.experimental import pallas as pl
from jax.experimental.pallas import tpu as pltpu
from jax.sharding import Mesh
from jax.sharding import PartitionSpec as P

C = 768
HD = 32
WIN_TOK = 49
TABLE = 169
ENT = 176
F32 = jnp.float32
BF16 = jnp.bfloat16
MESH = pl.DeviceIdType.MESH
VM = pl.BlockSpec(memory_space=pltpu.VMEM)
MP = ("x", "core")
DP_WIN_MP = ("dp", "win", "x", "core")
BIG = (0, C // 2)


def dot(a, b, ca, cb):
    return lax.dot_general(a, b, (((ca,), (cb,)), ((), ())), preferred_element_type=F32)


def onehot_rows(relp, p):
    rows = jnp.concatenate([relp[16 * a + p : 16 * a + p + 1, 0:64] for a in range(4)], axis=1)
    entry = lax.broadcasted_iota(jnp.int32, (ENT, 256), 0)
    return jnp.where(entry == rows, 1.0, 0.0).astype(BF16)


def shift(v, d, n):
    return lax.rem(v + (d % n), n)


def whole_kernel(count, *refs):
    (
        tok_hbm, tgt_hbm, reg_hbm, rel_hbm, gain_hbm, table_hbm, wqkv_hbm, wproj_hbm,
        gi_ref, gq_ref, gp_ref, gtab_ref, ggain_ref, loss_ref,
        tok_ref, tgt_ref, reg_ref, rel_ref, gain_ref, table_ref, tab_s, w_ref, t_ref,
        send_w, recv_x, recv_o, recv_n, send_c, recv_c, send_t, recv_t, own_sem,
        pad_s, x_s, t_s, xh_s, xn_s, xt_s, xtf_s, xtp_s, ysum_s, err_s, gb_s, dxn_s,
        relp_s, bt_s, bias_s, p_s, q_s, k_s, v_s, at_s, dsum_s, sm_ref,
        grads, sums, direct, cxf, s2, s2x, flat, a3, b3, x3, r3a, r3b, r3x, part_s, sm0, sm1, sm2, ss1, ss2,
        send_d, recv_d, send_v, recv_v, send_rx, recv_rx,
        send_2, recv_2, send_3, recv_3, send_s, recv_s,
    ) = refs
    z, y, x, c = (lax.axis_index(name) for name in DP_WIN_MP)
    mp = 2 * x + c
    scale = HD**-0.5
    shrink = count**-0.5
    partner = (z, y, x, 1 - c)
    talk = [partner] + [(z, y, shift(x, d, 4), core) for d in (1, 2, 3) for core in (c, 1 - c)]
    line_y = [(z, shift(y, d, 8), x, c) for d in range(1, 8)]
    line_z = [(shift(z, d, 8), y, x, c) for d in range(1, 8)]
    line_x = [(z, y, shift(x, d, 4), c) for d in range(1, 4)]
    def push(src, dst, ssem, rsem, to):
        pltpu.make_async_remote_copy(
            src_ref=src, dst_ref=dst, send_sem=ssem, recv_sem=rsem, device_id=to, device_id_type=MESH
        ).start()

    def landed(dst, rsem):
        pltpu.make_async_remote_copy(
            src_ref=dst, dst_ref=dst, send_sem=rsem, recv_sem=rsem, device_id=partner, device_id_type=MESH
        ).wait_recv()

    def left_here(amount, ssem):
        pltpu.make_async_remote_copy(
            src_ref=amount, dst_ref=amount, send_sem=ssem, recv_sem=ssem, device_id=partner, device_id_type=MESH
        ).wait_send()

    barrier = pltpu.get_barrier_semaphore()
    peers = talk + line_y + line_z
    peers += [to[:3] + (1 - c,) for to in line_y + line_z]
    for peer in peers:
        pl.semaphore_signal(barrier, inc=1, device_id=peer, device_id_type=MESH)

    load = [
        pltpu.make_async_copy(src, dst, own_sem.at[k])
        for k, (src, dst) in enumerate(
            (
                (tok_hbm, tok_ref), (wqkv_hbm.at[0], w_ref.at[x, 0, c]), (wqkv_hbm.at[1], w_ref.at[x, 1, c]),
                (wqkv_hbm.at[2], w_ref.at[x, 2, c]), (wproj_hbm, w_ref.at[x, 3, c]), (table_hbm, table_ref),
                (gain_hbm, gain_ref), (tgt_hbm, tgt_ref), (rel_hbm, rel_ref), (reg_hbm, reg_ref),
            )
        )
    ]
    for one in load:
        one.start()
    tab_s[...] = jnp.zeros_like(tab_s)
    load[5].wait()
    for h in range(3):
        tab_s[:, 256 * h : 256 * h + TABLE] = table_ref[h : h + 1, :]
    t_ref[mp] = tab_s[...]
    load[0].wait()
    load[6].wait()
    load[7].wait()
    x_s[...] = jnp.zeros_like(x_s)
    t_s[...] = jnp.zeros_like(t_s)
    pad_s[0:147, :] = tok_ref[...].astype(F32)
    for w in range(3):
        x_s[64 * w : 64 * w + 49, :] = pad_s[49 * w : 49 * w + 49, :]
    pad_s[0:147, :] = tgt_ref[...].astype(F32)
    for w in range(3):
        t_s[64 * w : 64 * w + 49, :] = pad_s[49 * w : 49 * w + 49, :]
    xx = x_s[...]
    mean = jnp.sum(xx, axis=1, keepdims=True) * (1.0 / C)
    cen = xx - mean
    var = jnp.sum(cen * cen, axis=1, keepdims=True) * (1.0 / C)
    inv = lax.rsqrt(var + 1e-05)
    xh_s[...] = cen * inv
    xn_s[...] = (xh_s[...] * gain_ref[...].reshape(1, C)).astype(BF16)

    pl.semaphore_wait(barrier, len(peers))

    colors = (lax.rem(y + 2 * z, 4), lax.rem(z + 2 * y, 4))
    near_y = [(z, shift(y, d, 8), x, c) for d in (1, -1)]
    near_z = [(shift(z, d, 8), y, x, c) for d in (1, -1)]
    strong = (near_y, near_z)
    weak = (near_z, near_y)

    def rows_of(m):
        return pl.ds(48 * m, 48)

    def piece(xs, tint, core, m):
        return w_ref.at[xs, tint, core, rows_of(m)]

    def lanes(xs, tint, core, m, j):
        return w_ref.at[xs, tint, core, rows_of(m), pl.ds(BIG[j], C // 2)]

    for to in talk:
        push(tab_s, t_ref.at[mp], send_t.at[0], recv_t.at[0], to)
    for k in range(1, 5):
        load[k].wait()
    for m in range(2):
        for j, d in enumerate((1, -1)):
            there = piece(x, colors[m], c, m)
            push(there, there, send_w.at[0], recv_x.at[m], (z, y, shift(x, d, 4), c))
    for one in range(4):
        there = w_ref.at[x, one, c]
        push(there, there, send_c.at[0], recv_c.at[3], partner)
    load[8].wait()
    load[9].wait()

    xt = jnp.transpose(xn_s[...].astype(F32))
    xt_s[:, 0:192] = xt.astype(BF16)
    xtf_s[...] = xt
    for b in range(8):
        block = jnp.concatenate([xtf_s[96 * k + 12 * b : 96 * k + 12 * b + 12, :] for k in range(8)], axis=0)
        xtp_s[96 * b : 96 * b + 96, 0:192] = block.astype(BF16)
    relp_s[...] = jnp.full(relp_s.shape, -1, jnp.int32)
    relp_s[0:49, 0:49] = rel_ref[...]
    relp = relp_s[...]
    regs = jnp.concatenate(
        [reg_ref[pl.ds(3 * mp + w, 1), :].astype(F32) for w in range(3)] + [jnp.zeros((5, 49), F32)], axis=0
    )
    regs = jnp.concatenate([regs, jnp.zeros((8, 15), F32)], axis=1)
    lane = lax.broadcasted_iota(jnp.int32, (64, 384), 1)
    query_of = (lane // 96) * 16 + lane % 16
    pick = jnp.where(lax.broadcasted_iota(jnp.int32, (64, 384), 0) == query_of, 1.0, 0.0)
    reg_q = dot(regs, pick, 1, 0)
    eye = jnp.where(
        lax.broadcasted_iota(jnp.int32, (64, 64), 0) == lax.broadcasted_iota(jnp.int32, (64, 64), 1), 1.0, 0.0
    )
    reg_k = dot(eye, regs, 1, 1)
    row = lax.broadcasted_iota(jnp.int32, (96, 192), 0)
    col = lax.broadcasted_iota(jnp.int32, (96, 192), 1)
    own = jnp.where(row // 16 == col // 32, 1.0, 0.0)
    own_bf = own.astype(BF16)

    left, right, opposite = shift(x, -1, 4), shift(x, 1, 4), shift(x, 2, 4)
    sources = (left, right, opposite)

    def hand_on(slot, m):
        xs = sources[slot]
        tint = colors[m]
        for j in range(2):
            push(piece(xs, tint, c, m), piece(xs, tint, c, m), send_w.at[0], recv_n.at[slot], strong[m][j])
        for j in range(2):
            push(lanes(xs, tint, c, m, j), lanes(xs, tint, c, m, j), send_w.at[0], recv_n.at[slot], weak[m][j])
        push(piece(xs, tint, c, m), piece(xs, tint, c, m), send_c.at[0], recv_c.at[slot], partner)

    def from_sides(m):
        landed(w_ref.at[left, 0, c], recv_x.at[m])
        there = piece(sources[m], colors[m], c, m)
        push(there, there, send_w.at[0], recv_o.at[m], (z, y, shift(x, 1 - 2 * m, 4), c))
        hand_on(0, m)

    landed(t_ref.at[pl.ds(0, 7)], recv_t.at[0])
    tab = jnp.concatenate(
        [t_ref[g, 0:1, 256 * h : 256 * h + ENT] for g in range(8) for h in range(3)], axis=0
    )
    hi = tab.astype(BF16)
    rest = tab - hi.astype(F32)
    mid = rest.astype(BF16)
    low = (rest - mid.astype(F32)).astype(BF16)
    zero8 = jnp.zeros((8, ENT), F32)
    parts = jnp.concatenate(
        [t for one in (hi, mid, low) for t in (one.astype(F32), zero8)], axis=0
    ).astype(BF16)
    for p in range(16):
        got = dot(parts, onehot_rows(relp, p), 1, 0)
        got = got[0:24] + got[32:56] + got[64:88]
        bt_s.at[0][pl.ds(p, 24, stride=16), :] = got[:, 0:128]
        bt_s.at[1][pl.ds(p, 24, stride=16), :] = got[:, 128:256]
    keypad = jnp.where(lax.broadcasted_iota(jnp.int32, (64, 384), 0) < WIN_TOK, 0.0, -1e30)
    for i in range(4):
        turned = [jnp.transpose(bt_s[j, 96 * i : 96 * i + 96, :]) for j in range(2)]
        turned = [t[64 * a : 64 * a + 64] for t in turned for a in range(2)]
        bias_s[i] = jnp.concatenate(turned, axis=1) + keypad

    def shift_mask(w):
        return jnp.where(reg_k[:, w : w + 1] == reg_q[w : w + 1, :], 0.0, -100.0)

    def spread(block):
        return jnp.concatenate(
            [jnp.concatenate([block[16 * a : 16 * a + 16]] * 6, axis=0) * own_bf for a in range(4)], axis=0
        )

    def collapse(big):
        out = []
        for a in range(4):
            part = big[96 * a : 96 * a + 96] * own
            out.append(sum(part[16 * h : 16 * h + 16] for h in range(6)))
        return jnp.concatenate(out, axis=0)

    def weight(xs, t):
        return w_ref[xs, t].reshape(192, C)

    def forward(i, xs, first):
        xn = xn_s[...]
        q_s[i] = (dot(xn, weight(xs, 0), 1, 1) * scale).astype(BF16)
        k_s[i] = dot(xn, weight(xs, 1), 1, 1).astype(BF16)
        v_s[i] = dot(xn, weight(xs, 2), 1, 1).astype(BF16)
        for w in range(3):
            rows = slice(64 * w, 64 * w + 64)
            sc = dot(k_s[i, rows, :], spread(q_s[i, rows, :]), 1, 1)
            sc = sc + bias_s[xs] + shift_mask(w)
            ex = jnp.exp(sc - jnp.max(sc, axis=0, keepdims=True))
            pr = ex / jnp.sum(ex, axis=0, keepdims=True)
            p_s[i, w] = pr
            at_s[i, rows, :] = collapse(dot(pr.astype(BF16), v_s[i, rows, :], 0, 0)).astype(BF16)
        part = dot(at_s[i], weight(xs, 3), 1, 0)
        ysum_s[...] = part if first else ysum_s[...] + part

    order = (opposite, right, left, x)

    def near_tints(m):
        return [lax.rem(colors[m] + d, 4) for d in (3, 1)], lax.rem(colors[m] + 2, 4)

    def hand_over(slot):
        xs = sources[slot]
        landed(w_ref.at[xs, pl.ds(0, 3), c], recv_n.at[slot])
        for m in range(2):
            tints, across = near_tints(m)
            for j in range(2):
                there = piece(xs, tints[j], c, m)
                push(there, there, send_c.at[0], recv_c.at[slot], partner)
            for j in range(2):
                there = lanes(xs, across, c, m, j)
                push(there, there, send_c.at[0], recv_c.at[slot], partner)

    def whole_slot(slot):
        landed(w_ref.at[sources[slot], :, 1 - c], recv_c.at[slot])

    from_sides(0)
    from_sides(1)
    hand_on(1, 0)
    hand_on(1, 1)
    landed(w_ref.at[x, :, 1 - c], recv_c.at[3])
    forward(3, x, True)
    for m in range(2):
        landed(piece(opposite, colors[m], c, m), recv_o.at[m])
        hand_on(2, m)
    hand_over(0)
    hand_over(1)
    whole_slot(0)
    forward(2, left, False)
    hand_over(2)
    whole_slot(1)
    forward(1, right, False)
    whole_slot(2)
    forward(0, opposite, False)

    rowid = lax.broadcasted_iota(jnp.int32, (192, C), 0) % 64
    err = jnp.where(rowid < WIN_TOK, x_s[...] + ysum_s[...] - t_s[...], 0.0)
    err_s[...] = err
    gb_s[...] = err.astype(BF16)
    turned = jnp.transpose(err)
    xt_s[:, 192:384] = turned.astype(BF16)
    xtf_s[...] = turned
    for b in range(8):
        block = jnp.concatenate([xtf_s[96 * k + 12 * b : 96 * k + 12 * b + 12, :] for k in range(8)], axis=0)
        xtp_s[96 * b : 96 * b + 96, 192:384] = block.astype(BF16)

    def backward(i, first, middle):
        xs = order[i]
        datt = dot(gb_s[...], weight(xs, 3), 1, 1).astype(BF16)
        dqs, dks, dvs = [], [], []
        total = jnp.zeros((64, 384), F32)
        for w in range(3):
            rows = slice(64 * w, 64 * w + 64)
            da = spread(datt[rows])
            dp = dot(v_s[i, rows, :], da, 1, 1)
            pr = p_s[i, w]
            ds = pr * (dp - jnp.sum(pr * dp, axis=0, keepdims=True))
            total = total + ds
            db = ds.astype(BF16)
            dvs.append(dot(pr.astype(BF16), da, 1, 0))
            dks.append(dot(db, spread(q_s[i, rows, :]), 1, 0))
            dqs.append(collapse(dot(db, k_s[i, rows, :], 0, 0)) * scale)
        turned = [jnp.transpose(total[:, 96 * a : 96 * a + 96]) for a in range(4)]
        here = pl.ds(pl.multiple_of(96 * xs, 96), 96)
        dsum_s[0, here, :] = jnp.concatenate(turned[0:2], axis=1)
        dsum_s[1, here, :] = jnp.concatenate(turned[2:4], axis=1)
        dq = jnp.concatenate(dqs, axis=0)
        dk = jnp.concatenate(dks, axis=0)
        dv = jnp.concatenate(dvs, axis=0)
        dqb, dkb, dvb = dq.astype(BF16), dk.astype(BF16), dv.astype(BF16)
        middle()
        lead = jnp.concatenate([dqb[:, 0:128], dvb[:, 0:128]], axis=1)
        low_half = jnp.concatenate([dq[:, 128:192], dk], axis=1).astype(BF16)
        zeros = jnp.zeros((192, 64), F32)
        att = at_s[i].astype(F32)
        mixed = jnp.concatenate(
            [
                jnp.concatenate([dv[:, 128:192], zeros], axis=1),
                jnp.concatenate([zeros, att[:, 0:64]], axis=1),
            ],
            axis=0,
        ).astype(BF16)
        last = att[:, 64:192].astype(BF16)
        for b in range(8):
            rows = slice(96 * b, 96 * b + 96)
            one = dot(xtp_s[rows, 0:192], lead, 1, 0).astype(BF16)
            grads[0, 0, i, b] = one[:, 0:128]
            grads[0, 1, i, b] = one[:, 128:256]
            two = dot(xt_s[rows, 0:192], low_half, 1, 0).astype(BF16)
            grads[2, 0, i, b] = two[:, 0:128]
            grads[1, 0, i, b] = two[:, 128:256]
            grads[2, 1, i, b] = dot(xtp_s[rows, :], mixed, 1, 0).astype(BF16)
            grads[1, 1, i, b] = dot(xt_s[rows, 192:384], last, 1, 0).astype(BF16)
        for num in range(3):
            push(grads.at[num, 1 - c, i], sums.at[num, i], send_d.at[0], recv_d.at[i], partner)
        part = (
            dot(dqb, weight(xs, 0), 1, 0) + dot(dkb, weight(xs, 1), 1, 0) + dot(dvb, weight(xs, 2), 1, 0)
        )
        dxn_s[...] = part if first else dxn_s[...] + part

    lines = (
        (0, y, lambda d: (z, shift(y, d, 8), x, c)),
        (1, z, lambda d: (shift(z, d, 8), y, x, c)),
    )
    far_first = (4, 3, 5, 2, 6, 1, 7)

    def take(i):
        landed(sums.at[:, i], recv_d.at[i])
        for num in range(3):
            for b in range(8):
                sums[num, i, b] = sums[num, i, b] + grads[num, c, i, b]
        if i < 3:
            push(sums.at[2, i], cxf.at[i], send_rx.at[0], recv_rx.at[0], (z, y, order[i], c))
        for d in far_first:
            for num, me, reach in lines:
                push(sums.at[num, i, shift(me, d, 8)], direct.at[num, i, d - 1], send_v.at[0], recv_v.at[i], reach(d))

    def finish(i):
        landed(direct.at[:, i], recv_v.at[i])
        for num, me, reach in lines:
            total = sums[num, i, me].astype(F32)
            for d in range(1, 8):
                total = total + direct[num, i, d - 1].astype(F32)
            sums[num, i, me] = total.astype(BF16)
            if i < 3:
                push(sums.at[num, i, me], s2.at[num, i], send_2.at[0], recv_2.at[0], (z, y, order[i], c))

    backward(0, True, lambda: None)
    backward(1, False, lambda: take(0))
    backward(2, False, lambda: take(1))
    backward(3, False, lambda: take(2))

    dxn = dxn_s[...]
    xhat = xh_s[...]
    dxh = dxn * gain_ref[...].reshape(1, C)
    m1 = jnp.sum(dxh, axis=1, keepdims=True) * (1.0 / C)
    m2 = jnp.sum(dxh * xhat, axis=1, keepdims=True) * (1.0 / C)
    out = err_s[...] + inv * (dxh - m1 - xhat * m2)
    for w in range(3):
        gi_ref[49 * w : 49 * w + 49, :] = out[64 * w : 64 * w + 49, :]
    gain = jnp.sum(dxn * xhat, axis=0, keepdims=True)
    sq = err_s[...]
    loss = jnp.sum(sq * sq, axis=0, keepdims=True)
    loss = sum(loss[:, 128 * j : 128 * j + 128] for j in range(6))
    loss = jnp.sum(loss, axis=1, keepdims=True) + jnp.zeros((1, 128), F32)
    tail = jnp.concatenate(
        [gain[:, 128 * j : 128 * j + 128] for j in range(6)] + [loss, jnp.zeros((1, 128), F32)], axis=0
    )

    dtab = jnp.zeros((64, ENT), F32)
    for p in range(16):
        ds = jnp.concatenate([dsum_s.at[j][pl.ds(p, 24, stride=16), :] for j in range(2)], axis=1)
        top = ds.astype(BF16)
        rem = (ds - top.astype(F32)).astype(BF16)
        z8 = jnp.zeros((8, 256), F32)
        both = jnp.concatenate([top.astype(F32), z8, rem.astype(F32), z8], axis=0).astype(BF16)
        dtab = dtab + dot(both, onehot_rows(relp, p), 1, 1)
    dtab = dtab[0:24] + dtab[32:56]
    for g in range(8):
        sm_ref[g] = jnp.zeros((8, 384), F32)
        sm_ref[g, 0:3, 0:ENT] = dtab[3 * g : 3 * g + 3]
        sm_ref[g, :, 256:384] = tail
    for j, peer in enumerate(talk):
        push(sm_ref.at[2 * peer[2] + peer[3]], sm0.at[j], send_s.at[0], recv_s.at[0], peer)

    take(3)
    finish(0)
    first_x = z * (1 - c) + y * c
    then_x = y * (1 - c) + z * c
    landed(cxf, recv_rx.at[0])
    for b in range(8):
        total = sums[2, 3, b].astype(F32)
        for i in range(3):
            total = total + cxf[i, b].astype(F32)
        sums[2, 3, b] = total.astype(BF16)
    for d in far_first:
        to = (lax.rem(z + d * (1 - c), 8), lax.rem(y + d * c, 8), x, c)
        push(sums.at[2, 3, shift(first_x, d, 8)], s2x.at[d - 1], send_2.at[1], recv_2.at[1], to)
    finish(1)
    landed(sm0, recv_s.at[0])
    ss1[...] = sm_ref[mp] + sum(sm0[j] for j in range(7))
    for j, to in enumerate(line_y):
        push(ss1, sm1.at[j], send_s.at[1], recv_s.at[1], to)
    finish(2)
    finish(3)

    a3[...] = jnp.zeros_like(a3)
    b3[...] = jnp.zeros_like(b3)
    x3[...] = jnp.zeros_like(x3)

    def collect(num, me):
        total = sums[num, 3, me].astype(F32)
        for i in range(3):
            total = total + s2[num, i].astype(F32)
        flat[num] = total

    def spread_out(src, me, dst, num, reach):
        for d in (4, 3, 5, 2, 6, 1, 7, 0):
            for k, core in enumerate((c, 1 - c)):
                if d or k:
                    push(src.at[shift(me, d, 8)], dst.at[8 * k + d - 1], send_3.at[num], recv_3.at[num], reach(d, core))

    def gathered(src, me, dst, k):
        total = src[me] if k == 0 else dst[7]
        for d in range(1, 8):
            total = total + dst[8 * k + d - 1]
        return total

    landed(s2, recv_2.at[0])
    collect(0, y)
    for i in range(8):
        a3[i, 0:12, :] = flat[0, 12 * i : 12 * i + 12, :]
    spread_out(a3, z, r3a, 0, lambda d, core: (shift(z, d, 8), y, x, core))
    collect(1, z)
    for i in range(8):
        b3[i, 0:12, :] = flat[1, 12 * i : 12 * i + 12, :]
    spread_out(b3, y, r3b, 1, lambda d, core: (z, shift(y, d, 8), x, core))
    landed(s2x, recv_2.at[1])
    total = sums[2, 3, first_x].astype(F32)
    for j in range(7):
        total = total + s2x[j].astype(F32)
    flat[2] = total
    for i in range(8):
        x3[i, 0:12, :] = flat[2, 12 * i : 12 * i + 12, :]
    spread_out(
        x3, then_x, r3x, 2, lambda d, core: (lax.rem(z + d * c, 8), lax.rem(y + d * (1 - c), 8), x, core)
    )

    landed(sm1, recv_s.at[1])
    ss2[...] = ss1[...] + sum(sm1[j] for j in range(7))
    for j, to in enumerate(line_z):
        push(ss2, sm2.at[j], send_s.at[2], recv_s.at[2], to)
    landed(r3a, recv_3.at[0])
    for k, core in enumerate((c, 1 - c)):
        part_s[core, :, 0:128] = gathered(a3, z, r3a, k)
    landed(r3b, recv_3.at[1])
    for k, core in enumerate((c, 1 - c)):
        part_s[core, :, 256:384] = gathered(b3, y, r3b, k)
    landed(r3x, recv_3.at[2])
    for k, core in enumerate((c, 1 - c)):
        part_s[core, :, 128:256] = gathered(x3, then_x, r3x, k)
    for t in range(4):
        at = 192 * (t % 2)
        both = part_s[t // 2, 0:12, :] * shrink
        mine = jnp.where(c == 0, both[:, at : at + 96], both[:, at + 96 : at + 192])
        if t < 3:
            gq_ref[t] = mine
        else:
            gp_ref[...] = mine
    landed(sm2, recv_s.at[2])
    total = ss2[...] + sum(sm2[j] for j in range(7))
    gtab_ref[...] = total[0:3, 0:TABLE] * shrink
    for j in range(6):
        ggain_ref[pl.ds(128 * j, 128)] = total[j : j + 1, 256:384].reshape(128) * shrink
    loss_ref[...] = total[6:7, 256:384] * (0.5 / count)
    left_here(w_ref.at[:, pl.ds(0, 3), 0], send_w.at[0])
    left_here(w_ref.at[:, :, 0], send_c.at[0])
    left_here(t_ref.at[pl.ds(0, 7)], send_t.at[0])
    left_here(grads.at[:, 0], send_d.at[0])
    left_here(grads.at[0, :, :, pl.ds(0, 7)], send_v.at[0])
    left_here(cxf, send_rx.at[0])
    left_here(s2, send_2.at[0])
    left_here(s2x, send_2.at[1])
    left_here(r3a, send_3.at[0])
    left_here(r3b, send_3.at[1])
    left_here(r3x, send_3.at[2])
    for k, amount in enumerate((sm0, sm1, sm2)):
        left_here(amount, send_s.at[k])


def whole(count, *args):
    dma = pltpu.SemaphoreType.DMA
    f = lambda *s: pltpu.VMEM(s, F32)
    b = lambda *s: pltpu.VMEM(s, BF16)
    shape = jax.ShapeDtypeStruct
    return pl.pallas_call(
        functools.partial(whole_kernel, count),
        name="window_layer",
        out_shape=(
            shape((147, C), F32), shape((3, 12, 96), F32), shape((12, 96), F32),
            shape((3, TABLE), F32), shape((C,), F32), shape((1, 128), F32),
        ),
        in_specs=[pl.BlockSpec(memory_space=pltpu.HBM)] * 8,
        out_specs=(VM,) * 6,
        scratch_shapes=[
            b(147, C), b(147, C), pltpu.VMEM((24, 49), jnp.int32), pltpu.VMEM((49, 49), jnp.int32), f(C), f(3, TABLE),
            f(1, C), b(4, 4, 2, 96, C), f(8, 1, C),
            dma((1,)), dma((2,)), dma((2,)), dma((3,)), dma((1,)), dma((4,)), dma((1,)), dma((1,)), dma((10,)),
            f(152, C), f(192, C), f(192, C), f(192, C), b(192, C), b(C, 384), f(C, 192), b(C, 384),
            f(192, C), f(192, C), b(192, C), f(192, C),
            pltpu.VMEM((64, 128), jnp.int32), f(2, 384, 128), f(4, 64, 384), f(4, 3, 64, 384),
            b(4, 192, 192), b(4, 192, 192), b(4, 192, 192), b(4, 192, 192), f(2, 384, 128), f(8, 8, 384),
            b(3, 2, 4, 8, 96, 128), b(3, 4, 8, 96, 128), b(2, 4, 7, 96, 128),
            b(3, 8, 96, 128), b(2, 3, 96, 128), b(7, 96, 128), f(3, 96, 128),
            f(8, 16, 128), f(8, 16, 128), f(8, 16, 128), f(15, 16, 128), f(15, 16, 128), f(15, 16, 128),
            f(2, 16, 384),
            f(7, 8, 384), f(7, 8, 384), f(7, 8, 384), f(8, 384), f(8, 384),
            dma((1,)), dma((4,)), dma((1,)), dma((4,)), dma((1,)), dma((1,)),
            dma((2,)), dma((2,)), dma((3,)), dma((3,)), dma((3,)), dma((3,)),
        ],
        compiler_params=pltpu.CompilerParams(
            collective_id=0, has_side_effects=True, vmem_limit_bytes=40 * 2**20
        ),
    )(*args)


def hand_out_kernel(*refs):
    copies = [pltpu.make_async_copy(refs[k], refs[6 + k], refs[12].at[k]) for k in range(6)]
    for copy in copies:
        copy.start()
    for copy in copies:
        copy.wait()


def hand_out(*arrays):
    return pl.pallas_call(
        hand_out_kernel,
        name="hand_out",
        out_shape=tuple(jax.ShapeDtypeStruct(a.shape, a.dtype) for a in arrays),
        in_specs=[VM] * 6,
        out_specs=(pl.BlockSpec(memory_space=pl.ANY),) * 6,
        scratch_shapes=[pltpu.SemaphoreType.DMA((6,))],
        compiler_params=pltpu.CompilerParams(vmem_limit_bytes=8 * 2**20),
    )(*arrays)


def per_device(tokens, target, regions, rel_index, layer_norm_gain, bias_table, w_qkv, w_proj):
    count = tokens.shape[0] * lax.axis_size(DP_WIN_MP)
    args = (tokens, target, regions, rel_index, layer_norm_gain, bias_table.T, w_qkv, w_proj)
    done = whole(count, *[pltpu.with_memory_space_constraint(one, pltpu.HBM) for one in args])
    gi, gq, gp, gtab, ggain, loss = hand_out(*done)
    return gi, jnp.transpose(gq, (0, 2, 1)), gp.T, gtab.T, ggain, loss[0, 0]


def solution(mesh):
    split = Mesh(mesh.devices.reshape(mesh.shape["dp"], mesh.shape["win"], 4, 2), DP_WIN_MP)
    return jax.shard_map(
        per_device,
        mesh=split,
        in_specs=(
            P(DP_WIN_MP, None), P(DP_WIN_MP, None), P(("dp", "win"), None), P(), P(),
            P(None, MP), P(None, MP, None), P(MP, None),
        ),
        out_specs=(
            P(DP_WIN_MP, None), P(None, MP, ("dp", "win")), P(MP, ("dp", "win")), P(None, MP), P(), P(),
        ),
        check_vma=False,
    )
```

```python
import functools

import jax
import jax.numpy as jnp
from jax import lax
from jax.experimental import pallas as pl
from jax.experimental.pallas import tpu as pltpu
from jax.sharding import Mesh
from jax.sharding import PartitionSpec as P

C = 768
HD = 32
WIN_TOK = 49
TABLE = 169
ENT = 176
F32 = jnp.float32
BF16 = jnp.bfloat16
MESH = pl.DeviceIdType.MESH
VM = pl.BlockSpec(memory_space=pltpu.VMEM)
MP = ("x", "core")
DP_WIN_MP = ("dp", "win", "x", "core")
BIG = (0, C // 2)


def dot(a, b, ca, cb):
    return lax.dot_general(a, b, (((ca,), (cb,)), ((), ())), preferred_element_type=F32)


def onehot_rows(relp, p):
    rows = jnp.concatenate([relp[16 * a + p : 16 * a + p + 1, 0:64] for a in range(4)], axis=1)
    entry = lax.broadcasted_iota(jnp.int32, (ENT, 256), 0)
    return jnp.where(entry == rows, 1.0, 0.0).astype(BF16)


def shift(v, d, n):
    return lax.rem(v + (d % n), n)


def whole_kernel(count, *refs):
    (
        tok_hbm, tgt_hbm, reg_hbm, rel_hbm, gain_hbm, table_hbm, wqkv_hbm, wproj_hbm,
        gi_ref, gq_ref, gp_ref, gtab_ref, ggain_ref, loss_ref,
        tok_ref, tgt_ref, reg_ref, rel_ref, gain_ref, table_ref, tab_s, w_ref, t_ref,
        send_w, recv_x, recv_o, recv_n, send_c, recv_c, send_t, recv_t, own_sem,
        pad_s, x_s, t_s, xh_s, xn_s, xt_s, xtf_s, xtp_s, ysum_s, err_s, gb_s, dxn_s,
        relp_s, bt_s, bias_s, p_s, q_s, k_s, v_s, at_s, dsum_s, sm_ref,
        grads, sums, direct, cxf, s2, s2x, flat, a3, b3, x3, r3a, r3b, r3x, part_s, sm0, sm1, sm2, ss1, ss2,
        send_d, recv_d, send_v, recv_v, send_rx, recv_rx,
        send_2, recv_2, send_3, recv_3, send_s, recv_s,
    ) = refs
    z, y, x, c = (lax.axis_index(name) for name in DP_WIN_MP)
    mp = 2 * x + c
    scale = HD**-0.5
    shrink = count**-0.5
    partner = (z, y, x, 1 - c)
    talk = [partner] + [(z, y, shift(x, d, 4), core) for d in (1, 2, 3) for core in (c, 1 - c)]
    line_y = [(z, shift(y, d, 8), x, c) for d in range(1, 8)]
    line_z = [(shift(z, d, 8), y, x, c) for d in range(1, 8)]
    line_x = [(z, y, shift(x, d, 4), c) for d in range(1, 4)]
    def push(src, dst, ssem, rsem, to):
        pltpu.make_async_remote_copy(
            src_ref=src, dst_ref=dst, send_sem=ssem, recv_sem=rsem, device_id=to, device_id_type=MESH
        ).start()

    def landed(dst, rsem):
        pltpu.make_async_remote_copy(
            src_ref=dst, dst_ref=dst, send_sem=rsem, recv_sem=rsem, device_id=partner, device_id_type=MESH
        ).wait_recv()

    def left_here(amount, ssem):
        pltpu.make_async_remote_copy(
            src_ref=amount, dst_ref=amount, send_sem=ssem, recv_sem=ssem, device_id=partner, device_id_type=MESH
        ).wait_send()

    barrier = pltpu.get_barrier_semaphore()
    peers = talk + line_y + line_z
    peers += [to[:3] + (1 - c,) for to in line_y + line_z]
    for peer in peers:
        pl.semaphore_signal(barrier, inc=1, device_id=peer, device_id_type=MESH)

    load = [
        pltpu.make_async_copy(src, dst, own_sem.at[k])
        for k, (src, dst) in enumerate(
            (
                (tok_hbm, tok_ref), (wqkv_hbm.at[0], w_ref.at[x, 0, c]), (wqkv_hbm.at[1], w_ref.at[x, 1, c]),
                (wqkv_hbm.at[2], w_ref.at[x, 2, c]), (wproj_hbm, w_ref.at[x, 3, c]), (table_hbm, table_ref),
                (gain_hbm, gain_ref), (tgt_hbm, tgt_ref), (rel_hbm, rel_ref), (reg_hbm, reg_ref),
            )
        )
    ]
    for one in load:
        one.start()
    tab_s[...] = jnp.zeros_like(tab_s)
    load[5].wait()
    for h in range(3):
        tab_s[:, 256 * h : 256 * h + TABLE] = table_ref[h : h + 1, :]
    t_ref[mp] = tab_s[...]
    load[0].wait()
    load[6].wait()
    load[7].wait()
    x_s[...] = jnp.zeros_like(x_s)
    t_s[...] = jnp.zeros_like(t_s)
    pad_s[0:147, :] = tok_ref[...].astype(F32)
    for w in range(3):
        x_s[64 * w : 64 * w + 49, :] = pad_s[49 * w : 49 * w + 49, :]
    pad_s[0:147, :] = tgt_ref[...].astype(F32)
    for w in range(3):
        t_s[64 * w : 64 * w + 49, :] = pad_s[49 * w : 49 * w + 49, :]
    xx = x_s[...]
    mean = jnp.sum(xx, axis=1, keepdims=True) * (1.0 / C)
    cen = xx - mean
    var = jnp.sum(cen * cen, axis=1, keepdims=True) * (1.0 / C)
    inv = lax.rsqrt(var + 1e-05)
    xh_s[...] = cen * inv
    xn_s[...] = (xh_s[...] * gain_ref[...].reshape(1, C)).astype(BF16)

    pl.semaphore_wait(barrier, len(peers))

    colors = (lax.rem(y + 2 * z, 4), lax.rem(z + 2 * y, 4))
    near_y = [(z, shift(y, d, 8), x, c) for d in (1, -1)]
    near_z = [(shift(z, d, 8), y, x, c) for d in (1, -1)]
    strong = (near_y, near_z)
    weak = (near_z, near_y)

    def rows_of(m):
        return pl.ds(48 * m, 48)

    def piece(xs, tint, core, m):
        return w_ref.at[xs, tint, core, rows_of(m)]

    def lanes(xs, tint, core, m, j):
        return w_ref.at[xs, tint, core, rows_of(m), pl.ds(BIG[j], C // 2)]

    for to in talk:
        push(tab_s, t_ref.at[mp], send_t.at[0], recv_t.at[0], to)
    for k in range(1, 5):
        load[k].wait()
    for m in range(2):
        for j, d in enumerate((1, -1)):
            there = piece(x, colors[m], c, m)
            push(there, there, send_w.at[0], recv_x.at[m], (z, y, shift(x, d, 4), c))
    for one in range(4):
        there = w_ref.at[x, one, c]
        push(there, there, send_c.at[0], recv_c.at[3], partner)
    load[8].wait()
    load[9].wait()

    xt = jnp.transpose(xn_s[...].astype(F32))
    xt_s[:, 0:192] = xt.astype(BF16)
    xtf_s[0:C, :] = xt
    for b in range(8):
        block = jnp.concatenate([xtf_s[96 * k + 12 * b : 96 * k + 12 * b + 12, :] for k in range(8)], axis=0)
        xtp_s[96 * b : 96 * b + 96, 0:192] = block.astype(BF16)
    relp_s[...] = jnp.full(relp_s.shape, -1, jnp.int32)
    relp_s[0:49, 0:49] = rel_ref[...]
    relp = relp_s[...]
    regs = jnp.concatenate(
        [reg_ref[pl.ds(3 * mp + w, 1), :].astype(F32) for w in range(3)] + [jnp.zeros((5, 49), F32)], axis=0
    )
    regs = jnp.concatenate([regs, jnp.zeros((8, 15), F32)], axis=1)
    lane = lax.broadcasted_iota(jnp.int32, (64, 384), 1)
    query_of = (lane // 96) * 16 + lane % 16
    pick = jnp.where(lax.broadcasted_iota(jnp.int32, (64, 384), 0) == query_of, 1.0, 0.0)
    reg_q = dot(regs, pick, 1, 0)
    eye = jnp.where(
        lax.broadcasted_iota(jnp.int32, (64, 64), 0) == lax.broadcasted_iota(jnp.int32, (64, 64), 1), 1.0, 0.0
    )
    reg_k = dot(eye, regs, 1, 1)
    row = lax.broadcasted_iota(jnp.int32, (96, 192), 0)
    col = lax.broadcasted_iota(jnp.int32, (96, 192), 1)
    own = jnp.where(row // 16 == col // 32, 1.0, 0.0)
    own_bf = own.astype(BF16)

    left, right, opposite = shift(x, -1, 4), shift(x, 1, 4), shift(x, 2, 4)
    sources = (left, right, opposite)

    def hand_on(slot, m):
        xs = sources[slot]
        tint = colors[m]
        for j in range(2):
            push(piece(xs, tint, c, m), piece(xs, tint, c, m), send_w.at[0], recv_n.at[slot], strong[m][j])
        for j in range(2):
            push(lanes(xs, tint, c, m, j), lanes(xs, tint, c, m, j), send_w.at[0], recv_n.at[slot], weak[m][j])
        push(piece(xs, tint, c, m), piece(xs, tint, c, m), send_c.at[0], recv_c.at[slot], partner)

    def from_sides(m):
        landed(w_ref.at[left, 0, c], recv_x.at[m])
        there = piece(sources[m], colors[m], c, m)
        push(there, there, send_w.at[0], recv_o.at[m], (z, y, shift(x, 1 - 2 * m, 4), c))
        hand_on(0, m)

    landed(t_ref.at[pl.ds(0, 7)], recv_t.at[0])
    tab = jnp.concatenate(
        [t_ref[g, 0:1, 256 * h : 256 * h + ENT] for g in range(8) for h in range(3)], axis=0
    )
    hi = tab.astype(BF16)
    rest = tab - hi.astype(F32)
    mid = rest.astype(BF16)
    low = (rest - mid.astype(F32)).astype(BF16)
    zero8 = jnp.zeros((8, ENT), F32)
    parts = jnp.concatenate(
        [t for one in (hi, mid, low) for t in (one.astype(F32), zero8)], axis=0
    ).astype(BF16)
    for p in range(16):
        got = dot(parts, onehot_rows(relp, p), 1, 0)
        got = got[0:24] + got[32:56] + got[64:88]
        bt_s.at[0][pl.ds(p, 24, stride=16), :] = got[:, 0:128]
        bt_s.at[1][pl.ds(p, 24, stride=16), :] = got[:, 128:256]
    keypad = jnp.where(lax.broadcasted_iota(jnp.int32, (64, 384), 0) < WIN_TOK, 0.0, -1e30)
    for i in range(4):
        turned = [jnp.transpose(bt_s[j, 96 * i : 96 * i + 96, :]) for j in range(2)]
        turned = [t[64 * a : 64 * a + 64] for t in turned for a in range(2)]
        bias_s[i] = jnp.concatenate(turned, axis=1) + keypad

    def shift_mask(w):
        return jnp.where(reg_k[:, w : w + 1] == reg_q[w : w + 1, :], 0.0, -100.0)

    def spread(block):
        return jnp.concatenate(
            [jnp.concatenate([block[16 * a : 16 * a + 16]] * 6, axis=0) * own_bf for a in range(4)], axis=0
        )

    def collapse(big):
        out = []
        for a in range(4):
            part = big[96 * a : 96 * a + 96] * own
            out.append(sum(part[16 * h : 16 * h + 16] for h in range(6)))
        return jnp.concatenate(out, axis=0)

    def weight(xs, t):
        return w_ref[xs, t].reshape(192, C)

    def forward(i, xs, first):
        xn = xn_s[...]
        q_s[i] = (dot(xn, weight(xs, 0), 1, 1) * scale).astype(BF16)
        k_s[i] = dot(xn, weight(xs, 1), 1, 1).astype(BF16)
        v_s[i] = dot(xn, weight(xs, 2), 1, 1).astype(BF16)
        for w in range(3):
            rows = slice(64 * w, 64 * w + 64)
            sc = dot(k_s[i, rows, :], spread(q_s[i, rows, :]), 1, 1)
            sc = sc + bias_s[xs] + shift_mask(w)
            ex = jnp.exp(sc - jnp.max(sc, axis=0, keepdims=True))
            pr = ex / jnp.sum(ex, axis=0, keepdims=True)
            p_s[i, w] = pr
            at_s[i, rows, :] = collapse(dot(pr.astype(BF16), v_s[i, rows, :], 0, 0)).astype(BF16)
        part = dot(at_s[i], weight(xs, 3), 1, 0)
        ysum_s[...] = part if first else ysum_s[...] + part

    order = (opposite, right, left, x)

    def near_tints(m):
        return [lax.rem(colors[m] + d, 4) for d in (3, 1)], lax.rem(colors[m] + 2, 4)

    def hand_over(slot):
        xs = sources[slot]
        landed(w_ref.at[xs, pl.ds(0, 3), c], recv_n.at[slot])
        for m in range(2):
            tints, across = near_tints(m)
            for j in range(2):
                there = piece(xs, tints[j], c, m)
                push(there, there, send_c.at[0], recv_c.at[slot], partner)
            for j in range(2):
                there = lanes(xs, across, c, m, j)
                push(there, there, send_c.at[0], recv_c.at[slot], partner)

    def whole_slot(slot):
        landed(w_ref.at[sources[slot], :, 1 - c], recv_c.at[slot])

    from_sides(0)
    from_sides(1)
    hand_on(1, 0)
    hand_on(1, 1)
    landed(w_ref.at[x, :, 1 - c], recv_c.at[3])
    forward(3, x, True)
    for m in range(2):
        landed(piece(opposite, colors[m], c, m), recv_o.at[m])
        hand_on(2, m)
    hand_over(0)
    hand_over(1)
    whole_slot(0)
    forward(2, left, False)
    hand_over(2)
    whole_slot(1)
    forward(1, right, False)
    whole_slot(2)
    forward(0, opposite, False)

    rowid = lax.broadcasted_iota(jnp.int32, (192, C), 0) % 64
    err = jnp.where(rowid < WIN_TOK, x_s[...] + ysum_s[...] - t_s[...], 0.0)
    err_s[...] = err
    gb_s[...] = err.astype(BF16)
    turned = jnp.transpose(err)
    xt_s[:, 192:384] = turned.astype(BF16)
    xtf_s[0:C, :] = turned
    for b in range(8):
        block = jnp.concatenate([xtf_s[96 * k + 12 * b : 96 * k + 12 * b + 12, :] for k in range(8)], axis=0)
        xtp_s[96 * b : 96 * b + 96, 192:384] = block.astype(BF16)

    def backward(i, first, middle):
        xs = order[i]
        datt = dot(gb_s[...], weight(xs, 3), 1, 1).astype(BF16)
        dqs, dks, dvs = [], [], []
        total = jnp.zeros((64, 384), F32)
        for w in range(3):
            rows = slice(64 * w, 64 * w + 64)
            da = spread(datt[rows])
            dp = dot(v_s[i, rows, :], da, 1, 1)
            pr = p_s[i, w]
            ds = pr * (dp - jnp.sum(pr * dp, axis=0, keepdims=True))
            total = total + ds
            db = ds.astype(BF16)
            dvs.append(dot(pr.astype(BF16), da, 1, 0))
            dks.append(dot(db, spread(q_s[i, rows, :]), 1, 0))
            dqs.append(collapse(dot(db, k_s[i, rows, :], 0, 0)) * scale)
        turned = [jnp.transpose(total[:, 96 * a : 96 * a + 96]) for a in range(4)]
        here = pl.ds(pl.multiple_of(96 * xs, 96), 96)
        dsum_s[0, here, :] = jnp.concatenate(turned[0:2], axis=1)
        dsum_s[1, here, :] = jnp.concatenate(turned[2:4], axis=1)
        dq = jnp.concatenate(dqs, axis=0)
        dk = jnp.concatenate(dks, axis=0)
        dv = jnp.concatenate(dvs, axis=0)
        dqb, dkb, dvb = dq.astype(BF16), dk.astype(BF16), dv.astype(BF16)
        middle()
        lead = jnp.concatenate([dqb[:, 0:128], dvb[:, 0:128]], axis=1)
        low_half = jnp.concatenate([dq[:, 128:192], dk], axis=1).astype(BF16)
        zeros = jnp.zeros((192, 64), F32)
        att = at_s[i].astype(F32)
        mixed = jnp.concatenate(
            [
                jnp.concatenate([dv[:, 128:192], zeros], axis=1),
                jnp.concatenate([zeros, att[:, 0:64]], axis=1),
            ],
            axis=0,
        ).astype(BF16)
        last = att[:, 64:192].astype(BF16)
        for b in range(8):
            rows = slice(96 * b, 96 * b + 96)
            one = dot(xtp_s[rows, 0:192], lead, 1, 0).astype(BF16)
            grads[0, 0, i, b] = one[:, 0:128]
            grads[0, 1, i, b] = one[:, 128:256]
            two = dot(xt_s[rows, 0:192], low_half, 1, 0).astype(BF16)
            grads[2, 0, i, b] = two[:, 0:128]
            grads[1, 0, i, b] = two[:, 128:256]
            grads[2, 1, i, b] = dot(xtp_s[rows, :], mixed, 1, 0).astype(BF16)
            grads[1, 1, i, b] = dot(xt_s[rows, 192:384], last, 1, 0).astype(BF16)
        for num in range(3):
            push(grads.at[num, 1 - c, i], sums.at[num, i], send_d.at[0], recv_d.at[i], partner)
        part = (
            dot(dqb, weight(xs, 0), 1, 0) + dot(dkb, weight(xs, 1), 1, 0) + dot(dvb, weight(xs, 2), 1, 0)
        )
        dxn_s[...] = part if first else dxn_s[...] + part

    lines = (
        (0, y, lambda d: (z, shift(y, d, 8), x, c)),
        (1, z, lambda d: (shift(z, d, 8), y, x, c)),
    )
    far_first = (4, 3, 5, 2, 6, 1, 7)

    def take(i):
        landed(sums.at[:, i], recv_d.at[i])
        for num in range(3):
            for b in range(8):
                sums[num, i, b] = sums[num, i, b] + grads[num, c, i, b]
        if i < 3:
            push(sums.at[2, i], cxf.at[i], send_rx.at[0], recv_rx.at[0], (z, y, order[i], c))
        for d in far_first:
            for num, me, reach in lines:
                push(sums.at[num, i, shift(me, d, 8)], direct.at[num, i, d - 1], send_v.at[0], recv_v.at[i], reach(d))

    def finish(i):
        landed(direct.at[:, i], recv_v.at[i])
        for num, me, reach in lines:
            total = sums[num, i, me].astype(F32)
            for d in range(1, 8):
                total = total + direct[num, i, d - 1].astype(F32)
            sums[num, i, me] = total.astype(BF16)
            if i < 3:
                push(sums.at[num, i, me], s2.at[num, i], send_2.at[0], recv_2.at[0], (z, y, order[i], c))

    backward(0, True, lambda: None)
    backward(1, False, lambda: take(0))
    backward(2, False, lambda: take(1))
    backward(3, False, lambda: take(2))

    dxn = dxn_s[...]
    xhat = xh_s[...]
    dxh = dxn * gain_ref[...].reshape(1, C)
    m1 = jnp.sum(dxh, axis=1, keepdims=True) * (1.0 / C)
    m2 = jnp.sum(dxh * xhat, axis=1, keepdims=True) * (1.0 / C)
    out = err_s[...] + inv * (dxh - m1 - xhat * m2)
    for w in range(3):
        pad_s[49 * w : 49 * w + 49, :] = out[64 * w : 64 * w + 49, :]
    gi_ref[...] = pad_s[0:147, :]
    gain = jnp.sum(dxn * xhat, axis=0, keepdims=True)
    sq = err_s[...]
    loss = jnp.sum(sq * sq, axis=0, keepdims=True)
    loss = sum(loss[:, 128 * j : 128 * j + 128] for j in range(6))
    loss = jnp.sum(loss, axis=1, keepdims=True) + jnp.zeros((1, 128), F32)
    tail = jnp.concatenate(
        [gain[:, 128 * j : 128 * j + 128] for j in range(6)] + [loss, jnp.zeros((1, 128), F32)], axis=0
    )

    dtab = jnp.zeros((64, ENT), F32)
    for p in range(16):
        ds = jnp.concatenate([dsum_s.at[j][pl.ds(p, 24, stride=16), :] for j in range(2)], axis=1)
        top = ds.astype(BF16)
        rem = (ds - top.astype(F32)).astype(BF16)
        z8 = jnp.zeros((8, 256), F32)
        both = jnp.concatenate([top.astype(F32), z8, rem.astype(F32), z8], axis=0).astype(BF16)
        dtab = dtab + dot(both, onehot_rows(relp, p), 1, 1)
    dtab = dtab[0:24] + dtab[32:56]
    for g in range(8):
        sm_ref[g] = jnp.zeros((8, 384), F32)
        sm_ref[g, 0:3, 0:ENT] = dtab[3 * g : 3 * g + 3]
        sm_ref[g, :, 256:384] = tail
    for j, peer in enumerate(talk):
        push(sm_ref.at[2 * peer[2] + peer[3]], sm0.at[j], send_s.at[0], recv_s.at[0], peer)

    take(3)
    finish(0)
    first_x = z * (1 - c) + y * c
    then_x = y * (1 - c) + z * c
    landed(cxf, recv_rx.at[0])
    for b in range(8):
        total = sums[2, 3, b].astype(F32)
        for i in range(3):
            total = total + cxf[i, b].astype(F32)
        sums[2, 3, b] = total.astype(BF16)
    for d in far_first:
        to = (lax.rem(z + d * (1 - c), 8), lax.rem(y + d * c, 8), x, c)
        push(sums.at[2, 3, shift(first_x, d, 8)], s2x.at[d - 1], send_2.at[1], recv_2.at[1], to)
    finish(1)
    landed(sm0, recv_s.at[0])
    ss1[...] = sm_ref[mp] + sum(sm0[j] for j in range(7))
    for j, to in enumerate(line_y):
        push(ss1, sm1.at[j], send_s.at[1], recv_s.at[1], to)
    finish(2)
    finish(3)

    a3[...] = jnp.zeros_like(a3)
    b3[...] = jnp.zeros_like(b3)
    x3[...] = jnp.zeros_like(x3)

    def collect(num, me):
        total = sums[num, 3, me].astype(F32)
        for i in range(3):
            total = total + s2[num, i].astype(F32)
        flat[num, 0:96, :] = total

    def spread_out(src, me, dst, num, reach):
        for d in (4, 3, 5, 2, 6, 1, 7, 0):
            for k, core in enumerate((c, 1 - c)):
                if d or k:
                    push(src.at[shift(me, d, 8)], dst.at[8 * k + d - 1], send_3.at[num], recv_3.at[num], reach(d, core))

    def gathered(src, me, dst, k):
        total = src[me] if k == 0 else dst[7]
        for d in range(1, 8):
            total = total + dst[8 * k + d - 1]
        return total

    landed(s2, recv_2.at[0])
    collect(0, y)
    for i in range(8):
        a3[i, 0:12, :] = flat[0, 12 * i : 12 * i + 12, :]
    spread_out(a3, z, r3a, 0, lambda d, core: (shift(z, d, 8), y, x, core))
    collect(1, z)
    for i in range(8):
        b3[i, 0:12, :] = flat[1, 12 * i : 12 * i + 12, :]
    spread_out(b3, y, r3b, 1, lambda d, core: (z, shift(y, d, 8), x, core))
    landed(s2x, recv_2.at[1])
    total = sums[2, 3, first_x].astype(F32)
    for j in range(7):
        total = total + s2x[j].astype(F32)
    flat[2, 0:96, :] = total
    for i in range(8):
        x3[i, 0:12, :] = flat[2, 12 * i : 12 * i + 12, :]
    spread_out(
        x3, then_x, r3x, 2, lambda d, core: (lax.rem(z + d * c, 8), lax.rem(y + d * (1 - c), 8), x, core)
    )

    landed(sm1, recv_s.at[1])
    ss2[...] = ss1[...] + sum(sm1[j] for j in range(7))
    for j, to in enumerate(line_z):
        push(ss2, sm2.at[j], send_s.at[2], recv_s.at[2], to)
    landed(r3a, recv_3.at[0])
    for k, core in enumerate((c, 1 - c)):
        part_s[core, :, 0:128] = gathered(a3, z, r3a, k)
    landed(r3b, recv_3.at[1])
    for k, core in enumerate((c, 1 - c)):
        part_s[core, :, 256:384] = gathered(b3, y, r3b, k)
    landed(r3x, recv_3.at[2])
    for k, core in enumerate((c, 1 - c)):
        part_s[core, :, 128:256] = gathered(x3, then_x, r3x, k)
    for t in range(4):
        at = 192 * (t % 2)
        both = part_s[t // 2, 0:12, :] * shrink
        mine = jnp.where(c == 0, both[:, at : at + 96], both[:, at + 96 : at + 192])
        if t < 3:
            gq_ref[t] = mine
        else:
            gp_ref[...] = mine
    landed(sm2, recv_s.at[2])
    total = ss2[...] + sum(sm2[j] for j in range(7))
    gtab_ref[...] = total[0:3, 0:TABLE] * shrink
    for j in range(6):
        ggain_ref[pl.ds(128 * j, 128)] = total[j : j + 1, 256:384].reshape(128) * shrink
    loss_ref[...] = total[6:7, 256:384] * (0.5 / count)
    left_here(w_ref.at[:, pl.ds(0, 3), 0], send_w.at[0])
    left_here(w_ref.at[:, :, 0], send_c.at[0])
    left_here(t_ref.at[pl.ds(0, 7)], send_t.at[0])
    left_here(grads.at[:, 0], send_d.at[0])
    left_here(grads.at[0, :, :, pl.ds(0, 7)], send_v.at[0])
    left_here(cxf, send_rx.at[0])
    left_here(s2, send_2.at[0])
    left_here(s2x, send_2.at[1])
    left_here(r3a, send_3.at[0])
    left_here(r3b, send_3.at[1])
    left_here(r3x, send_3.at[2])
    for k, amount in enumerate((sm0, sm1, sm2)):
        left_here(amount, send_s.at[k])


def whole(count, *args):
    dma = pltpu.SemaphoreType.DMA
    f = lambda *s: pltpu.VMEM(s, F32)
    b = lambda *s: pltpu.VMEM(s, BF16)
    shape = jax.ShapeDtypeStruct
    return pl.pallas_call(
        functools.partial(whole_kernel, count),
        name="window_layer",
        out_shape=(
            shape((147, C), F32), shape((3, 12, 96), F32), shape((12, 96), F32),
            shape((3, TABLE), F32), shape((C,), F32), shape((1, 128), F32),
        ),
        in_specs=[pl.BlockSpec(memory_space=pltpu.HBM)] * 8,
        out_specs=(VM,) * 6,
        scratch_shapes=[
            b(147, C), b(147, C), pltpu.VMEM((24, 49), jnp.int32), pltpu.VMEM((49, 49), jnp.int32), f(C), f(3, TABLE),
            f(1, C), b(4, 4, 2, 96, C), f(8, 1, C),
            dma((1,)), dma((2,)), dma((2,)), dma((3,)), dma((1,)), dma((4,)), dma((1,)), dma((1,)), dma((10,)),
            f(160, C), f(192, C), f(192, C), f(192, C), b(192, C), b(C, 384), f(C + 8, 192), b(C, 384),
            f(192, C), f(192, C), b(192, C), f(192, C),
            pltpu.VMEM((64, 128), jnp.int32), f(2, 384, 128), f(4, 64, 384), f(4, 3, 64, 384),
            b(4, 192, 192), b(4, 192, 192), b(4, 192, 192), b(4, 192, 192), f(2, 384, 128), f(8, 8, 384),
            b(3, 2, 4, 8, 96, 128), b(3, 4, 8, 96, 128), b(2, 4, 7, 96, 128),
            b(3, 8, 96, 128), b(2, 3, 96, 128), b(7, 96, 128), f(3, 104, 128),
            f(8, 16, 128), f(8, 16, 128), f(8, 16, 128), f(15, 16, 128), f(15, 16, 128), f(15, 16, 128),
            f(2, 16, 384),
            f(7, 8, 384), f(7, 8, 384), f(7, 8, 384), f(8, 384), f(8, 384),
            dma((1,)), dma((4,)), dma((1,)), dma((4,)), dma((1,)), dma((1,)),
            dma((2,)), dma((2,)), dma((3,)), dma((3,)), dma((3,)), dma((3,)),
        ],
        compiler_params=pltpu.CompilerParams(
            collective_id=0, has_side_effects=True, vmem_limit_bytes=40 * 2**20
        ),
    )(*args)


def hand_out_kernel(*refs):
    copies = [pltpu.make_async_copy(refs[k], refs[6 + k], refs[12].at[k]) for k in range(6)]
    for copy in copies:
        copy.start()
    for copy in copies:
        copy.wait()


def hand_out(*arrays):
    return pl.pallas_call(
        hand_out_kernel,
        name="hand_out",
        out_shape=tuple(jax.ShapeDtypeStruct(a.shape, a.dtype) for a in arrays),
        in_specs=[VM] * 6,
        out_specs=(pl.BlockSpec(memory_space=pl.ANY),) * 6,
        scratch_shapes=[pltpu.SemaphoreType.DMA((6,))],
        compiler_params=pltpu.CompilerParams(vmem_limit_bytes=8 * 2**20),
    )(*arrays)


def per_device(tokens, target, regions, rel_index, layer_norm_gain, bias_table, w_qkv, w_proj):
    count = tokens.shape[0] * lax.axis_size(DP_WIN_MP)
    args = (tokens, target, regions, rel_index, layer_norm_gain, bias_table.T, w_qkv, w_proj)
    done = whole(count, *[pltpu.with_memory_space_constraint(one, pltpu.HBM) for one in args])
    gi, gq, gp, gtab, ggain, loss = hand_out(*done)
    return gi, jnp.transpose(gq, (0, 2, 1)), gp.T, gtab.T, ggain, loss[0, 0]


def solution(mesh):
    split = Mesh(mesh.devices.reshape(mesh.shape["dp"], mesh.shape["win"], 4, 2), DP_WIN_MP)
    return jax.shard_map(
        per_device,
        mesh=split,
        in_specs=(
            P(DP_WIN_MP, None), P(DP_WIN_MP, None), P(("dp", "win"), None), P(), P(),
            P(None, MP), P(None, MP, None), P(MP, None),
        ),
        out_specs=(
            P(DP_WIN_MP, None), P(None, MP, ("dp", "win")), P(MP, ("dp", "win")), P(None, MP), P(), P(),
        ),
        check_vma=False,
    )
```
